128 devices in a mesh: row: 32 (over z, y_lo, x), col: 4 (over y_hi, core).
Axes of the slice: x: 4, y: 4 (y_hi: 2, y_lo: 2; y = y_hi * 2 + y_lo), z: 4, core: 2. Of those that a mesh axis runs over, the one named last changes fastest.
Arguments:
- voltage: float32 [2, 4096, 16384], P(None, ('row', 'col')), may hold values from -6 to 6
- chirp_phase: float32 [16384, 4096], P(('row', 'col')), may hold values from -3.140625 to 3.140625
- filter_taps: float32 [8, 1024], replicated, may hold values from -0.0625 to 0.0625
Outputs:
- filterbank: float32 [2, 1024, 65536], P(None, None, ('row', 'col'))
The draws below stay inside these ranges and needn't reach their ends.
All inputs are finite; a program needn't handle non-finite values.
Results may differ from the reference program's by a relative error of at most 0.00015.
Values sent between devices are 32-bit elements; how exact they have to be, the bound alone decides.
A program may use at most 128 MiB of HBM per device.

```python
import jax
import jax.numpy as jnp
from jax import lax

FFT_ROWS = 4096
FFT_COLS = 16384
CHANNELS = 1024
TAPS = 8
SPECTRA = 65536


def shard_levels(stream_key, shape, pieces, smallest, high):
    gain, own = 1.0, jax.random.fold_in(stream_key, 6)
    for axis_at, blocks in pieces:
        steps = jnp.exp(jax.random.uniform(jax.random.fold_in(own, axis_at), (blocks,), jnp.float32, smallest / len(pieces), high / len(pieces)))
        gain = gain * jnp.repeat(steps, shape[axis_at] // blocks).reshape([-1 if axis == axis_at else 1 for axis in range(len(shape))])
    return gain


def centred(key, extent, spread, bound, pieces=(), dtype=jnp.bfloat16):
    result = jax.random.normal(key, extent, jnp.float32) * spread
    if len(pieces) > 0:
        result = shard_levels(key, extent, pieces, -0.22, 0.18) * result
    return jnp.clip(result, min=-bound, max=bound).astype(dtype)


def setup_inputs(seed: int = 0) -> dict:
    key_list = jax.random.split(jax.random.key(seed), 4)
    return {
        "voltage": centred(key_list[0], (2, FFT_ROWS, FFT_COLS), 1.0, 6.0, ((1, 128),), jnp.float32),
        "chirp_phase": jnp.clip(jax.random.uniform(key_list[1], (FFT_COLS, FFT_ROWS), jnp.float32, -3.140625, 3.140625), -3.140625, 3.140625),
        "filter_taps": centred(key_list[2], (TAPS, CHANNELS), (TAPS * CHANNELS) ** -0.5, 0.0625, (), jnp.float32),
    }


def reference(voltage, chirp_phase, filter_taps):
    series = lax.complex(voltage[0], voltage[1]).reshape(-1)
    spectrum = jnp.fft.fft(series)
    rotation = lax.complex(jnp.cos(chirp_phase), jnp.sin(chirp_phase)).reshape(-1)
    cleaned = jnp.fft.ifft(spectrum * rotation)
    frames = cleaned.reshape(SPECTRA, CHANNELS)
    padded = jnp.pad(frames, ((TAPS - 1, 0), (0, 0)))
    weighted = jnp.zeros_like(frames)
    for tap_delay in range(TAPS):
        offset = TAPS - 1 - tap_delay
        weighted = weighted + filter_taps[tap_delay] * padded[offset:offset + SPECTRA]
    channels_out = jnp.fft.fft(weighted, axis=1)
    return jnp.stack([jnp.real(channels_out).T, jnp.imag(channels_out).T])
```

```python
import math

import jax
import jax.numpy as jnp
from jax import lax
from jax.experimental import pallas as pl
from jax.experimental.pallas import tpu as pltpu
from jax.sharding import PartitionSpec as P

precise = lax.Precision.HIGHEST
device_total = 128
by_mesh = pl.DeviceIdType.MESH


def partner(step):
    row = lax.axis_index("row")
    col = lax.axis_index("col")
    low = lax.rem(step, 4)
    mid = lax.rem(step // 4, 4)
    high = lax.rem(step // 16, 4)
    z = lax.rem(row // 8 + low, 4)
    y = lax.rem((col // 2) * 2 + lax.rem(row // 4, 2) + low + mid, 4)
    x = lax.rem(row + low + mid + high, 4)
    core = lax.rem(col + step // 64, 2)
    return z * 8 + lax.rem(y, 2) * 4 + x, (y // 2) * 2 + core


def exchange_kernel(source, landed, send, recv):
    me = lax.axis_index("row") * 4 + lax.axis_index("col")
    barrier = pltpu.get_barrier_semaphore()

    def greet(step, carry):
        pl.semaphore_signal(barrier, inc=1, device_id=partner(step), device_id_type=by_mesh)
        return carry

    lax.fori_loop(1, device_total, greet, 0)
    pl.semaphore_wait(barrier, device_total - 1)

    def start(step, carry):
        row, col = partner(step)
        pltpu.make_async_remote_copy(
            src_ref=source.at[row * 4 + col],
            dst_ref=landed.at[me],
            send_sem=send,
            recv_sem=recv,
            device_id=(row, col),
            device_id_type=by_mesh,
        ).start()
        return carry

    lax.fori_loop(1, device_total, start, 0)
    landed[me] = source[me]
    others = landed.at[pl.ds(0, device_total - 1)]
    pltpu.make_async_copy(others, others, recv).wait()
    pltpu.make_async_copy(others, others, send).wait()


def exchange(pieces, number):
    return pl.pallas_call(
        exchange_kernel,
        out_shape=jax.ShapeDtypeStruct(pieces.shape, pieces.dtype),
        in_specs=[pl.BlockSpec(memory_space=pltpu.VMEM)],
        out_specs=pl.BlockSpec(memory_space=pltpu.VMEM),
        scratch_shapes=[pltpu.SemaphoreType.DMA, pltpu.SemaphoreType.DMA],
        compiler_params=pltpu.CompilerParams(collective_id=number, has_side_effects=True),
    )(pieces)


def split_up(x, dim, size):
    dims = x.shape
    pieces = x.reshape(*dims[:dim], size, dims[dim] // size, *dims[dim + 1 :])
    return jnp.moveaxis(pieces, dim, 0)


def laid_out(pieces, dim):
    pieces = jnp.moveaxis(pieces, 0, dim)
    dims = pieces.shape
    return pieces.reshape(*dims[:dim], dims[dim] * dims[dim + 1], *dims[dim + 2 :])


def joined_exchange(x, axis, axes, splits, concats):
    sizes = [lax.axis_size(a) for a in axes]
    pieces = split_up(x, splits[0], sizes[0])
    pieces = jnp.moveaxis(split_up(pieces, splits[1] + 1, sizes[1]), 0, 1)
    inside = pieces.shape[2:]
    pieces = pieces.reshape(-1, *inside)
    shape = pieces.shape
    pieces = exchange(pieces.reshape(128, 64, 128), 0).reshape(shape)
    pieces = laid_out(pieces.reshape(*sizes, *inside), concats[0] + 1)
    return laid_out(pieces, concats[1])


def passed_along(block, axis, distance):
    devices = range(lax.axis_size(axis))
    route = [(i - distance, i) for i in devices if i - distance in devices]
    return lax.ppermute(block, axis, route)


def dft_table(radix, direction):
    digits = jnp.arange(radix, dtype=jnp.int32)
    product = digits[:, None] * digits[None, :] % radix
    turn = direction * 2.0 * math.pi / radix * product.astype(jnp.float32)
    cos_part = jnp.cos(turn)
    sin_part = jnp.sin(turn)
    upper = jnp.stack([cos_part, sin_part], axis=1)
    lower = jnp.stack([-sin_part, cos_part], axis=1)
    return jnp.stack([upper, lower], axis=0)


def complex_product(values, cos_part, sin_part):
    real_part = values[0] * cos_part - values[1] * sin_part
    imag_part = values[0] * sin_part + values[1] * cos_part
    return jnp.stack([real_part, imag_part])


def inner_twist(outer_radix, inner_radix, direction):
    outer_digits = jnp.arange(outer_radix, dtype=jnp.int32)
    inner_digits = jnp.arange(inner_radix, dtype=jnp.int32)
    length = outer_radix * inner_radix
    product = outer_digits[:, None] * inner_digits[None, :] % length
    turn = direction * 2.0 * math.pi / length * product.astype(jnp.float32)
    return (jnp.cos(turn), jnp.sin(turn))


def dft_rows(values, direction):
    length = values.shape[1]
    column_count = values.shape[2]
    inner_radix = min(length, 128)
    outer_radix = length // inner_radix
    blocked = values.reshape(2, outer_radix, inner_radix, column_count)
    partial_value = jnp.einsum(
        "cadk,cabm->dkbm", dft_table(outer_radix, direction), blocked, precision=precise
    )
    cos_part, sin_part = inner_twist(outer_radix, inner_radix, direction)
    partial_value = complex_product(partial_value, cos_part[:, :, None], sin_part[:, :, None])
    result = jnp.einsum(
        "cbdq,ckbm->dqkm", dft_table(inner_radix, direction), partial_value, precision=precise
    )
    return result.reshape(2, length, column_count)


def dft_cols(values, direction):
    length = values.shape[2]
    row_count = values.shape[1]
    inner_radix = min(length, 128)
    outer_radix = length // inner_radix
    blocked = values.reshape(2, row_count, outer_radix, inner_radix)
    partial_value = jnp.einsum(
        "cadk,cmab->dmkb", dft_table(outer_radix, direction), blocked, precision=precise
    )
    cos_part, sin_part = inner_twist(outer_radix, inner_radix, direction)
    partial_value = complex_product(partial_value, cos_part, sin_part)
    result = jnp.einsum(
        "cbdq,cmkb->dmqk", dft_table(inner_radix, direction), partial_value, precision=precise
    )
    return result.reshape(2, row_count, length)


def rotate(values, row_index, col_index, total, direction, factor):
    product = row_index[:, None] * col_index[None, :] % total
    turn = direction * 2.0 * math.pi / total * product.astype(jnp.float32)
    return complex_product(values, factor * jnp.cos(turn), factor * jnp.sin(turn))


def spread(values):
    row_devices = lax.axis_size("row")
    col_devices = lax.axis_size("col")
    depth_rows = values.shape[1]
    span_cols = values.shape[2] // (row_devices * col_devices)
    blocked = values.reshape(2, 1, 1, depth_rows, row_devices, col_devices, span_cols)
    arrived = joined_exchange(blocked, ("row", "col"), ("row", "col"), (4, 5), (1, 2))
    return arrived.reshape(2, row_devices * col_devices * depth_rows, span_cols)


def collect(values):
    row_devices = lax.axis_size("row")
    col_devices = lax.axis_size("col")
    depth_rows = values.shape[1] // (row_devices * col_devices)
    span_cols = values.shape[2]
    blocked = values.reshape(2, row_devices, col_devices, depth_rows, 1, 1, span_cols)
    arrived = joined_exchange(blocked, ("row", "col"), ("row", "col"), (1, 2), (4, 5))
    return arrived.reshape(2, depth_rows, row_devices * col_devices * span_cols)


def local(voltage, chirp_phase, filter_taps):
    device_count = lax.axis_size("row") * lax.axis_size("col")
    device = lax.axis_index(("row", "col"))
    local_rows = voltage.shape[1]
    total_rows = local_rows * device_count
    total_cols = voltage.shape[2]
    local_cols = total_cols // device_count
    total = total_rows * total_cols
    signal = spread(voltage)
    signal = dft_rows(signal, -1.0)
    row_index = jnp.arange(total_rows, dtype=jnp.int32)
    col_index = device * local_cols + jnp.arange(local_cols, dtype=jnp.int32)
    signal = rotate(signal, row_index, col_index, total, -1.0, 1.0)
    signal = collect(signal)
    signal = dft_cols(signal, -1.0)
    turned_phase = jnp.transpose(chirp_phase)
    local_phase = lax.all_to_all(
        turned_phase, ("row", "col"), split_axis=0, concat_axis=1, tiled=True
    )
    signal = complex_product(signal, jnp.cos(local_phase), jnp.sin(local_phase))
    signal = dft_cols(signal, 1.0)
    row_index = device * local_rows + jnp.arange(local_rows, dtype=jnp.int32)
    col_index = jnp.arange(total_cols, dtype=jnp.int32)
    signal = rotate(signal, row_index, col_index, total, 1.0, 1.0 / total)
    signal = spread(signal)
    signal = dft_rows(signal, 1.0)
    signal = collect(signal)
    tap_count = filter_taps.shape[0]
    channel_count = filter_taps.shape[1]
    samples = signal.reshape(2, local_rows * total_cols)
    frame_count = samples.shape[1] // channel_count
    frames = samples.reshape(2, frame_count, channel_count)
    history = passed_along(frames[:, frame_count - tap_count + 1 :, :], ("row", "col"), 1)
    extended = jnp.concatenate([history, frames], axis=1)
    turned = jnp.transpose(extended, (0, 2, 1))
    weighted = jnp.zeros((2, channel_count, frame_count), jnp.float32)
    for tap_delay in range(tap_count):
        offset = tap_count - 1 - tap_delay
        weighted = (
            weighted
            + filter_taps[tap_delay][None, :, None] * turned[:, :, offset : offset + frame_count]
        )
    return dft_rows(weighted, -1.0)


def solution(mesh):
    in_specs = (P(None, ("row", "col"), None), P(("row", "col"), None), P())
    out_specs = P(None, None, ("row", "col"))
    return jax.shard_map(local, mesh=mesh, in_specs=in_specs, out_specs=out_specs, check_vma=False)
```

```python
import math

import jax
import jax.numpy as jnp
import numpy as np
from jax import lax
from jax.experimental import pallas as pl
from jax.experimental.pallas import tpu as pltpu
from jax.sharding import PartitionSpec as P

DEVICES = 128
ROWS = 32
TILE = 8
PARTS = ROWS // TILE
LANES = 128
LOG_TOTAL = 26
BY_MESH = pl.DeviceIdType.MESH
F32 = jnp.float32
BF16 = jnp.bfloat16


def partner(step):
    row = lax.axis_index("row")
    col = lax.axis_index("col")
    low = lax.rem(step, 4)
    mid = low + lax.rem(step // 4, 4)
    high = mid + lax.rem(step // 16, 4)
    z = lax.rem(row // 8 + low, 4)
    y = lax.rem((col // 2) * 2 + lax.rem(row // 4, 2) + mid, 4)
    x = lax.rem(row + high, 4)
    core = lax.rem(col + step // 64, 2)
    return z * 8 + lax.rem(y, 2) * 4 + x, (y // 2) * 2 + core


def times(a, b):
    return a[0] * b[0] - a[1] * b[1], a[0] * b[1] + a[1] * b[0]


def times_conj(a, b):
    return a[0] * b[0] + a[1] * b[1], a[1] * b[0] - a[0] * b[1]


def plus(a, b):
    return a[0] + b[0], a[1] + b[1]


def minus(a, b):
    return a[0] - b[0], a[1] - b[1]


def turned(a, part, whole, sign):
    part = part % whole
    eighths = 8 * part / whole
    if eighths == 0:
        return a
    if eighths == 2:
        return (-a[1], a[0]) if sign > 0 else (a[1], -a[0])
    if eighths == 4:
        return -a[0], -a[1]
    if eighths == 6:
        return (a[1], -a[0]) if sign > 0 else (-a[1], a[0])
    angle = sign * 2.0 * math.pi * part / whole
    cos_part, sin_part = math.cos(angle), math.sin(angle)
    if eighths in (1, 3, 5, 7):
        half = math.sqrt(0.5)
        c = half if cos_part > 0 else -half
        same = (cos_part > 0) == (sin_part > 0)
        if same:
            return (a[0] - a[1]) * c, (a[0] + a[1]) * c
        return (a[0] + a[1]) * c, (a[1] - a[0]) * c
    return a[0] * cos_part - a[1] * sin_part, a[0] * sin_part + a[1] * cos_part


def small_dft(xs, sign):
    n = len(xs)
    if n == 1:
        return xs
    if n == 2:
        return [plus(xs[0], xs[1]), minus(xs[0], xs[1])]
    parts = [small_dft(xs[r::4], sign) for r in range(4)]
    out = [None] * n
    for k in range(n // 4):
        a, b, c, d = (turned(parts[r][k], r * k, n, sign) for r in range(4))
        ac, bd = plus(a, c), plus(b, d)
        ac_, bd_ = minus(a, c), turned(minus(b, d), 1, 4, sign)
        out[k] = plus(ac, bd)
        out[k + n // 4] = plus(ac_, bd_)
        out[k + n // 2] = minus(ac, bd)
        out[k + 3 * n // 4] = minus(ac_, bd_)
    return out


def block_dft(load, scratch, finish, sign):
    for low in range(8):
        values = small_dft([load(8 * high + low) for high in range(16)], sign)
        for k, value in enumerate(values):
            value = turned(value, low * k, 128, sign)
            scratch[8 * k + low, 0] = value[0]
            scratch[8 * k + low, 1] = value[1]

    def second(k, carry):
        values = small_dft(
            [(scratch[8 * k + low, 0], scratch[8 * k + low, 1]) for low in range(8)], sign
        )
        for high, value in enumerate(values):
            finish(k + 16 * high, value)
        return carry

    lax.fori_loop(0, 16, second, 0)


def quarter_sincos(angle, quarter):
    square = angle * angle
    sin_part = angle * (
        1.0 + square * (-1.0 / 6 + square * (1.0 / 120 + square * (-1.0 / 5040 + square / 362880)))
    )
    cos_part = 1.0 + square * (
        -0.5 + square * (1.0 / 24 + square * (-1.0 / 720 + square * (1.0 / 40320)))
    )
    odd = (quarter & 1) == 1
    first = jnp.where(odd, sin_part, cos_part)
    second = jnp.where(odd, cos_part, sin_part)
    return (
        jnp.where(((quarter + 1) & 2) == 2, -first, first),
        jnp.where((quarter & 2) == 2, -second, second),
    )


def unit(product, log_whole):
    quarter = (product + (1 << (log_whole - 3))) >> (log_whole - 2)
    rest = product - (quarter << (log_whole - 2))
    return quarter_sincos(rest.astype(F32) * (2.0 * math.pi / 2**log_whole), quarter)


def phase_unit(phase):
    quarter = jnp.floor(phase * (2.0 / math.pi) + 0.5)
    high = float(np.float32(1.5703125))
    angle = (phase - quarter * high) - quarter * (math.pi / 2 - high)
    return quarter_sincos(angle, quarter.astype(jnp.int32))


def halves(x):
    high = x.astype(BF16)
    return high, (x - high.astype(F32)).astype(BF16)


def kernel(
    voltage,
    phase,
    taps,
    rows_fwd,
    rows_inv,
    lanes_fwd,
    lanes_inv,
    lanes_out,
    mid_turn,
    out_turn,
    result,
    recv1,
    work,
    send2,
    recv2,
    send3,
    recv3,
    send4,
    recv4,
    phase_in,
    phase_send,
    phase_recv,
    chirp,
    table_a,
    table_b,
    tiles,
    wide,
    edge_send,
    edge_recv,
    local_sem,
    sems1,
    sems2,
    sems3,
    sems4,
    phase_sem,
    edge_sem,
    send_sems,
    out_sem,
):
    row = lax.axis_index("row")
    col = lax.axis_index("col")
    me = row * 4 + col
    sublane = lax.broadcasted_iota(jnp.int32, (ROWS, LANES), 0)
    lane = lax.broadcasted_iota(jnp.int32, (ROWS, LANES), 1)

    phase_copy = pltpu.make_async_copy(phase, phase_in, local_sem.at[0])
    phase_copy.start()
    own_copy = pltpu.make_async_copy(
        voltage.at[:, :, pl.ds(pl.multiple_of(me * LANES, LANES), LANES)],
        recv1.at[me],
        local_sem.at[1],
    )
    own_copy.start()

    barrier = pltpu.get_barrier_semaphore()

    def greet(step, carry):
        pl.semaphore_signal(barrier, inc=1, device_id=partner(step), device_id_type=BY_MESH)
        return carry

    lax.fori_loop(1, DEVICES, greet, 0)
    pl.semaphore_wait(barrier, DEVICES - 1)

    def send_piece(step, source_of, target, send_sem, recv_sem):
        to_row, to_col = partner(step)
        pltpu.make_async_remote_copy(
            src_ref=source_of(to_row * 4 + to_col),
            dst_ref=target,
            send_sem=send_sem,
            recv_sem=recv_sem,
            device_id=(to_row, to_col),
            device_id_type=BY_MESH,
        ).start()

    def tile_rows(part):
        return pl.ds(pl.multiple_of(part * TILE, TILE), TILE)

    def wait_part(buffer, sem):
        ref = buffer.at[pl.ds(0, DEVICES - 1), :, pl.ds(0, TILE), :]
        pltpu.make_async_copy(ref, ref, sem).wait()

    def voltage_part(part, carry):
        def one(step, inner):
            send_piece(
                step,
                lambda to: voltage.at[
                    :, tile_rows(part), pl.ds(pl.multiple_of(to * LANES, LANES), LANES)
                ],
                recv1.at[me, :, tile_rows(part), :],
                send_sems.at[0],
                sems1.at[part],
            )
            return inner

        lax.fori_loop(1, DEVICES, one, 0)
        return carry

    lax.fori_loop(0, PARTS, voltage_part, 0)

    phase_copy.wait()

    def phase_out(b, carry):
        block = phase_in[:, pl.ds(pl.multiple_of(b * LANES, LANES), LANES)]
        phase_send[:, pl.ds(b, 1), :] = jnp.transpose(block).reshape(DEVICES, 1, LANES)
        return carry

    lax.fori_loop(0, ROWS, phase_out, 0)

    def phase_piece(step, carry):
        send_piece(
            step, lambda to: phase_send.at[to], phase_recv.at[me], send_sems.at[1], phase_sem
        )
        return carry

    lax.fori_loop(1, DEVICES, phase_piece, 0)
    phase_recv[me] = phase_send[me]

    def fill(a, carry):
        cos_part, sin_part = unit(sublane * a, 12)
        table_a[a, 0] = cos_part
        table_a[a, 1] = -sin_part
        cos_part, sin_part = unit((a + 128 * sublane) * (128 * me + lane), LOG_TOTAL)
        table_b[a, 0] = cos_part
        table_b[a, 1] = -sin_part
        return carry

    lax.fori_loop(0, DEVICES, fill, 0)

    own_copy.wait()

    def first_part(part, carry):
        wait_part(recv1, sems1.at[part])
        at = tile_rows(part)

        def load(n):
            return recv1[n, 0, at, :], recv1[n, 1, at, :]

        def finish(k, value):
            turn = table_a[k, 0, at, :], table_a[k, 1, at, :]
            value = times(value, turn)
            work[k, 0, at, :] = value[0]
            work[k, 1, at, :] = value[1]

        block_dft(load, tiles, finish, -1)
        return carry

    lax.fori_loop(0, PARTS, first_part, 0)

    def row_dft(matrix, first, second):
        high, low = halves(
            jnp.concatenate([first.reshape(64, LANES), second.reshape(64, LANES)], axis=1)
        )
        return jnp.dot(
            matrix[...],
            jnp.concatenate([high, low, high], axis=0),
            preferred_element_type=F32,
        )

    def index_of(step):
        to_row, to_col = partner(step)
        return to_row * 4 + to_col

    def second_step(pair, carry):
        places = index_of(2 * pair), index_of(2 * pair + 1)
        both = row_dft(rows_fwd, work[places[0]], work[places[1]])
        for at, place in enumerate(places):
            value = (
                both[:ROWS, at * LANES : (at + 1) * LANES],
                both[ROWS:, at * LANES : (at + 1) * LANES],
            )
            value = times(value, (table_b[place, 0], table_b[place, 1]))
            send2[place, 0] = value[0]
            send2[place, 1] = value[1]
        return carry

    def send_part(buffer, target, part, send_sem, recv_sem):
        def one(step, inner):
            send_piece(
                step,
                lambda to: buffer.at[to, :, tile_rows(part), :],
                target.at[me, :, tile_rows(part), :],
                send_sem,
                recv_sem,
            )
            return inner

        lax.fori_loop(1, DEVICES, one, 0)

    lax.fori_loop(0, DEVICES // 2, second_step, 0)
    recv2[me] = send2[me]

    def send2_part(part, carry):
        send_part(send2, recv2, part, send_sems.at[2], sems2.at[part])
        return carry

    lax.fori_loop(0, PARTS, send2_part, 0)

    phase_all = phase_recv.at[pl.ds(0, DEVICES - 1)]
    pltpu.make_async_copy(phase_all, phase_all, phase_sem).wait()

    def phase_back(b, carry):
        block = phase_recv[:, pl.ds(b, 1), :].reshape(DEVICES, LANES)
        cos_part, sin_part = phase_unit(jnp.transpose(block))
        chirp[:, 0, pl.ds(b, 1), :] = cos_part.reshape(DEVICES, 1, LANES)
        chirp[:, 1, pl.ds(b, 1), :] = sin_part.reshape(DEVICES, 1, LANES)
        return carry

    lax.fori_loop(0, ROWS, phase_back, 0)

    def refill(h, carry):
        cos_part, sin_part = unit((me + 128 * sublane) * (128 * h + lane), LOG_TOTAL)
        table_b[h, 0] = cos_part
        table_b[h, 1] = sin_part
        return carry

    lax.fori_loop(0, DEVICES, refill, 0)

    def middle_part(part, carry):
        wait_part(recv2, sems2.at[part])
        at = tile_rows(part)

        def load(n):
            return recv2[n, 0, at, :], recv2[n, 1, at, :]

        def finish(k, value):
            turn = mid_turn[0, pl.ds(k, 1), :], mid_turn[1, pl.ds(k, 1), :]
            value = times(value, turn)
            wide[k, :, :LANES] = value[0]
            wide[k, :, LANES:] = value[1]

        block_dft(load, tiles, finish, -1)

        def lanes_step(group, inner):
            rows = pl.ds(group * 32, 32)
            high, low = halves(wide[rows].reshape(32 * TILE, 2 * LANES))
            there = jnp.dot(
                jnp.concatenate([high, low, high], axis=1),
                lanes_fwd[...],
                preferred_element_type=F32,
            )
            turn = (
                chirp[rows, 0, at, :].reshape(32 * TILE, LANES),
                chirp[rows, 1, at, :].reshape(32 * TILE, LANES),
            )
            there = times((there[:, :LANES], there[:, LANES:]), turn)
            high, low = halves(jnp.concatenate(there, axis=1))
            back = jnp.dot(
                jnp.concatenate([high, low, high], axis=1),
                lanes_inv[...],
                preferred_element_type=F32,
            )
            wide[rows] = back.reshape(32, TILE, 2 * LANES)
            return inner

        lax.fori_loop(0, 4, lanes_step, 0)

        def load_back(n):
            turn = mid_turn[0, pl.ds(n, 1), :], mid_turn[1, pl.ds(n, 1), :]
            return times_conj((wide[n, :, :LANES], wide[n, :, LANES:]), turn)

        def finish_back(k, value):
            value = times(value, (table_b[k, 0, at, :], table_b[k, 1, at, :]))
            send3[k, 0, at, :] = value[0]
            send3[k, 1, at, :] = value[1]

        block_dft(load_back, tiles, finish_back, 1)
        recv3[me, :, at, :] = send3[me, :, at, :]
        send_part(send3, recv3, part, send_sems.at[3], sems3.at[part])
        return carry

    lax.fori_loop(0, PARTS, middle_part, 0)

    def wait3(part, carry):
        wait_part(recv3, sems3.at[part])
        return carry

    lax.fori_loop(0, PARTS, wait3, 0)

    def third_step(pair, carry):
        both = row_dft(rows_inv, recv3[2 * pair], recv3[2 * pair + 1])
        for at in range(2):
            place = 2 * pair + at
            value = (
                both[:ROWS, at * LANES : (at + 1) * LANES],
                both[ROWS:, at * LANES : (at + 1) * LANES],
            )
            value = times_conj(value, (table_a[place, 0], table_a[place, 1]))
            work[place, 0] = value[0]
            work[place, 1] = value[1]
        return carry

    lax.fori_loop(0, DEVICES // 2, third_step, 0)

    def fourth_part(turn, carry):
        part = PARTS - 1 - turn
        at = tile_rows(part)

        def load(n):
            return work[n, 0, at, :], work[n, 1, at, :]

        def finish(k, value):
            send4[k, 0, at, :] = value[0]
            send4[k, 1, at, :] = value[1]

        block_dft(load, tiles, finish, 1)
        recv4[me, :, at, :] = send4[me, :, at, :]
        send_part(send4, recv4, part, send_sems.at[4], sems4.at[part])
        return carry

    lax.fori_loop(0, PARTS, fourth_part, 0)

    wait_part(recv4, sems4.at[3])

    def edge_out(j, carry):
        edge_send[j, 0:1, :] = recv4[72 + j, 0, ROWS - 1 : ROWS, :]
        edge_send[j, 1:2, :] = recv4[72 + j, 1, ROWS - 1 : ROWS, :]
        return carry

    lax.fori_loop(0, 56, edge_out, 0)
    following = lax.rem(me + 1, DEVICES)
    edge_copy = pltpu.make_async_remote_copy(
        src_ref=edge_send,
        dst_ref=edge_recv,
        send_sem=send_sems.at[5],
        recv_sem=edge_sem,
        device_id=(following // 4, lax.rem(following, 4)),
        device_id_type=BY_MESH,
    )
    edge_copy.start()
    first_row = lax.broadcasted_iota(jnp.int32, (TILE, LANES), 0) == 0
    ahead = me > 0

    def filter_half(half):
        tile_list = (2 * half, 2 * half + 1)

        def one_position(high, carry):
            weights = [
                taps[t : t + 1, pl.ds(pl.multiple_of(high * LANES, LANES), LANES)]
                for t in range(8)
            ]
            for part in tile_list:
                at = slice(part * TILE, part * TILE + TILE)
                for c in range(2):
                    now = [recv4[8 * m + high, c, at, :] for m in range(16)]
                    old = [None] * 16
                    for m in range(9, 16):
                        shifted = pltpu.roll(now[m], 1, 0)
                        if part == 0:
                            edge = edge_recv[8 * (m - 9) + high, c : c + 1, :]
                            edge = jnp.where(ahead, edge, 0.0)
                        else:
                            edge = recv4[8 * m + high, c, part * TILE - 1 : part * TILE, :]
                        old[m] = jnp.where(first_row, edge, shifted)
                    for m in range(16):
                        total = weights[0] * now[m]
                        for t in range(1, 8):
                            total = total + weights[t] * (now[m - t] if m >= t else old[m - t + 16])
                        work[16 * high + m, c, at, :] = total
            return carry

        lax.fori_loop(0, 8, one_position, 0)

        def one_frame(m, carry):
            for at_tile, part in enumerate(tile_list):
                at = slice(part * TILE, part * TILE + TILE)
                values = small_dft(
                    [(work[16 * high + m, 0, at, :], work[16 * high + m, 1, at, :]) for high in range(8)],
                    -1,
                )
                for a, value in enumerate(values):
                    value = times(value, (out_turn[0, a : a + 1, :], out_turn[1, a : a + 1, :]))
                    for c in range(2):
                        tiles_out[a, c, pl.ds(128 * at_tile + m, TILE, stride=16), :] = value[c]
            return carry

        lax.fori_loop(0, 16, one_frame, 0)

        def one_class(a, carry):
            frames = jnp.concatenate([tiles_out[a, 0], tiles_out[a, 1]], axis=1)
            high, low = halves(frames)
            both = lax.dot_general(
                lanes_out[...],
                jnp.concatenate([high, low, high], axis=1),
                (((1,), (1,)), ((), ())),
                preferred_element_type=F32,
            )
            for c in range(2):
                for side in range(2):
                    gathered[c, 2 * half + side, pl.ds(a, 128, stride=8), :] = both[
                        c * 128 : c * 128 + 128, side * LANES : side * LANES + LANES
                    ]
            return carry

        lax.fori_loop(0, 8, one_class, 0)
        for side in range(2):
            column = 2 * half + side
            pltpu.make_async_copy(
                gathered.at[:, column],
                result.at[:, :, pl.ds(column * LANES, LANES)],
                out_sem.at[column],
            ).start()

    tiles_out = table_a.reshape(16, 2, 256, LANES)
    gathered = table_b.reshape(2, 4, 1024, LANES)

    wait_part(recv4, sems4.at[2])
    wait_part(recv4, sems4.at[1])
    filter_half(1)
    wait_part(recv4, sems4.at[0])
    edge_copy.wait_recv()
    filter_half(0)

    for column in range(4):
        pltpu.make_async_copy(
            gathered.at[:, column],
            result.at[:, :, pl.ds(column * LANES, LANES)],
            out_sem.at[column],
        ).wait()
    edge_copy.wait_send()
    pieces = recv1.at[pl.ds(0, DEVICES - 1)]
    for at in (0, 2, 3, 4):
        pltpu.make_async_copy(pieces, pieces, send_sems.at[at]).wait()
    pltpu.make_async_copy(phase_all, phase_all, send_sems.at[1]).wait()


def dft_parts(size, sign, scale=1.0):
    digits = np.arange(size)
    angle = sign * 2.0 * np.pi * ((digits[:, None] * digits[None, :]) % size) / size
    return scale * np.cos(angle), scale * np.sin(angle)


def bf16_halves(matrix):
    matrix = np.asarray(matrix, np.float32)
    high = matrix.astype(BF16)
    return high, (matrix - high.astype(np.float32)).astype(BF16)


def left_matrix(size, sign):
    c, s = dft_parts(size, sign)
    high, low = bf16_halves(np.block([[c, -s], [s, c]]))
    return np.concatenate([high, high, low], axis=1)


def right_matrix(size, sign, scale=1.0):
    c, s = dft_parts(size, sign, scale)
    high, low = bf16_halves(np.block([[c, s], [-s, c]]))
    return np.concatenate([high, high, low], axis=0)


def turn_table(rows, cols, whole):
    product = np.arange(rows)[:, None] * np.arange(cols)[None, :] % whole
    angle = -2.0 * np.pi * product / whole
    return np.stack([np.cos(angle), np.sin(angle)]).astype(np.float32)


def local(voltage, chirp_phase, filter_taps):
    constants = [
        left_matrix(ROWS, -1),
        left_matrix(ROWS, 1),
        right_matrix(LANES, -1),
        right_matrix(LANES, 1, 2.0**-LOG_TOTAL),
        left_matrix(LANES, -1),
        turn_table(128, LANES, 128 * LANES),
        turn_table(8, LANES, 8 * LANES),
    ]
    blocks = pltpu.VMEM((DEVICES, 2, ROWS, LANES), F32)
    phases = pltpu.VMEM((DEVICES, ROWS, LANES), F32)
    in_vmem = pl.BlockSpec(memory_space=pltpu.VMEM)
    in_hbm = pl.BlockSpec(memory_space=pl.ANY)
    return pl.pallas_call(
        kernel,
        out_shape=jax.ShapeDtypeStruct((2, 1024, 512), F32),
        in_specs=[in_hbm, in_hbm] + [in_vmem] * (1 + len(constants)),
        out_specs=in_hbm,
        scratch_shapes=[blocks] * 8
        + [pltpu.VMEM((DEVICES, 4096), F32)]
        + [phases] * 2
        + [blocks] * 3
        + [
            pltpu.VMEM((DEVICES, 2, TILE, LANES), F32),
            pltpu.VMEM((DEVICES, TILE, 2 * LANES), F32),
            pltpu.VMEM((56, 2, LANES), F32),
            pltpu.VMEM((56, 2, LANES), F32),
            pltpu.SemaphoreType.DMA((2,)),
            pltpu.SemaphoreType.DMA((PARTS,)),
            pltpu.SemaphoreType.DMA((PARTS,)),
            pltpu.SemaphoreType.DMA((PARTS,)),
            pltpu.SemaphoreType.DMA((PARTS,)),
            pltpu.SemaphoreType.DMA,
            pltpu.SemaphoreType.DMA,
            pltpu.SemaphoreType.DMA((6,)),
            pltpu.SemaphoreType.DMA((4,)),
        ],
        compiler_params=pltpu.CompilerParams(
            collective_id=0, has_side_effects=True, vmem_limit_bytes=67043328
        ),
    )(voltage, chirp_phase, filter_taps, *[jnp.asarray(c) for c in constants])


def solution(mesh):
    in_specs = (P(None, ("row", "col"), None), P(("row", "col"), None), P())
    out_specs = P(None, None, ("row", "col"))
    return jax.shard_map(local, mesh=mesh, in_specs=in_specs, out_specs=out_specs, check_vma=False)
```

```python
import math

import jax
import jax.numpy as jnp
import numpy as np
from jax import lax
from jax.experimental import pallas as pl
from jax.experimental.pallas import tpu as pltpu
from jax.sharding import PartitionSpec as P

DEVICES = 128
ROWS = 32
TILE = 8
PARTS = ROWS // TILE
LANES = 128
LOG_TOTAL = 26
GROUPS = DEVICES // 16
CONSTANTS = 8
BY_MESH = pl.DeviceIdType.MESH
F32 = jnp.float32
BF16 = jnp.bfloat16


def device_at(z, y, x, core):
    return z * 8 + lax.rem(y, 2) * 4 + x, (y // 2) * 2 + core


def partner(here, step, way=1):
    z, y, x, core = here
    low = lax.rem(step, 4)
    mid = low + lax.rem(step // 4, 4)
    high = mid + lax.rem(step // 16, 4)
    return device_at(
        lax.rem(z + way * low, 4),
        lax.rem(y + way * mid, 4),
        lax.rem(x + way * high, 4),
        lax.rem(core + step // 64, 2),
    )


def times(a, b):
    return a[0] * b[0] - a[1] * b[1], a[0] * b[1] + a[1] * b[0]


def times_conj(a, b):
    return a[0] * b[0] + a[1] * b[1], a[1] * b[0] - a[0] * b[1]


def plus(a, b):
    return a[0] + b[0], a[1] + b[1]


def minus(a, b):
    return a[0] - b[0], a[1] - b[1]


def turned(a, part, whole, sign):
    part = part % whole
    eighths = 8 * part / whole
    if eighths == 0:
        return a
    if eighths == 2:
        return (-a[1], a[0]) if sign > 0 else (a[1], -a[0])
    if eighths == 4:
        return -a[0], -a[1]
    if eighths == 6:
        return (a[1], -a[0]) if sign > 0 else (-a[1], a[0])
    angle = sign * 2.0 * math.pi * part / whole
    cos_part, sin_part = math.cos(angle), math.sin(angle)
    if eighths in (1, 3, 5, 7):
        half = math.sqrt(0.5)
        c = half if cos_part > 0 else -half
        same = (cos_part > 0) == (sin_part > 0)
        if same:
            return (a[0] - a[1]) * c, (a[0] + a[1]) * c
        return (a[0] + a[1]) * c, (a[1] - a[0]) * c
    return a[0] * cos_part - a[1] * sin_part, a[0] * sin_part + a[1] * cos_part


def small_dft(xs, sign):
    n = len(xs)
    if n == 1:
        return xs
    if n == 2:
        return [plus(xs[0], xs[1]), minus(xs[0], xs[1])]
    parts = [small_dft(xs[r::4], sign) for r in range(4)]
    out = [None] * n
    for k in range(n // 4):
        a, b, c, d = (turned(parts[r][k], r * k, n, sign) for r in range(4))
        ac, bd = plus(a, c), plus(b, d)
        ac_, bd_ = minus(a, c), turned(minus(b, d), 1, 4, sign)
        out[k] = plus(ac, bd)
        out[k + n // 4] = plus(ac_, bd_)
        out[k + n // 2] = minus(ac, bd)
        out[k + 3 * n // 4] = minus(ac_, bd_)
    return out


def block_dft(load, scratch, finish, sign):
    for low in range(8):
        values = small_dft([load(8 * high + low) for high in range(16)], sign)
        for k, value in enumerate(values):
            value = turned(value, low * k, 128, sign)
            scratch[8 * k + low, 0] = value[0]
            scratch[8 * k + low, 1] = value[1]

    def second(k, carry):
        values = small_dft(
            [(scratch[8 * k + low, 0], scratch[8 * k + low, 1]) for low in range(8)], sign
        )
        for high, value in enumerate(values):
            finish(k + 16 * high, value)
        return carry

    lax.fori_loop(0, 16, second, 0)


def quarter_sincos(angle, quarter):
    square = angle * angle
    sin_part = angle * (
        1.0 + square * (-1.0 / 6 + square * (1.0 / 120 + square * (-1.0 / 5040 + square / 362880)))
    )
    cos_part = 1.0 + square * (
        -0.5 + square * (1.0 / 24 + square * (-1.0 / 720 + square * (1.0 / 40320)))
    )
    odd = (quarter & 1) == 1
    first = jnp.where(odd, sin_part, cos_part)
    second = jnp.where(odd, cos_part, sin_part)
    return (
        jnp.where(((quarter + 1) & 2) == 2, -first, first),
        jnp.where((quarter & 2) == 2, -second, second),
    )


def unit(product, log_whole):
    quarter = (product + (1 << (log_whole - 3))) >> (log_whole - 2)
    rest = product - (quarter << (log_whole - 2))
    return quarter_sincos(rest.astype(F32) * (2.0 * math.pi / 2**log_whole), quarter)


def phase_unit(phase):
    quarter = jnp.floor(phase * (2.0 / math.pi) + 0.5)
    high = float(np.float32(1.5703125))
    angle = (phase - quarter * high) - quarter * (math.pi / 2 - high)
    return quarter_sincos(angle, quarter.astype(jnp.int32))


def halves(x):
    high = x.astype(BF16)
    return high, (x - high.astype(F32)).astype(BF16)


def frames_dft(matrix, real_part, imag_part):
    high, low = halves(jnp.concatenate([real_part, imag_part], axis=1))
    return lax.dot_general(
        matrix[...],
        jnp.concatenate([high, low, high], axis=1),
        (((1,), (1,)), ((), ())),
        preferred_element_type=F32,
    )


def kernel(
    voltage,
    phase,
    *refs,
):
    given, refs = refs[:CONSTANTS], refs[CONSTANTS:]
    late, ready, refs = refs[0], refs[1], refs[2:]
    held, refs = refs[:CONSTANTS], refs[CONSTANTS:]
    taps, rows_fwd, rows_inv, lanes_fwd, lanes_inv, lanes_out, mid_turn, out_turn = held
    (
    recv1,
    work,
    send2,
    recv2,
    send3,
    recv3,
    send4,
    recv4,
    phase_in,
    phase_send,
    phase_recv,
    chirp,
    table_a,
    table_b,
    tiles,
    wide,
    edge_send,
    edge_recv,
    local_sem,
    sems1,
    sems2,
    sems3,
    sems4,
    phase_sem,
    edge_sem,
    send_sems,
    out_sem,
    given_sem,
    plane_sem,
    ) = refs
    row = lax.axis_index("row")
    col = lax.axis_index("col")
    me = row * 4 + col
    sublane = lax.broadcasted_iota(jnp.int32, (ROWS, LANES), 0)
    lane = lax.broadcasted_iota(jnp.int32, (ROWS, LANES), 1)

    phase_copy = pltpu.make_async_copy(phase, phase_in, local_sem.at[0])
    phase_copy.start()
    own_copy = pltpu.make_async_copy(
        voltage.at[:, :, pl.ds(pl.multiple_of(me * LANES, LANES), LANES)],
        recv1.at[me],
        local_sem.at[1],
    )
    own_copy.start()
    given_copies = [
        pltpu.make_async_copy(a, b, given_sem.at[n]) for n, (a, b) in enumerate(zip(given, held))
    ]
    for copy in given_copies:
        copy.start()

    place = row // 8, (col // 2) * 2 + lax.rem(row // 4, 2), lax.rem(row, 4), lax.rem(col, 2)
    z, y, x, core = place
    barrier = pltpu.get_barrier_semaphore()

    def greet(step, carry):
        to = device_at(
            z,
            lax.rem(y + lax.rem(step, 4), 4),
            lax.rem(x + lax.rem(step // 4, 4), 4),
            lax.rem(core + step // 16, 2),
        )
        pl.semaphore_signal(barrier, inc=1, device_id=to, device_id_type=BY_MESH)
        return carry

    def greet_along(other):
        to = device_at(lax.rem(z + other, 4), y, x, core)
        return dict(inc=1, device_id=to, device_id_type=BY_MESH)

    for other in range(1, 4):
        pl.semaphore_signal(barrier, **greet_along(other))
    lax.fori_loop(1, 32, greet, 0)
    pl.semaphore_wait(barrier, 34)
    for other in range(1, 4):
        pl.semaphore_signal(plane_sem, **greet_along(other))
    pl.semaphore_wait(plane_sem, 3)

    def send_piece(step, source_of, target, send_sem, recv_sem):
        to_row, to_col = partner(place, step)
        pltpu.make_async_remote_copy(
            src_ref=source_of(to_row * 4 + to_col),
            dst_ref=target,
            send_sem=send_sem,
            recv_sem=recv_sem,
            device_id=(to_row, to_col),
            device_id_type=BY_MESH,
        ).start()

    def tile_rows(part):
        return pl.ds(pl.multiple_of(part * TILE, TILE), TILE)

    def wait_part(buffer, sem):
        ref = buffer.at[pl.ds(0, DEVICES - 1), :, pl.ds(0, TILE), :]
        pltpu.make_async_copy(ref, ref, sem).wait()

    def voltage_part(part, carry):
        def one(step, inner):
            send_piece(
                step,
                lambda to: voltage.at[
                    :, tile_rows(part), pl.ds(pl.multiple_of(to * LANES, LANES), LANES)
                ],
                recv1.at[me, :, tile_rows(part), :],
                send_sems.at[0],
                sems1.at[part],
            )
            return inner

        lax.fori_loop(1, DEVICES, one, 0)
        return carry

    lax.fori_loop(0, PARTS, voltage_part, 0)

    phase_copy.wait()

    def phase_out(b, carry):
        block = phase_in[:, pl.ds(pl.multiple_of(b * LANES, LANES), LANES)]
        phase_send[:, pl.ds(b, 1), :] = jnp.transpose(block).reshape(DEVICES, 1, LANES)
        return carry

    lax.fori_loop(0, ROWS, phase_out, 0)

    def phase_piece(step, carry):
        send_piece(
            step, lambda to: phase_send.at[to], phase_recv.at[me], send_sems.at[1], phase_sem
        )
        return carry

    lax.fori_loop(1, DEVICES, phase_piece, 0)
    phase_recv[me] = phase_send[me]

    def fill(a, carry):
        cos_part, sin_part = unit(sublane * a, 12)
        table_a[a, 0] = cos_part
        table_a[a, 1] = -sin_part
        cos_part, sin_part = unit((a + 128 * sublane) * (128 * me + lane), LOG_TOTAL)
        table_b[a, 0] = cos_part
        table_b[a, 1] = -sin_part
        return carry

    lax.fori_loop(0, DEVICES, fill, 0)

    own_copy.wait()

    def first_part(part, carry):
        wait_part(recv1, sems1.at[part])
        at = tile_rows(part)

        def load(n):
            return recv1[n, 0, at, :], recv1[n, 1, at, :]

        def finish(k, value):
            turn = table_a[k, 0, at, :], table_a[k, 1, at, :]
            value = times(value, turn)
            work[k, 0, at, :] = value[0]
            work[k, 1, at, :] = value[1]

        block_dft(load, tiles, finish, -1)
        return carry

    lax.fori_loop(0, PARTS, first_part, 0)

    for copy in given_copies:
        copy.wait()

    def row_dft(matrix, first, second):
        high, low = halves(
            jnp.concatenate([first.reshape(64, LANES), second.reshape(64, LANES)], axis=1)
        )
        return jnp.dot(
            matrix[...],
            jnp.concatenate([high, low, high], axis=0),
            preferred_element_type=F32,
        )

    def row_dfts(matrix, source, places):
        done = []
        for first, second in zip(places[::2], places[1::2]):
            both = row_dft(matrix, source[first], source[second])
            done.append((first, (both[:ROWS, :LANES], both[ROWS:, :LANES])))
            done.append((second, (both[:ROWS, LANES:], both[ROWS:, LANES:])))
        return done

    def second_step(group, carry):
        for at, value in row_dfts(rows_fwd, work, [8 * group + n for n in range(8)]):
            value = times(value, (table_b[at, 0], table_b[at, 1]))
            send2[at, 0] = value[0]
            send2[at, 1] = value[1]
        return carry

    def send_part(buffer, target, part, send_sem, recv_sem_of):
        def one(step, inner):
            send_piece(
                step,
                lambda to: buffer.at[to, :, tile_rows(part), :],
                target.at[me, :, tile_rows(part), :],
                send_sem,
                recv_sem_of(step),
            )
            return inner

        lax.fori_loop(1, DEVICES, one, 0)

    lax.fori_loop(0, DEVICES // 8, second_step, 0)
    recv2[me] = send2[me]

    def send2_part(part, carry):
        send_part(send2, recv2, part, send_sems.at[2], lambda step: sems2.at[part])
        return carry

    lax.fori_loop(0, PARTS, send2_part, 0)

    phase_all = phase_recv.at[pl.ds(0, DEVICES - 1)]
    pltpu.make_async_copy(phase_all, phase_all, phase_sem).wait()

    def phase_back(b, carry):
        block = phase_recv[:, pl.ds(b, 1), :].reshape(DEVICES, LANES)
        cos_part, sin_part = phase_unit(jnp.transpose(block))
        chirp[:, 0, pl.ds(b, 1), :] = cos_part.reshape(DEVICES, 1, LANES)
        chirp[:, 1, pl.ds(b, 1), :] = sin_part.reshape(DEVICES, 1, LANES)
        return carry

    lax.fori_loop(0, ROWS, phase_back, 0)

    def refill(h, carry):
        cos_part, sin_part = unit((me + 128 * sublane) * (128 * h + lane), LOG_TOTAL)
        table_b[h, 0] = cos_part
        table_b[h, 1] = sin_part
        return carry

    lax.fori_loop(0, DEVICES, refill, 0)

    def middle_part(part, carry):
        wait_part(recv2, sems2.at[part])
        at = tile_rows(part)

        def load(n):
            return recv2[n, 0, at, :], recv2[n, 1, at, :]

        def finish(k, value):
            turn = mid_turn[0, pl.ds(k, 1), :], mid_turn[1, pl.ds(k, 1), :]
            value = times(value, turn)
            wide[k, :, :LANES] = value[0]
            wide[k, :, LANES:] = value[1]

        block_dft(load, tiles, finish, -1)

        def lanes_step(group, inner):
            rows = pl.ds(group * 32, 32)
            high, low = halves(wide[rows].reshape(32 * TILE, 2 * LANES))
            there = jnp.dot(
                jnp.concatenate([high, low, high], axis=1),
                lanes_fwd[...],
                preferred_element_type=F32,
            )
            turn = (
                chirp[rows, 0, at, :].reshape(32 * TILE, LANES),
                chirp[rows, 1, at, :].reshape(32 * TILE, LANES),
            )
            there = times((there[:, :LANES], there[:, LANES:]), turn)
            high, low = halves(jnp.concatenate(there, axis=1))
            back = jnp.dot(
                jnp.concatenate([high, low, high], axis=1),
                lanes_inv[...],
                preferred_element_type=F32,
            )
            wide[rows] = back.reshape(32, TILE, 2 * LANES)
            return inner

        lax.fori_loop(0, 4, lanes_step, 0)

        def load_back(n):
            turn = mid_turn[0, pl.ds(n, 1), :], mid_turn[1, pl.ds(n, 1), :]
            return times_conj((wide[n, :, :LANES], wide[n, :, LANES:]), turn)

        def finish_back(k, value):
            value = times(value, (table_b[k, 0, at, :], table_b[k, 1, at, :]))
            send3[k, 0, at, :] = value[0]
            send3[k, 1, at, :] = value[1]

        block_dft(load_back, tiles, finish_back, 1)
        recv3[me, :, at, :] = send3[me, :, at, :]
        send_part(
            send3, recv3, part, send_sems.at[3], lambda step: sems3.at[GROUPS * part + step // 16]
        )
        return carry

    lax.fori_loop(0, PARTS, middle_part, 0)

    def third_step(group, half):
        places = []
        for n in range(8):
            from_row, from_col = partner(place, 16 * group + 8 * half + n, 3)
            places.append(from_row * 4 + from_col)
        for at, value in row_dfts(rows_inv, recv3, places):
            value = times_conj(value, (table_a[at, 0], table_a[at, 1]))
            work[at, 0] = value[0]
            work[at, 1] = value[1]

    def third_group(group, count):
        def wait_one(part, inner):
            ref = recv3.at[pl.ds(0, count), :, pl.ds(0, TILE), :]
            pltpu.make_async_copy(ref, ref, sems3.at[GROUPS * part + group]).wait()
            return inner

        lax.fori_loop(0, PARTS, wait_one, 0)

        def one(half, inner):
            third_step(group, half)
            return inner

        lax.fori_loop(0, 2, one, 0)

    def later_group(group, carry):
        third_group(group, 16)
        return carry

    third_group(0, 15)
    lax.fori_loop(1, GROUPS, later_group, 0)

    def fourth_part(turn, carry):
        part = PARTS - 1 - turn
        at = tile_rows(part)

        def load(n):
            return work[n, 0, at, :], work[n, 1, at, :]

        def finish(k, value):
            send4[k, 0, at, :] = value[0]
            send4[k, 1, at, :] = value[1]

        block_dft(load, tiles, finish, 1)
        recv4[me, :, at, :] = send4[me, :, at, :]
        send_part(send4, recv4, part, send_sems.at[4], lambda step: sems4.at[part])
        return carry

    lax.fori_loop(0, PARTS, fourth_part, 0)

    wait_part(recv4, sems4.at[3])

    def edge_out(j, carry):
        edge_send[j, 0:1, :] = recv4[72 + j, 0, ROWS - 1 : ROWS, :]
        edge_send[j, 1:2, :] = recv4[72 + j, 1, ROWS - 1 : ROWS, :]
        return carry

    lax.fori_loop(0, 56, edge_out, 0)
    following = lax.rem(me + 1, DEVICES)
    edge_copy = pltpu.make_async_remote_copy(
        src_ref=edge_send,
        dst_ref=edge_recv,
        send_sem=send_sems.at[5],
        recv_sem=edge_sem,
        device_id=(following // 4, lax.rem(following, 4)),
        device_id_type=BY_MESH,
    )
    edge_copy.start()
    first_row = lax.broadcasted_iota(jnp.int32, (TILE, LANES), 0) == 0
    ahead = me > 0

    def filter_half(half):
        tile_list = (2 * half + 1, 2 * half)
        tiles_out = all_tiles.at[half]

        def one_position(high, part):
            weights = [
                taps[t : t + 1, pl.ds(pl.multiple_of(high * LANES, LANES), LANES)]
                for t in range(8)
            ]
            at = slice(part * TILE, part * TILE + TILE)
            for c in range(2):
                now = [recv4[8 * m + high, c, at, :] for m in range(16)]
                old = [None] * 16
                for m in range(9, 16):
                    shifted = pltpu.roll(now[m], 1, 0)
                    if part == 0:
                        edge = edge_recv[8 * (m - 9) + high, c : c + 1, :]
                        edge = jnp.where(ahead, edge, 0.0)
                    else:
                        edge = recv4[8 * m + high, c, part * TILE - 1 : part * TILE, :]
                    old[m] = jnp.where(first_row, edge, shifted)
                for m in range(16):
                    total = weights[0] * now[m]
                    for t in range(1, 8):
                        total = total + weights[t] * (now[m - t] if m >= t else old[m - t + 16])
                    work[16 * high + m, c, at, :] = total

        for part in tile_list:
            if part == 0:
                edge_copy.wait_recv()

            def position_of(high, carry, part=part):
                one_position(high, part)
                return carry

            lax.fori_loop(0, 8, position_of, 0)

        def one_frame(m, carry):
            for part in tile_list:
                at_tile = part % 2
                at = slice(part * TILE, part * TILE + TILE)
                values = small_dft(
                    [(work[16 * high + m, 0, at, :], work[16 * high + m, 1, at, :]) for high in range(8)],
                    -1,
                )
                for a, value in enumerate(values):
                    value = times(value, (out_turn[0, a : a + 1, :], out_turn[1, a : a + 1, :]))
                    for c in range(2):
                        tiles_out[a, c, pl.ds(128 * at_tile + m, TILE, stride=16), :] = value[c]
            return carry

        lax.fori_loop(0, 16, one_frame, 0)

        if half == 0:
            return

        def one_class(a, carry):
            both = frames_dft(lanes_out, tiles_out[a, 0], tiles_out[a, 1])
            for c in range(2):
                for side in range(2):
                    gathered[side, c, pl.ds(a, 128, stride=8), :] = both[
                        c * 128 : c * 128 + 128, side * LANES : side * LANES + LANES
                    ]
            return carry

        lax.fori_loop(0, 8, one_class, 0)
        ready_copy.start()

    all_tiles = table_a.reshape(2, 8, 2, 256, LANES)
    gathered = table_b.reshape(4, 2, 1024, LANES).at[pl.ds(0, 2)]
    ready_copy = pltpu.make_async_copy(gathered, ready, out_sem.at[0])
    late_copy = pltpu.make_async_copy(all_tiles.at[0], late, out_sem.at[1])

    wait_part(recv4, sems4.at[2])
    wait_part(recv4, sems4.at[1])
    filter_half(1)
    wait_part(recv4, sems4.at[0])
    filter_half(0)

    late_copy.start()
    ready_copy.wait()
    late_copy.wait()
    edge_copy.wait_send()
    pieces = recv1.at[pl.ds(0, DEVICES - 1)]
    for at in (0, 2, 3, 4):
        pltpu.make_async_copy(pieces, pieces, send_sems.at[at]).wait()
    pltpu.make_async_copy(phase_all, phase_all, send_sems.at[1]).wait()


def last_kernel(late, ready, lanes_out, result, frames, passing, gathered, matrix, sems, more):
    frame_copies = [pltpu.make_async_copy(late.at[a], frames.at[a], sems.at[a]) for a in range(8)]
    matrix_copy = pltpu.make_async_copy(lanes_out, matrix, more.at[0])
    pass_in = pltpu.make_async_copy(ready, passing, more.at[1])

    def to_result(source, side, column, sem):
        return pltpu.make_async_copy(
            source.at[side], result.at[:, :, pl.ds(column * LANES, LANES)], sem
        )

    passed = [to_result(passing, side, 2 + side, more.at[2 + side]) for side in range(2)]
    computed = [to_result(gathered, side, side, more.at[4 + side]) for side in range(2)]
    matrix_copy.start()
    for copy in frame_copies:
        copy.start()
    pass_in.start()
    matrix_copy.wait()
    for a in range(8):
        frame_copies[a].wait()
        both = frames_dft(matrix, frames[a, 0], frames[a, 1])
        for c in range(2):
            for side in range(2):
                gathered[side, c, pl.ds(a, 128, stride=8), :] = both[
                    c * 128 : c * 128 + 128, side * LANES : side * LANES + LANES
                ]
        if a == 3:
            pass_in.wait()
            for copy in passed:
                copy.start()
    for copy in computed:
        copy.start()
    for copy in passed + computed:
        copy.wait()


def dft_parts(size, sign, scale=1.0):
    digits = np.arange(size)
    angle = sign * 2.0 * np.pi * ((digits[:, None] * digits[None, :]) % size) / size
    return scale * np.cos(angle), scale * np.sin(angle)


def bf16_halves(matrix):
    matrix = np.asarray(matrix, np.float32)
    high = matrix.astype(BF16)
    return high, (matrix - high.astype(np.float32)).astype(BF16)


def left_matrix(size, sign):
    c, s = dft_parts(size, sign)
    high, low = bf16_halves(np.block([[c, -s], [s, c]]))
    return np.concatenate([high, high, low], axis=1)


def right_matrix(size, sign, scale=1.0):
    c, s = dft_parts(size, sign, scale)
    high, low = bf16_halves(np.block([[c, s], [-s, c]]))
    return np.concatenate([high, high, low], axis=0)


def turn_table(rows, cols, whole):
    product = np.arange(rows)[:, None] * np.arange(cols)[None, :] % whole
    angle = -2.0 * np.pi * product / whole
    return np.stack([np.cos(angle), np.sin(angle)]).astype(np.float32)


def local(voltage, chirp_phase, filter_taps):
    constants = [
        left_matrix(ROWS, -1),
        left_matrix(ROWS, 1),
        right_matrix(LANES, -1),
        right_matrix(LANES, 1, 2.0**-LOG_TOTAL),
        left_matrix(LANES, -1),
        turn_table(128, LANES, 128 * LANES),
        turn_table(8, LANES, 8 * LANES),
    ]
    blocks = pltpu.VMEM((DEVICES, 2, ROWS, LANES), F32)
    phases = pltpu.VMEM((DEVICES, ROWS, LANES), F32)
    in_hbm = pl.BlockSpec(memory_space=pl.ANY)
    given = [filter_taps] + [jnp.asarray(c) for c in constants]
    late, ready = pl.pallas_call(
        kernel,
        out_shape=[
            jax.ShapeDtypeStruct((8, 2, 256, LANES), F32),
            jax.ShapeDtypeStruct((2, 2, 1024, LANES), F32),
        ],
        in_specs=[in_hbm] * (2 + len(given)),
        out_specs=[in_hbm] * 2,
        scratch_shapes=[pltpu.VMEM(c.shape, c.dtype) for c in given]
        + [blocks] * 8
        + [pltpu.VMEM((DEVICES, 4096), F32)]
        + [phases] * 2
        + [blocks] * 3
        + [
            pltpu.VMEM((DEVICES, 2, TILE, LANES), F32),
            pltpu.VMEM((DEVICES, TILE, 2 * LANES), F32),
            pltpu.VMEM((56, 2, LANES), F32),
            pltpu.VMEM((56, 2, LANES), F32),
            pltpu.SemaphoreType.DMA((2,)),
            pltpu.SemaphoreType.DMA((PARTS,)),
            pltpu.SemaphoreType.DMA((PARTS,)),
            pltpu.SemaphoreType.DMA((PARTS * GROUPS,)),
            pltpu.SemaphoreType.DMA((PARTS,)),
            pltpu.SemaphoreType.DMA,
            pltpu.SemaphoreType.DMA,
            pltpu.SemaphoreType.DMA((6,)),
            pltpu.SemaphoreType.DMA((2,)),
            pltpu.SemaphoreType.DMA((CONSTANTS,)),
            pltpu.SemaphoreType.REGULAR,
        ],
        compiler_params=pltpu.CompilerParams(
            collective_id=0, has_side_effects=True, vmem_limit_bytes=67043328
        ),
    )(voltage, chirp_phase, *given)
    return pl.pallas_call(
        last_kernel,
        out_shape=jax.ShapeDtypeStruct((2, 1024, 512), F32),
        in_specs=[in_hbm] * 3,
        out_specs=in_hbm,
        scratch_shapes=[
            pltpu.VMEM((8, 2, 256, LANES), F32),
            pltpu.VMEM((2, 2, 1024, LANES), F32),
            pltpu.VMEM((2, 2, 1024, LANES), F32),
            pltpu.VMEM((256, 768), BF16),
            pltpu.SemaphoreType.DMA((8,)),
            pltpu.SemaphoreType.DMA((6,)),
        ],
        compiler_params=pltpu.CompilerParams(vmem_limit_bytes=67043328),
    )(late, ready, given[5])


def solution(mesh):
    in_specs = (P(None, ("row", "col"), None), P(("row", "col"), None), P())
    out_specs = P(None, None, ("row", "col"))
    return jax.shard_map(local, mesh=mesh, in_specs=in_specs, out_specs=out_specs, check_vma=False)
```

```python
import math
import random

import jax
import jax.numpy as jnp
import numpy as np
from jax import lax
from jax.experimental import pallas as pl
from jax.experimental.pallas import tpu as pltpu
from jax.sharding import PartitionSpec as P

DEVICES = 128
ROWS = 32
TILE = 8
PARTS = ROWS // TILE
LANES = 128
LOG_TOTAL = 26
GROUPS = DEVICES // 16
CONSTANTS = 8
FIRST_EDGE = 72
FAR_FIRST = [
    (n % 4, (n + n // 4) % 4, (n + n // 4 + n // 16) % 4, n // 64) for n in range(1, DEVICES)
]
random.Random(1).shuffle(FAR_FIRST)
FAR_FIRST.sort(key=lambda offset: -sum(min(d, 4 - d) for d in offset[:3]))
BY_MESH = pl.DeviceIdType.MESH
F32 = jnp.float32
BF16 = jnp.bfloat16


def device_at(z, y, x, core):
    return z * 8 + lax.rem(y, 2) * 4 + x, (y // 2) * 2 + core


def partner(here, step, way=1):
    z, y, x, core = here
    low = lax.rem(step, 4)
    mid = low + lax.rem(step // 4, 4)
    high = mid + lax.rem(step // 16, 4)
    return device_at(
        lax.rem(z + way * low, 4),
        lax.rem(y + way * mid, 4),
        lax.rem(x + way * high, 4),
        lax.rem(core + step // 64, 2),
    )


def times(a, b):
    return a[0] * b[0] - a[1] * b[1], a[0] * b[1] + a[1] * b[0]


def times_conj(a, b):
    return a[0] * b[0] + a[1] * b[1], a[1] * b[0] - a[0] * b[1]


def plus(a, b):
    return a[0] + b[0], a[1] + b[1]


def minus(a, b):
    return a[0] - b[0], a[1] - b[1]


def turned(a, part, whole, sign):
    part = part % whole
    eighths = 8 * part / whole
    if eighths == 0:
        return a
    if eighths == 2:
        return (-a[1], a[0]) if sign > 0 else (a[1], -a[0])
    if eighths == 4:
        return -a[0], -a[1]
    if eighths == 6:
        return (a[1], -a[0]) if sign > 0 else (-a[1], a[0])
    angle = sign * 2.0 * math.pi * part / whole
    cos_part, sin_part = math.cos(angle), math.sin(angle)
    if eighths in (1, 3, 5, 7):
        half = math.sqrt(0.5)
        c = half if cos_part > 0 else -half
        same = (cos_part > 0) == (sin_part > 0)
        if same:
            return (a[0] - a[1]) * c, (a[0] + a[1]) * c
        return (a[0] + a[1]) * c, (a[1] - a[0]) * c
    return a[0] * cos_part - a[1] * sin_part, a[0] * sin_part + a[1] * cos_part


def small_dft(xs, sign):
    n = len(xs)
    if n == 1:
        return xs
    if n == 2:
        return [plus(xs[0], xs[1]), minus(xs[0], xs[1])]
    parts = [small_dft(xs[r::4], sign) for r in range(4)]
    out = [None] * n
    for k in range(n // 4):
        a, b, c, d = (turned(parts[r][k], r * k, n, sign) for r in range(4))
        ac, bd = plus(a, c), plus(b, d)
        ac_, bd_ = minus(a, c), turned(minus(b, d), 1, 4, sign)
        out[k] = plus(ac, bd)
        out[k + n // 4] = plus(ac_, bd_)
        out[k + n // 2] = minus(ac, bd)
        out[k + 3 * n // 4] = minus(ac_, bd_)
    return out


def block_dft(load, scratch, finish, sign):
    for low in range(8):
        values = small_dft([load(8 * high + low) for high in range(16)], sign)
        for k, value in enumerate(values):
            value = turned(value, low * k, 128, sign)
            scratch[8 * k + low, 0] = value[0]
            scratch[8 * k + low, 1] = value[1]

    def second(k, carry):
        values = small_dft(
            [(scratch[8 * k + low, 0], scratch[8 * k + low, 1]) for low in range(8)], sign
        )
        for high, value in enumerate(values):
            finish(k + 16 * high, value)
        return carry

    lax.fori_loop(0, 16, second, 0)


def quarter_sincos(angle, quarter):
    square = angle * angle
    sin_part = angle * (
        1.0 + square * (-1.0 / 6 + square * (1.0 / 120 + square * (-1.0 / 5040 + square / 362880)))
    )
    cos_part = 1.0 + square * (
        -0.5 + square * (1.0 / 24 + square * (-1.0 / 720 + square * (1.0 / 40320)))
    )
    odd = (quarter & 1) == 1
    first = jnp.where(odd, sin_part, cos_part)
    second = jnp.where(odd, cos_part, sin_part)
    return (
        jnp.where(((quarter + 1) & 2) == 2, -first, first),
        jnp.where((quarter & 2) == 2, -second, second),
    )


def unit(product, log_whole):
    quarter = (product + (1 << (log_whole - 3))) >> (log_whole - 2)
    rest = product - (quarter << (log_whole - 2))
    return quarter_sincos(rest.astype(F32) * (2.0 * math.pi / 2**log_whole), quarter)


def phase_unit(phase):
    quarter = jnp.floor(phase * (2.0 / math.pi) + 0.5)
    high = float(np.float32(1.5703125))
    angle = (phase - quarter * high) - quarter * (math.pi / 2 - high)
    return quarter_sincos(angle, quarter.astype(jnp.int32))


def halves(x):
    high = x.astype(BF16)
    return high, (x - high.astype(F32)).astype(BF16)


def frames_dft(matrix, real_part, imag_part):
    high, low = halves(jnp.concatenate([real_part, imag_part], axis=1))
    return lax.dot_general(
        matrix[...],
        jnp.concatenate([high, low, high], axis=1),
        (((1,), (1,)), ((), ())),
        preferred_element_type=F32,
    )


def kernel(
    voltage,
    phase,
    *refs,
):
    given, refs = refs[:CONSTANTS], refs[CONSTANTS:]
    late, ready, refs = refs[0], refs[1], refs[2:]
    held, refs = refs[:CONSTANTS], refs[CONSTANTS:]
    taps, rows_fwd, rows_inv, lanes_fwd, lanes_inv, lanes_out, mid_turn, out_turn = held
    (
    recv1,
    work,
    send2,
    recv2,
    send3,
    recv3,
    send4,
    recv4,
    phase_in,
    phase_send,
    phase_recv,
    chirp,
    table_a,
    table_b,
    tiles,
    wide,
    edge_send,
    edge_recv,
    span_send,
    span_recv,
    local_sem,
    sems1,
    sems2,
    sems3,
    sems4,
    phase_sem,
    edge_sem,
    span_sem,
    send_sems,
    out_sem,
    given_sem,
    plane_sem,
    ) = refs
    row = lax.axis_index("row")
    col = lax.axis_index("col")
    me = row * 4 + col
    sublane = lax.broadcasted_iota(jnp.int32, (ROWS, LANES), 0)
    lane = lax.broadcasted_iota(jnp.int32, (ROWS, LANES), 1)

    phase_copy = pltpu.make_async_copy(phase, phase_in, local_sem.at[0])
    phase_copy.start()
    own_copy = pltpu.make_async_copy(
        voltage.at[:, :, pl.ds(pl.multiple_of(me * LANES, LANES), LANES)],
        recv1.at[me],
        local_sem.at[1],
    )
    own_copy.start()
    given_copies = [
        pltpu.make_async_copy(a, b, given_sem.at[n]) for n, (a, b) in enumerate(zip(given, held))
    ]
    for copy in given_copies:
        copy.start()

    place = row // 8, (col // 2) * 2 + lax.rem(row // 4, 2), lax.rem(row, 4), lax.rem(col, 2)
    z, y, x, core = place
    barrier = pltpu.get_barrier_semaphore()

    def greet(step, carry):
        to = device_at(
            z,
            lax.rem(y + lax.rem(step, 4), 4),
            lax.rem(x + lax.rem(step // 4, 4), 4),
            lax.rem(core + step // 16, 2),
        )
        pl.semaphore_signal(barrier, inc=1, device_id=to, device_id_type=BY_MESH)
        return carry

    def greet_along(other):
        to = device_at(lax.rem(z + other, 4), y, x, core)
        return dict(inc=1, device_id=to, device_id_type=BY_MESH)

    for other in range(1, 4):
        pl.semaphore_signal(barrier, **greet_along(other))
    lax.fori_loop(1, 32, greet, 0)
    pl.semaphore_wait(barrier, 34)
    for other in range(1, 4):
        pl.semaphore_signal(plane_sem, **greet_along(other))
    pl.semaphore_wait(plane_sem, 3)

    def send_piece(step, source_of, target, send_sem, recv_sem):
        to_row, to_col = partner(place, step)
        pltpu.make_async_remote_copy(
            src_ref=source_of(to_row * 4 + to_col),
            dst_ref=target,
            send_sem=send_sem,
            recv_sem=recv_sem,
            device_id=(to_row, to_col),
            device_id_type=BY_MESH,
        ).start()

    def tile_rows(part):
        return pl.ds(pl.multiple_of(part * TILE, TILE), TILE)

    def wait_part(buffer, sem):
        ref = buffer.at[pl.ds(0, DEVICES - 1), :, pl.ds(0, TILE), :]
        pltpu.make_async_copy(ref, ref, sem).wait()

    def voltage_part(part, carry):
        def one(step, inner):
            send_piece(
                step,
                lambda to: voltage.at[
                    :, tile_rows(part), pl.ds(pl.multiple_of(to * LANES, LANES), LANES)
                ],
                recv1.at[me, :, tile_rows(part), :],
                send_sems.at[0],
                sems1.at[part],
            )
            return inner

        lax.fori_loop(1, DEVICES, one, 0)
        return carry

    lax.fori_loop(0, PARTS, voltage_part, 0)

    phase_copy.wait()

    def phase_out(b, carry):
        block = phase_in[:, pl.ds(pl.multiple_of(b * LANES, LANES), LANES)]
        phase_send[:, pl.ds(b, 1), :] = jnp.transpose(block).reshape(DEVICES, 1, LANES)
        return carry

    lax.fori_loop(0, ROWS, phase_out, 0)

    def phase_piece(step, carry):
        send_piece(
            step, lambda to: phase_send.at[to], phase_recv.at[me], send_sems.at[1], phase_sem
        )
        return carry

    lax.fori_loop(1, DEVICES, phase_piece, 0)
    phase_recv[me] = phase_send[me]

    def fill(a, carry):
        cos_part, sin_part = unit(sublane * a, 12)
        table_a[a, 0] = cos_part
        table_a[a, 1] = -sin_part
        cos_part, sin_part = unit((a + 128 * sublane) * (128 * me + lane), LOG_TOTAL)
        table_b[a, 0] = cos_part
        table_b[a, 1] = -sin_part
        return carry

    lax.fori_loop(0, DEVICES, fill, 0)

    own_copy.wait()

    def first_part(part, carry):
        wait_part(recv1, sems1.at[part])
        at = tile_rows(part)

        def load(n):
            return recv1[n, 0, at, :], recv1[n, 1, at, :]

        def finish(k, value):
            turn = table_a[k, 0, at, :], table_a[k, 1, at, :]
            value = times(value, turn)
            work[k, 0, at, :] = value[0]
            work[k, 1, at, :] = value[1]

        block_dft(load, tiles, finish, -1)
        return carry

    lax.fori_loop(0, PARTS, first_part, 0)

    for copy in given_copies:
        copy.wait()

    def row_dft(matrix, first, second):
        high, low = halves(
            jnp.concatenate([first.reshape(64, LANES), second.reshape(64, LANES)], axis=1)
        )
        return jnp.dot(
            matrix[...],
            jnp.concatenate([high, low, high], axis=0),
            preferred_element_type=F32,
        )

    def row_dfts(matrix, source, places):
        done = []
        for first, second in zip(places[::2], places[1::2]):
            both = row_dft(matrix, source[first], source[second])
            done.append((first, (both[:ROWS, :LANES], both[ROWS:, :LANES])))
            done.append((second, (both[:ROWS, LANES:], both[ROWS:, LANES:])))
        return done

    def second_step(group, carry):
        for at, value in row_dfts(rows_fwd, work, [8 * group + n for n in range(8)]):
            value = times(value, (table_b[at, 0], table_b[at, 1]))
            send2[at, 0] = value[0]
            send2[at, 1] = value[1]
        return carry

    def send_part(buffer, target, part, send_sem, recv_sem_of):
        def one(step, inner):
            send_piece(
                step,
                lambda to: buffer.at[to, :, tile_rows(part), :],
                target.at[me, :, tile_rows(part), :],
                send_sem,
                recv_sem_of(step),
            )
            return inner

        lax.fori_loop(1, DEVICES, one, 0)

    lax.fori_loop(0, DEVICES // 8, second_step, 0)
    recv2[me] = send2[me]

    def send2_part(part, carry):
        send_part(send2, recv2, part, send_sems.at[2], lambda step: sems2.at[part])
        return carry

    lax.fori_loop(0, PARTS, send2_part, 0)

    phase_all = phase_recv.at[pl.ds(0, DEVICES - 1)]
    pltpu.make_async_copy(phase_all, phase_all, phase_sem).wait()

    def phase_back(b, carry):
        block = phase_recv[:, pl.ds(b, 1), :].reshape(DEVICES, LANES)
        cos_part, sin_part = phase_unit(jnp.transpose(block))
        chirp[:, 0, pl.ds(b, 1), :] = cos_part.reshape(DEVICES, 1, LANES)
        chirp[:, 1, pl.ds(b, 1), :] = sin_part.reshape(DEVICES, 1, LANES)
        return carry

    lax.fori_loop(0, ROWS, phase_back, 0)

    def refill(h, carry):
        cos_part, sin_part = unit((me + 128 * sublane) * (128 * h + lane), LOG_TOTAL)
        table_b[h, 0] = cos_part
        table_b[h, 1] = sin_part
        return carry

    lax.fori_loop(0, DEVICES, refill, 0)

    def middle_part(part, carry):
        wait_part(recv2, sems2.at[part])
        at = tile_rows(part)

        def load(n):
            return recv2[n, 0, at, :], recv2[n, 1, at, :]

        def finish(k, value):
            turn = mid_turn[0, pl.ds(k, 1), :], mid_turn[1, pl.ds(k, 1), :]
            value = times(value, turn)
            wide[k, :, :LANES] = value[0]
            wide[k, :, LANES:] = value[1]

        block_dft(load, tiles, finish, -1)

        def lanes_step(group, inner):
            rows = pl.ds(group * 32, 32)
            high, low = halves(wide[rows].reshape(32 * TILE, 2 * LANES))
            there = jnp.dot(
                jnp.concatenate([high, low, high], axis=1),
                lanes_fwd[...],
                preferred_element_type=F32,
            )
            turn = (
                chirp[rows, 0, at, :].reshape(32 * TILE, LANES),
                chirp[rows, 1, at, :].reshape(32 * TILE, LANES),
            )
            there = times((there[:, :LANES], there[:, LANES:]), turn)
            high, low = halves(jnp.concatenate(there, axis=1))
            back = jnp.dot(
                jnp.concatenate([high, low, high], axis=1),
                lanes_inv[...],
                preferred_element_type=F32,
            )
            wide[rows] = back.reshape(32, TILE, 2 * LANES)
            return inner

        lax.fori_loop(0, 4, lanes_step, 0)

        def load_back(n):
            turn = mid_turn[0, pl.ds(n, 1), :], mid_turn[1, pl.ds(n, 1), :]
            return times_conj((wide[n, :, :LANES], wide[n, :, LANES:]), turn)

        def finish_back(k, value):
            value = times(value, (table_b[k, 0, at, :], table_b[k, 1, at, :]))
            send3[k, 0, at, :] = value[0]
            send3[k, 1, at, :] = value[1]

        block_dft(load_back, tiles, finish_back, 1)
        recv3[me, :, at, :] = send3[me, :, at, :]
        send_part(
            send3, recv3, part, send_sems.at[3], lambda step: sems3.at[GROUPS * part + step // 16]
        )
        return carry

    lax.fori_loop(0, PARTS, middle_part, 0)

    def third_step(group, half):
        places = []
        for n in range(8):
            from_row, from_col = partner(place, 16 * group + 8 * half + n, 3)
            places.append(from_row * 4 + from_col)
        for at, value in row_dfts(rows_inv, recv3, places):
            value = times_conj(value, (table_a[at, 0], table_a[at, 1]))
            work[at, 0] = value[0]
            work[at, 1] = value[1]

    def third_group(group, count):
        def wait_one(part, inner):
            ref = recv3.at[pl.ds(0, count), :, pl.ds(0, TILE), :]
            pltpu.make_async_copy(ref, ref, sems3.at[GROUPS * part + group]).wait()
            return inner

        lax.fori_loop(0, PARTS, wait_one, 0)

        def one(half, inner):
            third_step(group, half)
            return inner

        lax.fori_loop(0, 2, one, 0)

    def later_group(group, carry):
        third_group(group, 16)
        return carry

    third_group(0, 15)
    lax.fori_loop(1, GROUPS, later_group, 0)

    def fourth_part(part):
        at = slice(part * TILE, part * TILE + TILE)

        def load(n):
            return work[n, 0, at, :], work[n, 1, at, :]

        def finish(k, value):
            for c in range(2):
                send4[k, c, at, :] = value[c]
                if part == 0:
                    edge_send[k, c : c + 1, :] = value[c][TILE - 1 :]

        block_dft(load, tiles, finish, 1)
        recv4[me, :, at, :] = send4[me, :, at, :]

    rows_of = [
        [lax.rem(z + n, 4) * 8 for n in range(4)],
        [lax.rem(y + n, 2) * 4 for n in range(4)],
        [lax.rem(x + n, 4) for n in range(4)],
    ]
    cols_of = [
        [lax.rem(y + n, 4) // 2 * 2 for n in range(4)],
        [lax.rem(core + n, 2) for n in range(2)],
    ]

    def send4_part(part):
        at = slice(part * TILE, part * TILE + TILE)
        for dz, dy, dx, dc in FAR_FIRST:
            to_row = rows_of[0][dz] + rows_of[1][dy] + rows_of[2][dx]
            to_col = cols_of[0][dy] + cols_of[1][dc]
            pltpu.make_async_remote_copy(
                src_ref=send4.at[to_row * 4 + to_col, :, at, :],
                dst_ref=recv4.at[me, :, at, :],
                send_sem=send_sems.at[4],
                recv_sem=sems4.at[part],
                device_id=(to_row, to_col),
                device_id_type=BY_MESH,
            ).start()

    def edge_pieces():
        for dz, dy, dx, dc in FAR_FIRST:
            to_row = rows_of[0][dz] + rows_of[1][dy] + rows_of[2][dx]
            to_col = cols_of[0][dy] + cols_of[1][dc]
            pltpu.make_async_remote_copy(
                src_ref=edge_send.at[to_row * 4 + to_col],
                dst_ref=edge_recv.at[me],
                send_sem=send_sems.at[5],
                recv_sem=edge_sem,
                device_id=(to_row, to_col),
                device_id_type=BY_MESH,
            ).start()

    with_edges = me >= FIRST_EDGE
    fourth_part(3)
    send4_part(3)
    fourth_part(2)
    send4_part(2)
    fourth_part(1)
    fourth_part(0)
    pl.when(with_edges)(edge_pieces)
    edge_recv[me] = edge_send[me]
    send4_part(1)
    wait_part(recv4, sems4.at[3])

    def span_edge(j, carry):
        span_send[j, 0:1, :] = recv4[FIRST_EDGE + j, 0, ROWS - 1 :, :]
        span_send[j, 1:2, :] = recv4[FIRST_EDGE + j, 1, ROWS - 1 :, :]
        return carry

    lax.fori_loop(0, DEVICES - FIRST_EDGE, span_edge, 0)
    following = lax.rem(me + 1, DEVICES)
    span_copy = pltpu.make_async_remote_copy(
        src_ref=span_send,
        dst_ref=span_recv,
        send_sem=send_sems.at[6],
        recv_sem=span_sem,
        device_id=(following // 4, lax.rem(following, 4)),
        device_id_type=BY_MESH,
    )
    span_copy.start()
    send4_part(0)

    first_row = lax.broadcasted_iota(jnp.int32, (TILE, LANES), 0) == 0
    ahead = me > 0
    frames = table_a.reshape(PARTS, 8, 2, 128, LANES)
    gathered = table_b.reshape(PARTS, 2, 1024, LANES)

    def filter_part(part):
        at = slice(part * TILE, part * TILE + TILE)

        def edge_row(high, m, c):
            if part == 0:
                edge = span_recv[8 * m + high - FIRST_EDGE, c : c + 1, :]
                return jnp.where(ahead, edge, 0.0)
            if part == 1:
                return edge_recv[8 * m + high, c : c + 1, :]
            return recv4[8 * m + high, c, part * TILE - 1 : part * TILE, :]

        def one_position(high, carry):
            weights = [
                taps[t : t + 1, pl.ds(pl.multiple_of(high * LANES, LANES), LANES)]
                for t in range(8)
            ]
            for c in range(2):
                now = [recv4[8 * m + high, c, at, :] for m in range(16)]
                old = [None] * 16
                for m in range(9, 16):
                    old[m] = jnp.where(first_row, edge_row(high, m, c), pltpu.roll(now[m], 1, 0))
                for m in range(16):
                    total = weights[0] * now[m]
                    for t in range(1, 8):
                        total = total + weights[t] * (now[m - t] if m >= t else old[m - t + 16])
                    work[16 * high + m, c, at, :] = total
            return carry

        lax.fori_loop(0, 8, one_position, 0)

        def one_frame(m, carry):
            values = small_dft(
                [(work[16 * high + m, 0, at, :], work[16 * high + m, 1, at, :]) for high in range(8)],
                -1,
            )
            for a, value in enumerate(values):
                value = times(value, (out_turn[0, a : a + 1, :], out_turn[1, a : a + 1, :]))
                for c in range(2):
                    frames[part, a, c, pl.ds(m, TILE, stride=16), :] = value[c]
            return carry

        lax.fori_loop(0, 16, one_frame, 0)

    def ready_copy(part):
        return pltpu.make_async_copy(gathered.at[part], ready.at[part - 1], out_sem.at[part])

    def finish_parts(parts):
        classes = 2 // len(parts)

        def some_classes(step, carry):
            each = [(p, classes * step + n) for n in range(classes) for p in parts]
            both = frames_dft(
                lanes_out, *[jnp.concatenate([frames[p, a, c] for p, a in each]) for c in range(2)]
            )
            for c in range(2):
                for n, (p, a) in enumerate(each):
                    gathered[p, c, pl.ds(a, 128, stride=8), :] = both[
                        c * 128 : c * 128 + 128, n * LANES : n * LANES + LANES
                    ]
            return carry

        lax.fori_loop(0, 8 // classes, some_classes, 0)
        for p in parts:
            ready_copy(p).start()

    wait_part(recv4, sems4.at[2])
    filter_part(3)
    wait_part(recv4, sems4.at[1])
    filter_part(2)
    finish_parts((2, 3))

    def wait_edges(count):
        ref = edge_recv.at[pl.ds(0, count)]
        pltpu.make_async_copy(ref, ref, edge_sem).wait()

    pl.when(with_edges)(lambda: wait_edges(DEVICES - FIRST_EDGE - 1))
    pl.when(jnp.logical_not(with_edges))(lambda: wait_edges(DEVICES - FIRST_EDGE))
    filter_part(1)
    finish_parts((1,))
    wait_part(recv4, sems4.at[0])
    span_copy.wait_recv()
    filter_part(0)
    late_copy = pltpu.make_async_copy(frames.at[0], late, out_sem.at[0])
    late_copy.start()
    for part in range(1, PARTS):
        ready_copy(part).wait()
    late_copy.wait()
    span_copy.wait_send()

    def wait_edges_sent():
        ref = edge_recv.at[pl.ds(0, DEVICES - 1)]
        pltpu.make_async_copy(ref, ref, send_sems.at[5]).wait()

    pl.when(with_edges)(wait_edges_sent)
    pieces = recv1.at[pl.ds(0, DEVICES - 1)]
    for at in (0, 2, 3, 4):
        pltpu.make_async_copy(pieces, pieces, send_sems.at[at]).wait()
    pltpu.make_async_copy(phase_all, phase_all, send_sems.at[1]).wait()


def last_kernel(late, ready, lanes_out, result, frames, passing, gathered, matrix, sems, more):
    frame_copies = [pltpu.make_async_copy(late.at[a], frames.at[a], sems.at[a]) for a in range(8)]
    matrix_copy = pltpu.make_async_copy(lanes_out, matrix, more.at[0])
    pass_in = [
        pltpu.make_async_copy(ready.at[n], passing.at[n], more.at[1 + n]) for n in range(3)
    ]

    def to_result(source, column, sem):
        return pltpu.make_async_copy(source, result.at[:, :, pl.ds(column * LANES, LANES)], sem)

    passed = [to_result(passing.at[n], 1 + n, more.at[4 + n]) for n in range(3)]
    computed = to_result(gathered, 0, more.at[7])
    matrix_copy.start()
    for copy in frame_copies + pass_in:
        copy.start()
    matrix_copy.wait()
    for a in range(0, 8, 2):
        frame_copies[a].wait()
        frame_copies[a + 1].wait()
        both = frames_dft(
            matrix, *[jnp.concatenate([frames[a, c], frames[a + 1, c]]) for c in range(2)]
        )
        for c in range(2):
            for n in range(2):
                gathered[c, pl.ds(a + n, 128, stride=8), :] = both[
                    c * 128 : c * 128 + 128, n * LANES : n * LANES + LANES
                ]
        if a < 6:
            pass_in[a // 2].wait()
            passed[a // 2].start()
    computed.start()
    for copy in passed + [computed]:
        copy.wait()


def dft_parts(size, sign, scale=1.0):
    digits = np.arange(size)
    angle = sign * 2.0 * np.pi * ((digits[:, None] * digits[None, :]) % size) / size
    return scale * np.cos(angle), scale * np.sin(angle)


def bf16_halves(matrix):
    matrix = np.asarray(matrix, np.float32)
    high = matrix.astype(BF16)
    return high, (matrix - high.astype(np.float32)).astype(BF16)


def left_matrix(size, sign):
    c, s = dft_parts(size, sign)
    high, low = bf16_halves(np.block([[c, -s], [s, c]]))
    return np.concatenate([high, high, low], axis=1)


def right_matrix(size, sign, scale=1.0):
    c, s = dft_parts(size, sign, scale)
    high, low = bf16_halves(np.block([[c, s], [-s, c]]))
    return np.concatenate([high, high, low], axis=0)


def turn_table(rows, cols, whole):
    product = np.arange(rows)[:, None] * np.arange(cols)[None, :] % whole
    angle = -2.0 * np.pi * product / whole
    return np.stack([np.cos(angle), np.sin(angle)]).astype(np.float32)


def local(voltage, chirp_phase, filter_taps):
    constants = [
        left_matrix(ROWS, -1),
        left_matrix(ROWS, 1),
        right_matrix(LANES, -1),
        right_matrix(LANES, 1, 2.0**-LOG_TOTAL),
        left_matrix(LANES, -1),
        turn_table(128, LANES, 128 * LANES),
        turn_table(8, LANES, 8 * LANES),
    ]
    blocks = pltpu.VMEM((DEVICES, 2, ROWS, LANES), F32)
    phases = pltpu.VMEM((DEVICES, ROWS, LANES), F32)
    in_hbm = pl.BlockSpec(memory_space=pl.ANY)
    given = [filter_taps] + [jnp.asarray(c) for c in constants]
    late, ready = pl.pallas_call(
        kernel,
        out_shape=[
            jax.ShapeDtypeStruct((8, 2, 128, LANES), F32),
            jax.ShapeDtypeStruct((3, 2, 1024, LANES), F32),
        ],
        in_specs=[in_hbm] * (2 + len(given)),
        out_specs=[in_hbm] * 2,
        scratch_shapes=[pltpu.VMEM(c.shape, c.dtype) for c in given]
        + [blocks] * 8
        + [pltpu.VMEM((DEVICES, 4096), F32)]
        + [phases] * 2
        + [blocks] * 3
        + [
            pltpu.VMEM((DEVICES, 2, TILE, LANES), F32),
            pltpu.VMEM((DEVICES, TILE, 2 * LANES), F32),
            pltpu.VMEM((DEVICES, 2, LANES), F32),
            pltpu.VMEM((DEVICES, 2, LANES), F32),
            pltpu.VMEM((DEVICES - FIRST_EDGE, 2, LANES), F32),
            pltpu.VMEM((DEVICES - FIRST_EDGE, 2, LANES), F32),
            pltpu.SemaphoreType.DMA((2,)),
            pltpu.SemaphoreType.DMA((PARTS,)),
            pltpu.SemaphoreType.DMA((PARTS,)),
            pltpu.SemaphoreType.DMA((PARTS * GROUPS,)),
            pltpu.SemaphoreType.DMA((PARTS,)),
            pltpu.SemaphoreType.DMA,
            pltpu.SemaphoreType.DMA,
            pltpu.SemaphoreType.DMA,
            pltpu.SemaphoreType.DMA((7,)),
            pltpu.SemaphoreType.DMA((PARTS,)),
            pltpu.SemaphoreType.DMA((CONSTANTS,)),
            pltpu.SemaphoreType.REGULAR,
        ],
        compiler_params=pltpu.CompilerParams(
            collective_id=0, has_side_effects=True, vmem_limit_bytes=67043328
        ),
    )(voltage, chirp_phase, *given)
    return pl.pallas_call(
        last_kernel,
        out_shape=jax.ShapeDtypeStruct((2, 1024, 512), F32),
        in_specs=[in_hbm] * 3,
        out_specs=in_hbm,
        scratch_shapes=[
            pltpu.VMEM((8, 2, 128, LANES), F32),
            pltpu.VMEM((3, 2, 1024, LANES), F32),
            pltpu.VMEM((2, 1024, LANES), F32),
            pltpu.VMEM((256, 768), BF16),
            pltpu.SemaphoreType.DMA((8,)),
            pltpu.SemaphoreType.DMA((8,)),
        ],
        compiler_params=pltpu.CompilerParams(vmem_limit_bytes=67043328),
    )(late, ready, given[5])


def solution(mesh):
    in_specs = (P(None, ("row", "col"), None), P(("row", "col"), None), P())
    out_specs = P(None, None, ("row", "col"))
    return jax.shard_map(local, mesh=mesh, in_specs=in_specs, out_specs=out_specs, check_vma=False)
```

```python
import math
import random

import jax
import jax.numpy as jnp
import numpy as np
from jax import lax
from jax.experimental import pallas as pl
from jax.experimental.pallas import tpu as pltpu
from jax.sharding import PartitionSpec as P

DEVICES = 128
ROWS = 32
TILE = 8
PARTS = ROWS // TILE
LANES = 128
HALF = LANES // 2
LOG_TOTAL = 26
GROUPS = DEVICES // 16
CONSTANTS = 9
FIRST_EDGE = 72
IN_STEPS = [
    (n % 4, (n % 4 + n // 4) % 4, (n % 4 + n // 4 + n // 16) % 4, n // 64)
    for n in range(1, DEVICES)
]
FAR_FIRST = list(IN_STEPS)
random.Random(1).shuffle(FAR_FIRST)
FAR_FIRST.sort(key=lambda offset: -sum(min(d, 4 - d) for d in offset[:3]))
BY_MESH = pl.DeviceIdType.MESH
F32 = jnp.float32
BF16 = jnp.bfloat16


def device_at(z, y, x, core):
    return z * 8 + lax.rem(y, 2) * 4 + x, (y // 2) * 2 + core


def partner(here, step, way=1):
    z, y, x, core = here
    low = lax.rem(step, 4)
    mid = low + lax.rem(step // 4, 4)
    high = mid + lax.rem(step // 16, 4)
    return device_at(
        lax.rem(z + way * low, 4),
        lax.rem(y + way * mid, 4),
        lax.rem(x + way * high, 4),
        lax.rem(core + step // 64, 2),
    )


def times(a, b):
    return a[0] * b[0] - a[1] * b[1], a[0] * b[1] + a[1] * b[0]


def plus(a, b):
    return tuple(x + y for x, y in zip(a, b))


def minus(a, b):
    return tuple(x - y for x, y in zip(a, b))


def turned(a, part, whole, sign):
    part = part % whole
    eighths = 8 * part / whole
    if eighths == 0:
        return a
    if eighths == 2:
        return (-a[1], a[0]) if sign > 0 else (a[1], -a[0])
    if eighths == 4:
        return -a[0], -a[1]
    if eighths == 6:
        return (a[1], -a[0]) if sign > 0 else (-a[1], a[0])
    angle = sign * 2.0 * math.pi * part / whole
    cos_part, sin_part = math.cos(angle), math.sin(angle)
    if eighths in (1, 3, 5, 7):
        half = math.sqrt(0.5)
        c = half if cos_part > 0 else -half
        same = (cos_part > 0) == (sin_part > 0)
        if same:
            return (a[0] - a[1]) * c, (a[0] + a[1]) * c
        return (a[0] + a[1]) * c, (a[1] - a[0]) * c
    return a[0] * cos_part - a[1] * sin_part, a[0] * sin_part + a[1] * cos_part


def lane_sign(shape):
    return jnp.where(lax.broadcasted_iota(jnp.int32, shape, len(shape) - 1) < HALF, -1.0, 1.0)


def swapped(x):
    return pltpu.roll(x, HALF, x.ndim - 1)


def packed_times(x, turn):
    return x * turn[0] + swapped(x) * turn[1]


def packed_turned(a, part, whole, sign):
    part = part % whole
    angle = sign * 2.0 * math.pi * part / whole
    (x,) = a
    if part == 0:
        return a
    if 2 * part == whole:
        return (-x,)
    if 4 * part in (whole, 3 * whole):
        up = (4 * part == whole) == (sign > 0)
        return (swapped(x) * (lane_sign(x.shape) if up else -lane_sign(x.shape)),)
    return (math.cos(angle) * x + swapped(x) * (math.sin(angle) * lane_sign(x.shape)),)


def small_dft(xs, sign):
    n = len(xs)
    turn = turned if len(xs[0]) == 2 else packed_turned
    if n == 1:
        return xs
    if n == 2:
        return [plus(xs[0], xs[1]), minus(xs[0], xs[1])]
    parts = [small_dft(xs[r::4], sign) for r in range(4)]
    out = [None] * n
    for k in range(n // 4):
        a, b, c, d = (turn(parts[r][k], r * k, n, sign) for r in range(4))
        ac, bd = plus(a, c), plus(b, d)
        ac_, bd_ = minus(a, c), turn(minus(b, d), 1, 4, sign)
        out[k] = plus(ac, bd)
        out[k + n // 4] = plus(ac_, bd_)
        out[k + n // 2] = minus(ac, bd)
        out[k + 3 * n // 4] = minus(ac_, bd_)
    return out


def block_dft(load, scratch, finish, sign):
    for low in range(8):
        values = small_dft([load(8 * high + low) for high in range(16)], sign)
        for k, value in enumerate(values):
            turn = turned if len(value) == 2 else packed_turned
            value = turn(value, low * k, 128, sign)
            for c, x in enumerate(value):
                scratch[8 * k + low, c] = x
    parts = range(len(value))
    together = 1 if len(value) == 2 else 4

    def second(step, carry):
        ks = [together * step + n for n in range(together)]
        given = [
            [tuple(scratch[8 * k + low, c] for c in parts) for low in range(8)] for k in ks
        ]
        done = [small_dft(values, sign) for values in given]
        for k, values in zip(ks, done):
            for high, value in enumerate(values):
                finish(k + 16 * high, value)
        return carry

    lax.fori_loop(0, 16 // together, second, 0)


def quarter_sincos(angle, quarter):
    square = angle * angle
    sin_part = angle * (
        1.0 + square * (-1.0 / 6 + square * (1.0 / 120 + square * (-1.0 / 5040 + square / 362880)))
    )
    cos_part = 1.0 + square * (
        -0.5 + square * (1.0 / 24 + square * (-1.0 / 720 + square * (1.0 / 40320)))
    )
    odd = (quarter & 1) == 1
    first = jnp.where(odd, sin_part, cos_part)
    second = jnp.where(odd, cos_part, sin_part)
    return (
        jnp.where(((quarter + 1) & 2) == 2, -first, first),
        jnp.where((quarter & 2) == 2, -second, second),
    )


def unit(product, log_whole):
    quarter = (product + (1 << (log_whole - 3))) >> (log_whole - 2)
    rest = product - (quarter << (log_whole - 2))
    return quarter_sincos(rest.astype(F32) * (2.0 * math.pi / 2**log_whole), quarter)


def phase_unit(phase):
    quarter = jnp.floor(phase * (2.0 / math.pi) + 0.5)
    high = float(np.float32(1.5703125))
    angle = (phase - quarter * high) - quarter * (math.pi / 2 - high)
    return quarter_sincos(angle, quarter.astype(jnp.int32))


def halves(x):
    high = x.astype(BF16)
    return high, (x - high.astype(F32)).astype(BF16)


def frames_dft(matrix, real_part, imag_part):
    high, low = halves(jnp.concatenate([real_part, imag_part], axis=1))
    return lax.dot_general(
        matrix[...],
        jnp.concatenate([high, low, high], axis=1),
        (((1,), (1,)), ((), ())),
        preferred_element_type=F32,
    )


def kernel(
    voltage,
    phase,
    *refs,
):
    given, refs = refs[:CONSTANTS], refs[CONSTANTS:]
    late, ready, refs = refs[0], refs[1], refs[2:]
    held, refs = refs[:CONSTANTS], refs[CONSTANTS:]
    taps, rows_fwd, rows_inv, lanes_fwd, lanes_inv, lanes_out, mid_turn, mid_back, out_turn = held
    (
    recv1,
    work,
    send2,
    recv2,
    send3,
    recv3,
    send4,
    recv4,
    phase_in,
    phase_send,
    phase_recv,
    chirp,
    table_a,
    table_b,
    tiles,
    wide,
    edge_send,
    edge_recv,
    span_send,
    span_recv,
    half_taps,
    local_sem,
    sems1,
    sems2,
    sems3,
    sems4,
    phase_sem,
    edge_sem,
    span_sems,
    send_sems,
    out_sem,
    given_sem,
    plane_sem,
    ) = refs
    row = lax.axis_index("row")
    col = lax.axis_index("col")
    me = row * 4 + col
    sublane = lax.broadcasted_iota(jnp.int32, (ROWS, LANES), 0)
    lane = lax.broadcasted_iota(jnp.int32, (ROWS, LANES), 1)

    phase_copy = pltpu.make_async_copy(phase, phase_in, local_sem.at[0])
    phase_copy.start()
    own_copy = pltpu.make_async_copy(
        voltage.at[:, :, pl.ds(pl.multiple_of(me * LANES, LANES), LANES)],
        recv1.at[me],
        local_sem.at[1],
    )
    own_copy.start()
    given_copies = [
        pltpu.make_async_copy(a, b, given_sem.at[n]) for n, (a, b) in enumerate(zip(given, held))
    ]
    for copy in given_copies:
        copy.start()

    place = row // 8, (col // 2) * 2 + lax.rem(row // 4, 2), lax.rem(row, 4), lax.rem(col, 2)
    z, y, x, core = place
    barrier = pltpu.get_barrier_semaphore()

    def greet(step, carry):
        to = device_at(
            z,
            lax.rem(y + lax.rem(step, 4), 4),
            lax.rem(x + lax.rem(step // 4, 4), 4),
            lax.rem(core + step // 16, 2),
        )
        pl.semaphore_signal(barrier, inc=1, device_id=to, device_id_type=BY_MESH)
        return carry

    def greet_along(other):
        to = device_at(lax.rem(z + other, 4), y, x, core)
        return dict(inc=1, device_id=to, device_id_type=BY_MESH)

    for other in range(1, 4):
        pl.semaphore_signal(barrier, **greet_along(other))
    lax.fori_loop(1, 32, greet, 0)
    pl.semaphore_wait(barrier, 34)
    for other in range(1, 4):
        pl.semaphore_signal(plane_sem, **greet_along(other))
    pl.semaphore_wait(plane_sem, 3)

    rows_of = [
        [lax.rem(z + n, 4) * 8 for n in range(4)],
        [lax.rem(y + n, 2) * 4 for n in range(4)],
        [lax.rem(x + n, 4) for n in range(4)],
    ]
    cols_of = [
        [lax.rem(y + n, 4) // 2 * 2 for n in range(4)],
        [lax.rem(core + n, 2) for n in range(2)],
    ]

    def send_loop(source_of, target, send_sem, recv_sem):
        def one(step, carry):
            to_row, to_col = partner(place, step)
            pltpu.make_async_remote_copy(
                src_ref=source_of(to_row * 4 + to_col),
                dst_ref=target,
                send_sem=send_sem,
                recv_sem=recv_sem,
                device_id=(to_row, to_col),
                device_id_type=BY_MESH,
            ).start()
            return carry

        lax.fori_loop(1, DEVICES, one, 0)

    def send_all(order, source_of, target, send_sem, recv_sem_of):
        for n, (dz, dy, dx, dc) in enumerate(order):
            to_row = rows_of[0][dz] + rows_of[1][dy] + rows_of[2][dx]
            to_col = cols_of[0][dy] + cols_of[1][dc]
            pltpu.make_async_remote_copy(
                src_ref=source_of(to_row * 4 + to_col),
                dst_ref=target,
                send_sem=send_sem,
                recv_sem=recv_sem_of(n + 1),
                device_id=(to_row, to_col),
                device_id_type=BY_MESH,
            ).start()

    def tile_rows(part):
        return pl.ds(pl.multiple_of(part * TILE, TILE), TILE)

    def wait_part(buffer, sem):
        ref = buffer.at[pl.ds(0, DEVICES - 1), :, pl.ds(0, TILE), :]
        pltpu.make_async_copy(ref, ref, sem).wait()

    def voltage_part(part, carry):
        send_loop(
            lambda to: voltage.at[
                :, tile_rows(part), pl.ds(pl.multiple_of(to * LANES, LANES), LANES)
            ],
            recv1.at[me, :, tile_rows(part), :],
            send_sems.at[0],
            sems1.at[part],
        )
        return carry

    lax.fori_loop(0, PARTS, voltage_part, 0)

    phase_copy.wait()

    def phase_out(b, carry):
        block = phase_in[:, pl.ds(pl.multiple_of(b * LANES, LANES), LANES)]
        phase_send[:, pl.ds(b, 1), :] = jnp.transpose(block).reshape(DEVICES, 1, LANES)
        return carry

    lax.fori_loop(0, ROWS, phase_out, 0)

    send_loop(
        lambda to: phase_send.at[to],
        phase_recv.at[me],
        send_sems.at[1],
        phase_sem,
    )
    phase_recv[me] = phase_send[me]

    def fill(a, carry):
        cos_part, sin_part = unit(sublane * a, 12)
        table_a[a, 0] = cos_part
        table_a[a, 1] = -sin_part
        cos_part, sin_part = unit((a + 128 * sublane) * (128 * me + lane), LOG_TOTAL)
        table_b[a, 0] = cos_part
        table_b[a, 1] = -sin_part
        return carry

    lax.fori_loop(0, DEVICES, fill, 0)

    own_copy.wait()

    def first_part(part, carry):
        wait_part(recv1, sems1.at[part])
        at = tile_rows(part)

        def load(n):
            return recv1[n, 0, at, :], recv1[n, 1, at, :]

        def finish(k, value):
            turn = table_a[k, 0, at, :], table_a[k, 1, at, :]
            value = times(value, turn)
            work[k, 0, at, :] = value[0]
            work[k, 1, at, :] = value[1]

        block_dft(load, tiles, finish, -1)
        return carry

    lax.fori_loop(0, PARTS, first_part, 0)

    for copy in given_copies:
        copy.wait()

    first_lanes = lax.broadcasted_iota(jnp.int32, (8, LANES), 1) < HALF
    for high in range(8):
        columns = slice(high * LANES, high * LANES + LANES)
        straight = taps[:, columns]
        half_taps[0, :, columns] = jnp.where(first_lanes, straight, swapped(straight))
        half_taps[1, :, columns] = jnp.where(first_lanes, swapped(straight), straight)

    def split_dot(matrix, columns):
        high, low = halves(columns)
        return jnp.dot(
            matrix[...],
            jnp.concatenate([high, low, high], axis=0),
            preferred_element_type=F32,
        )

    def in_pairs(places):
        return zip(places[::2], places[1::2])

    def second_step(group, carry):
        done = []
        for pair in in_pairs([8 * group + n for n in range(8)]):
            both = split_dot(
                rows_fwd, jnp.concatenate([work[a].reshape(64, LANES) for a in pair], axis=1)
            )
            for n, a in enumerate(pair):
                columns = slice(n * LANES, n * LANES + LANES)
                done.append((a, (both[:ROWS, columns], both[ROWS:, columns])))
        for a, value in done:
            value = times(value, (table_b[a, 0], table_b[a, 1]))
            send2[a, 0] = value[0]
            send2[a, 1] = value[1]
        return carry

    lax.fori_loop(0, DEVICES // 8, second_step, 0)
    recv2[me] = send2[me]

    def send2_part(part, carry):
        send_loop(
            lambda to: send2.at[to, :, tile_rows(part), :],
            recv2.at[me, :, tile_rows(part), :],
            send_sems.at[2],
            sems2.at[part],
        )
        return carry

    lax.fori_loop(0, PARTS, send2_part, 0)

    phase_all = phase_recv.at[pl.ds(0, DEVICES - 1)]
    pltpu.make_async_copy(phase_all, phase_all, phase_sem).wait()

    def phase_back(b, carry):
        block = phase_recv[:, pl.ds(b, 1), :].reshape(DEVICES, LANES)
        cos_part, sin_part = phase_unit(jnp.transpose(block))
        chirp[:, 0, pl.ds(b, 1), :] = cos_part.reshape(DEVICES, 1, LANES)
        chirp[:, 1, pl.ds(b, 1), :] = sin_part.reshape(DEVICES, 1, LANES)
        return carry

    lax.fori_loop(0, ROWS, phase_back, 0)

    back_tables = table_b, work
    sign = lane_sign((ROWS, LANES))

    def refill(h, carry):
        for half in range(2):
            at = 128 * h + HALF * half + (lane & (HALF - 1))
            cos_part, sin_part = unit((me + 128 * sublane) * at, LOG_TOTAL)
            back_tables[half][h, 0] = cos_part
            back_tables[half][h, 1] = sin_part * sign
        return carry

    lax.fori_loop(0, DEVICES, refill, 0)

    def middle_part(part, carry):
        wait_part(recv2, sems2.at[part])
        at = tile_rows(part)

        def load(n):
            return recv2[n, 0, at, :], recv2[n, 1, at, :]

        def finish(k, value):
            turn = mid_turn[0, pl.ds(k, 1), :], mid_turn[1, pl.ds(k, 1), :]
            value = times(value, turn)
            wide[k, :, :LANES] = value[0]
            wide[k, :, LANES:] = value[1]

        block_dft(load, tiles, finish, -1)

        def lanes_step(group, inner):
            rows = pl.ds(group * 32, 32)
            high, low = halves(wide[rows].reshape(32 * TILE, 2 * LANES))
            there = jnp.dot(
                jnp.concatenate([high, low, high], axis=1),
                lanes_fwd[...],
                preferred_element_type=F32,
            )
            turn = (
                chirp[rows, 0, at, :].reshape(32 * TILE, LANES),
                chirp[rows, 1, at, :].reshape(32 * TILE, LANES),
            )
            there = times((there[:, :LANES], there[:, LANES:]), turn)
            high, low = halves(jnp.concatenate(there, axis=1))
            back = jnp.dot(
                jnp.concatenate([high, low, high], axis=1),
                lanes_inv[...],
                preferred_element_type=F32,
            )
            wide[rows] = back.reshape(32, TILE, 2 * LANES)
            return inner

        lax.fori_loop(0, 4, lanes_step, 0)

        for half in range(2):
            columns = slice(half * LANES, half * LANES + LANES)

            def load_back(n, half=half, columns=columns):
                turn = mid_back[2 * half, pl.ds(n, 1), :], mid_back[2 * half + 1, pl.ds(n, 1), :]
                return (packed_times(wide[n, :, columns], turn),)

            def finish_back(k, value, half=half):
                table = back_tables[half]
                send3[k, half, at, :] = packed_times(
                    value[0], (table[k, 0, at, :], table[k, 1, at, :])
                )

            block_dft(load_back, tiles, finish_back, 1)
            recv3[me, half, at, :] = send3[me, half, at, :]
        send3_part(0, part)
        return carry

    def send3_part(half, part):
        send_all(
            IN_STEPS,
            lambda to: send3.at[to, half, tile_rows(part), :],
            recv3.at[me, half, tile_rows(part), :],
            send_sems.at[3],
            lambda n: sems3.at[(half * PARTS + part) * GROUPS + n // 16],
        )

    def send3_later(part, carry):
        send3_part(1, part)
        return carry

    lax.fori_loop(0, PARTS, middle_part, 0)
    lax.fori_loop(0, PARTS, send3_later, 0)

    def third_step(half, group, eighth):
        places = []
        for n in range(8):
            from_row, from_col = partner(place, 16 * group + 8 * eighth + n, 3)
            places.append(from_row * 4 + from_col)
        done = []
        for pair in in_pairs(places):
            straight = [recv3[a, half] for a in pair]
            turned_up = [swapped(value) * sign for value in straight]
            both = split_dot(
                rows_inv,
                jnp.concatenate(
                    [jnp.concatenate(straight, axis=1), jnp.concatenate(turned_up, axis=1)], axis=0
                ),
            )
            for n, a in enumerate(pair):
                done.append((a, both[:, n * LANES : n * LANES + LANES]))
        for a, value in done:
            work[a, half] = packed_times(value, (table_a[a, 0], -sign * table_a[a, 1]))

    def third_group(half, group, count):
        def wait_one(part, inner):
            ref = recv3.at[pl.ds(0, count), half, pl.ds(0, TILE), :]
            pltpu.make_async_copy(
                ref, ref, sems3.at[(half * PARTS + part) * GROUPS + group]
            ).wait()
            return inner

        lax.fori_loop(0, PARTS, wait_one, 0)

        def one(eighth, inner):
            third_step(half, group, eighth)
            return inner

        lax.fori_loop(0, 2, one, 0)

    def third_half(half):
        def later_group(group, carry):
            third_group(half, group, 16)
            return carry

        third_group(half, 0, 15)
        lax.fori_loop(1, GROUPS, later_group, 0)

    def fourth_part(half, part):
        at = slice(part * TILE, part * TILE + TILE)

        def load(n):
            return (work[n, half, at, :],)

        def finish(k, value):
            send4[k, half, at, :] = value[0]
            if (half, part) in ((1, 0), (1, 1)):
                edge_send[k, part : part + 1, :] = value[0][TILE - 1 :]

        block_dft(load, tiles, finish, 1)
        recv4[me, half, at, :] = send4[me, half, at, :]

    def send4_part(half, part):
        at = slice(part * TILE, part * TILE + TILE)
        send_all(
            FAR_FIRST,
            lambda to: send4.at[to, half, at, :],
            recv4.at[me, half, at, :],
            send_sems.at[4],
            lambda n: sems4.at[half * PARTS + part],
        )

    def edge_pieces():
        send_all(
            FAR_FIRST,
            lambda to: edge_send.at[to],
            edge_recv.at[me],
            send_sems.at[5],
            lambda n: edge_sem,
        )

    def wait4(half, part):
        ref = recv4.at[pl.ds(0, DEVICES - 1), half, pl.ds(0, TILE), :]
        pltpu.make_async_copy(ref, ref, sems4.at[half * PARTS + part]).wait()

    following = lax.rem(me + 1, DEVICES)
    span_copies = [
        pltpu.make_async_remote_copy(
            src_ref=span_send.at[half],
            dst_ref=span_recv.at[half],
            send_sem=send_sems.at[6 + half],
            recv_sem=span_sems.at[half],
            device_id=(following // 4, lax.rem(following, 4)),
            device_id_type=BY_MESH,
        )
        for half in range(2)
    ]

    def send_span(half):
        def span_row(j, carry):
            span_send[half, pl.ds(j, 1), :] = recv4[FIRST_EDGE + j, half, ROWS - 1 :, :]
            return carry

        wait4(half, 3)
        lax.fori_loop(0, DEVICES - FIRST_EDGE, span_row, 0)
        span_copies[half].start()

    with_edges = me >= FIRST_EDGE
    third_half(0)
    for part in (3, 2, 1, 0):
        fourth_part(0, part)
        send4_part(0, part)
    third_half(1)
    for part in (3, 2, 1, 0):
        fourth_part(1, part)
    edge_recv[me] = edge_send[me]
    send_span(0)
    send4_part(1, 3)
    pl.when(with_edges)(edge_pieces)
    send4_part(1, 2)
    send4_part(1, 1)

    first_row = lax.broadcasted_iota(jnp.int32, (TILE, LANES), 0) == 0
    ahead = me > 0
    frames = table_a.reshape(PARTS, 8, 2, 128, LANES)
    gathered = table_b.reshape(PARTS, 2, 1024, LANES)

    def filter_part(half, part):
        at = slice(part * TILE, part * TILE + TILE)

        def edge_row(high, m):
            if part == 0:
                edge = span_recv[half, pl.ds(8 * m + high - FIRST_EDGE, 1), :]
                return jnp.where(ahead, edge, 0.0)
            if (half, part) in ((1, 1), (1, 2)):
                return edge_recv[8 * m + high, part - 1 : part, :]
            return recv4[8 * m + high, half, part * TILE - 1 : part * TILE, :]

        def one_position(high, carry):
            weights = [
                half_taps[half, t : t + 1, pl.ds(pl.multiple_of(high * LANES, LANES), LANES)]
                for t in range(8)
            ]
            now = [recv4[8 * m + high, half, at, :] for m in range(16)]
            old = [None] * 16
            for m in range(9, 16):
                old[m] = jnp.where(first_row, edge_row(high, m), pltpu.roll(now[m], 1, 0))
            for m in range(16):
                total = weights[0] * now[m]
                for t in range(1, 8):
                    total = total + weights[t] * (now[m - t] if m >= t else old[m - t + 16])
                work[16 * high + m, half, at, :] = total
            return carry

        lax.fori_loop(0, 8, one_position, 0)

        def some_frames(step, carry):
            ms = [4 * step + n for n in range(4)]
            given = [[(work[16 * high + m, half, at, :],) for high in range(8)] for m in ms]
            done = [small_dft(values, -1) for values in given]
            for m, values in zip(ms, done):
                for a, value in enumerate(values):
                    turn = (
                        out_turn[2 * half, a : a + 1, :],
                        out_turn[2 * half + 1, a : a + 1, :],
                    )
                    frames[part, a, half, pl.ds(m, TILE, stride=16), :] = packed_times(
                        value[0], turn
                    )
            return carry

        lax.fori_loop(0, 4, some_frames, 0)

    def ready_copy(part):
        return pltpu.make_async_copy(gathered.at[part], ready.at[part - 1], out_sem.at[part])

    def finish_parts(parts):
        classes = 2 // len(parts)

        def some_classes(step, carry):
            each = [(p, classes * step + n) for n in range(classes) for p in parts]
            both = frames_dft(
                lanes_out, *[jnp.concatenate([frames[p, a, c] for p, a in each]) for c in range(2)]
            )
            for c in range(2):
                for n, (p, a) in enumerate(each):
                    gathered[p, c, pl.ds(a, 128, stride=8), :] = both[
                        c * 128 : c * 128 + 128, n * LANES : n * LANES + LANES
                    ]
            return carry

        lax.fori_loop(0, 8 // classes, some_classes, 0)
        for p in parts:
            ready_copy(p).start()

    for part in (2, 1, 0):
        wait4(0, part)
    for part in (3, 2, 1):
        filter_part(0, part)
    send_span(1)
    send4_part(1, 0)
    span_copies[0].wait_recv()
    filter_part(0, 0)
    wait4(1, 2)
    filter_part(1, 3)

    def wait_edges(count):
        ref = edge_recv.at[pl.ds(0, count)]
        pltpu.make_async_copy(ref, ref, edge_sem).wait()

    pl.when(with_edges)(lambda: wait_edges(DEVICES - FIRST_EDGE - 1))
    pl.when(jnp.logical_not(with_edges))(lambda: wait_edges(DEVICES - FIRST_EDGE))
    filter_part(1, 2)
    finish_parts((2, 3))
    wait4(1, 1)
    filter_part(1, 1)
    finish_parts((1,))
    wait4(1, 0)
    span_copies[1].wait_recv()
    filter_part(1, 0)
    late_copy = pltpu.make_async_copy(frames.at[0], late, out_sem.at[0])
    late_copy.start()
    for part in range(1, PARTS):
        ready_copy(part).wait()
    late_copy.wait()
    for copy in span_copies:
        copy.wait_send()

    def wait_edges_sent():
        ref = edge_recv.at[pl.ds(0, DEVICES - 1)]
        pltpu.make_async_copy(ref, ref, send_sems.at[5]).wait()

    pl.when(with_edges)(wait_edges_sent)
    pieces = recv1.at[pl.ds(0, DEVICES - 1)]
    for at in (0, 2, 3, 4):
        pltpu.make_async_copy(pieces, pieces, send_sems.at[at]).wait()
    pltpu.make_async_copy(phase_all, phase_all, send_sems.at[1]).wait()


def last_kernel(late, ready, lanes_out, result, frames, passing, gathered, matrix, sems, more):
    frame_copies = [pltpu.make_async_copy(late.at[a], frames.at[a], sems.at[a]) for a in range(8)]
    matrix_copy = pltpu.make_async_copy(lanes_out, matrix, more.at[0])
    pass_in = [
        pltpu.make_async_copy(ready.at[n], passing.at[n], more.at[1 + n]) for n in range(3)
    ]

    def to_result(source, column, sem):
        return pltpu.make_async_copy(source, result.at[:, :, pl.ds(column * LANES, LANES)], sem)

    passed = [to_result(passing.at[n], 1 + n, more.at[4 + n]) for n in range(3)]
    computed = to_result(gathered, 0, more.at[7])
    matrix_copy.start()
    for copy in frame_copies + pass_in:
        copy.start()
    matrix_copy.wait()
    for a in range(0, 8, 2):
        frame_copies[a].wait()
        frame_copies[a + 1].wait()
        both = frames_dft(
            matrix, *[jnp.concatenate([frames[a, c], frames[a + 1, c]]) for c in range(2)]
        )
        for c in range(2):
            for n in range(2):
                gathered[c, pl.ds(a + n, 128, stride=8), :] = both[
                    c * 128 : c * 128 + 128, n * LANES : n * LANES + LANES
                ]
        if a < 6:
            pass_in[a // 2].wait()
            passed[a // 2].start()
    computed.start()
    for copy in passed + [computed]:
        copy.wait()


def dft_parts(size, sign, scale=1.0):
    digits = np.arange(size)
    angle = sign * 2.0 * np.pi * ((digits[:, None] * digits[None, :]) % size) / size
    return scale * np.cos(angle), scale * np.sin(angle)


def bf16_halves(matrix):
    matrix = np.asarray(matrix, np.float32)
    high = matrix.astype(BF16)
    return high, (matrix - high.astype(np.float32)).astype(BF16)


BY_HALVES = np.concatenate([c * LANES + h * HALF + np.arange(HALF) for h in (0, 1) for c in (0, 1)])


def beside(matrix):
    high, low = bf16_halves(matrix)
    return np.concatenate([high, high, low], axis=1)


def above(matrix):
    high, low = bf16_halves(matrix)
    return np.concatenate([high, high, low], axis=0)


def left_matrix(size, sign):
    c, s = dft_parts(size, sign)
    return np.block([[c, -s], [s, c]])


def right_matrix(size, sign, scale=1.0):
    c, s = dft_parts(size, sign, scale)
    return np.block([[c, s], [-s, c]])


def turn_table(rows, cols, sign):
    whole = rows * cols
    angle = sign * 2.0 * np.pi * (np.arange(rows)[:, None] * np.arange(cols)[None, :]) / whole
    return np.stack([np.cos(angle), np.sin(angle)]).astype(np.float32)


def packed_table(rows, cols, sign):
    c, s = turn_table(rows, cols, sign)
    each = []
    for half in (slice(0, HALF), slice(HALF, LANES)):
        each.append(np.concatenate([c[:, half], c[:, half]], axis=1))
        each.append(np.concatenate([-s[:, half], s[:, half]], axis=1))
    return np.stack(each)


def local(voltage, chirp_phase, filter_taps):
    constants = [
        beside(left_matrix(ROWS, -1)),
        beside(np.concatenate(dft_parts(ROWS, 1), axis=1)),
        above(right_matrix(LANES, -1)),
        above(right_matrix(LANES, 1, 2.0**-LOG_TOTAL)[:, BY_HALVES]),
        beside(left_matrix(LANES, -1)[:, BY_HALVES]),
        turn_table(128, LANES, -1),
        packed_table(128, LANES, 1),
        packed_table(8, LANES, -1),
    ]
    blocks = pltpu.VMEM((DEVICES, 2, ROWS, LANES), F32)
    phases = pltpu.VMEM((DEVICES, ROWS, LANES), F32)
    in_hbm = pl.BlockSpec(memory_space=pl.ANY)
    given = [filter_taps] + [jnp.asarray(c) for c in constants]
    late, ready = pl.pallas_call(
        kernel,
        out_shape=[
            jax.ShapeDtypeStruct((8, 2, 128, LANES), F32),
            jax.ShapeDtypeStruct((3, 2, 1024, LANES), F32),
        ],
        in_specs=[in_hbm] * (2 + len(given)),
        out_specs=[in_hbm] * 2,
        scratch_shapes=[pltpu.VMEM(c.shape, c.dtype) for c in given]
        + [blocks] * 8
        + [pltpu.VMEM((DEVICES, 4096), F32)]
        + [phases] * 2
        + [blocks] * 3
        + [
            pltpu.VMEM((DEVICES, 2, TILE, LANES), F32),
            pltpu.VMEM((DEVICES, TILE, 2 * LANES), F32),
            pltpu.VMEM((DEVICES, 2, LANES), F32),
            pltpu.VMEM((DEVICES, 2, LANES), F32),
            pltpu.VMEM((2, DEVICES - FIRST_EDGE, LANES), F32),
            pltpu.VMEM((2, DEVICES - FIRST_EDGE, LANES), F32),
            pltpu.VMEM((2, 8, 1024), F32),
            pltpu.SemaphoreType.DMA((2,)),
            pltpu.SemaphoreType.DMA((PARTS,)),
            pltpu.SemaphoreType.DMA((PARTS,)),
            pltpu.SemaphoreType.DMA((2 * PARTS * GROUPS,)),
            pltpu.SemaphoreType.DMA((2 * PARTS,)),
            pltpu.SemaphoreType.DMA,
            pltpu.SemaphoreType.DMA,
            pltpu.SemaphoreType.DMA((2,)),
            pltpu.SemaphoreType.DMA((8,)),
            pltpu.SemaphoreType.DMA((PARTS,)),
            pltpu.SemaphoreType.DMA((CONSTANTS,)),
            pltpu.SemaphoreType.REGULAR,
        ],
        compiler_params=pltpu.CompilerParams(
            collective_id=0, has_side_effects=True, vmem_limit_bytes=67043328
        ),
    )(voltage, chirp_phase, *given)
    return pl.pallas_call(
        last_kernel,
        out_shape=jax.ShapeDtypeStruct((2, 1024, 512), F32),
        in_specs=[in_hbm] * 3,
        out_specs=in_hbm,
        scratch_shapes=[
            pltpu.VMEM((8, 2, 128, LANES), F32),
            pltpu.VMEM((3, 2, 1024, LANES), F32),
            pltpu.VMEM((2, 1024, LANES), F32),
            pltpu.VMEM((256, 768), BF16),
            pltpu.SemaphoreType.DMA((8,)),
            pltpu.SemaphoreType.DMA((8,)),
        ],
        compiler_params=pltpu.CompilerParams(vmem_limit_bytes=67043328),
    )(late, ready, given[5])


def solution(mesh):
    in_specs = (P(None, ("row", "col"), None), P(("row", "col"), None), P())
    out_specs = P(None, None, ("row", "col"))
    return jax.shard_map(local, mesh=mesh, in_specs=in_specs, out_specs=out_specs, check_vma=False)
```

```python
import math
import random

import jax
import jax.numpy as jnp
import numpy as np
from jax import lax
from jax.experimental import pallas as pl
from jax.experimental.pallas import tpu as pltpu
from jax.sharding import PartitionSpec as P

DEVICES = 128
ROWS = 32
TILE = 8
PARTS = ROWS // TILE
LANES = 128
HALF = LANES // 2
LOG_TOTAL = 26
GROUPS = DEVICES // 16
CONSTANTS = 9
FIRST_EDGE = 72
IN_STEPS = [
    (n % 4, (n % 4 + n // 4) % 4, (n % 4 + n // 4 + n // 16) % 4, n // 64)
    for n in range(1, DEVICES)
]
FAR_FIRST = list(IN_STEPS)
random.Random(1).shuffle(FAR_FIRST)
FAR_FIRST.sort(key=lambda offset: -sum(min(d, 4 - d) for d in offset[:3]))
BY_MESH = pl.DeviceIdType.MESH
F32 = jnp.float32
BF16 = jnp.bfloat16


def device_at(z, y, x, core):
    return z * 8 + lax.rem(y, 2) * 4 + x, (y // 2) * 2 + core


def partner(here, step, way=1):
    z, y, x, core = here
    low = lax.rem(step, 4)
    mid = low + lax.rem(step // 4, 4)
    high = mid + lax.rem(step // 16, 4)
    return device_at(
        lax.rem(z + way * low, 4),
        lax.rem(y + way * mid, 4),
        lax.rem(x + way * high, 4),
        lax.rem(core + step // 64, 2),
    )


def times(a, b):
    return a[0] * b[0] - a[1] * b[1], a[0] * b[1] + a[1] * b[0]


def plus(a, b):
    return tuple(x + y for x, y in zip(a, b))


def minus(a, b):
    return tuple(x - y for x, y in zip(a, b))


def turned(a, part, whole, sign):
    part = part % whole
    eighths = 8 * part / whole
    if eighths == 0:
        return a
    if eighths == 2:
        return (-a[1], a[0]) if sign > 0 else (a[1], -a[0])
    if eighths == 4:
        return -a[0], -a[1]
    if eighths == 6:
        return (a[1], -a[0]) if sign > 0 else (-a[1], a[0])
    angle = sign * 2.0 * math.pi * part / whole
    cos_part, sin_part = math.cos(angle), math.sin(angle)
    if eighths in (1, 3, 5, 7):
        half = math.sqrt(0.5)
        c = half if cos_part > 0 else -half
        same = (cos_part > 0) == (sin_part > 0)
        if same:
            return (a[0] - a[1]) * c, (a[0] + a[1]) * c
        return (a[0] + a[1]) * c, (a[1] - a[0]) * c
    return a[0] * cos_part - a[1] * sin_part, a[0] * sin_part + a[1] * cos_part


def lane_sign(shape):
    return jnp.where(lax.broadcasted_iota(jnp.int32, shape, len(shape) - 1) < HALF, -1.0, 1.0)


def swapped(x):
    return pltpu.roll(x, HALF, x.ndim - 1)


def packed_times(x, turn):
    return x * turn[0] + swapped(x) * turn[1]


def packed_turned(a, part, whole, sign):
    part = part % whole
    angle = sign * 2.0 * math.pi * part / whole
    (x,) = a
    if part == 0:
        return a
    if 2 * part == whole:
        return (-x,)
    if 4 * part in (whole, 3 * whole):
        up = (4 * part == whole) == (sign > 0)
        return (swapped(x) * (lane_sign(x.shape) if up else -lane_sign(x.shape)),)
    return (math.cos(angle) * x + swapped(x) * (math.sin(angle) * lane_sign(x.shape)),)


def small_dft(xs, sign):
    n = len(xs)
    turn = turned if len(xs[0]) == 2 else packed_turned
    if n == 1:
        return xs
    if n == 2:
        return [plus(xs[0], xs[1]), minus(xs[0], xs[1])]
    parts = [small_dft(xs[r::4], sign) for r in range(4)]
    out = [None] * n
    for k in range(n // 4):
        a, b, c, d = (turn(parts[r][k], r * k, n, sign) for r in range(4))
        ac, bd = plus(a, c), plus(b, d)
        ac_, bd_ = minus(a, c), turn(minus(b, d), 1, 4, sign)
        out[k] = plus(ac, bd)
        out[k + n // 4] = plus(ac_, bd_)
        out[k + n // 2] = minus(ac, bd)
        out[k + 3 * n // 4] = minus(ac_, bd_)
    return out


def block_dft(load, scratch, finish, sign):
    for low in range(8):
        values = small_dft([load(8 * high + low) for high in range(16)], sign)
        for k, value in enumerate(values):
            turn = turned if len(value) == 2 else packed_turned
            value = turn(value, low * k, 128, sign)
            for c, x in enumerate(value):
                scratch[8 * k + low, c] = x
    parts = range(len(value))
    together = 1 if len(value) == 2 else 4

    def second(step, carry):
        ks = [together * step + n for n in range(together)]
        given = [
            [tuple(scratch[8 * k + low, c] for c in parts) for low in range(8)] for k in ks
        ]
        done = [small_dft(values, sign) for values in given]
        for k, values in zip(ks, done):
            for high, value in enumerate(values):
                finish(k + 16 * high, value)
        return carry

    lax.fori_loop(0, 16 // together, second, 0)


def quarter_sincos(angle, quarter):
    square = angle * angle
    sin_part = angle * (
        1.0 + square * (-1.0 / 6 + square * (1.0 / 120 + square * (-1.0 / 5040 + square / 362880)))
    )
    cos_part = 1.0 + square * (
        -0.5 + square * (1.0 / 24 + square * (-1.0 / 720 + square * (1.0 / 40320)))
    )
    odd = (quarter & 1) == 1
    first = jnp.where(odd, sin_part, cos_part)
    second = jnp.where(odd, cos_part, sin_part)
    return (
        jnp.where(((quarter + 1) & 2) == 2, -first, first),
        jnp.where((quarter & 2) == 2, -second, second),
    )


def unit(product, log_whole):
    quarter = (product + (1 << (log_whole - 3))) >> (log_whole - 2)
    rest = product - (quarter << (log_whole - 2))
    return quarter_sincos(rest.astype(F32) * (2.0 * math.pi / 2**log_whole), quarter)


def phase_unit(phase):
    quarter = jnp.floor(phase * (2.0 / math.pi) + 0.5)
    high = float(np.float32(1.5703125))
    angle = (phase - quarter * high) - quarter * (math.pi / 2 - high)
    return quarter_sincos(angle, quarter.astype(jnp.int32))


def halves(x):
    high = x.astype(BF16)
    return high, (x - high.astype(F32)).astype(BF16)


def frames_dft(matrix, real_part, imag_part):
    high, low = halves(jnp.concatenate([real_part, imag_part], axis=1))
    return lax.dot_general(
        matrix[...],
        jnp.concatenate([high, low, high], axis=1),
        (((1,), (1,)), ((), ())),
        preferred_element_type=F32,
    )


def kernel(
    voltage,
    phase,
    *refs,
):
    given, refs = refs[:CONSTANTS], refs[CONSTANTS:]
    late, ready, refs = refs[0], refs[1], refs[2:]
    held, refs = refs[:CONSTANTS], refs[CONSTANTS:]
    taps, rows_fwd, rows_inv, lanes_fwd, lanes_inv, lanes_out, mid_turn, mid_back, out_turn = held
    (
    recv1,
    work,
    send2,
    recv2,
    send3,
    recv3,
    send4,
    recv4,
    phase_in,
    phase_send,
    phase_recv,
    chirp,
    table_a,
    table_b,
    tiles,
    wide,
    edge_send,
    edge_recv,
    span_send,
    span_recv,
    half_taps,
    local_sem,
    sems1,
    sems2,
    sems3,
    sems4,
    phase_sem,
    edge_sem,
    span_sems,
    send_sems,
    out_sem,
    given_sem,
    plane_sem,
    ) = refs
    row = lax.axis_index("row")
    col = lax.axis_index("col")
    me = row * 4 + col
    sublane = lax.broadcasted_iota(jnp.int32, (ROWS, LANES), 0)
    lane = lax.broadcasted_iota(jnp.int32, (ROWS, LANES), 1)

    phase_copy = pltpu.make_async_copy(phase, phase_in, local_sem.at[0])
    phase_copy.start()
    own_copy = pltpu.make_async_copy(
        voltage.at[:, :, pl.ds(pl.multiple_of(me * LANES, LANES), LANES)],
        recv1.at[me],
        local_sem.at[1],
    )
    own_copy.start()
    given_copies = [
        pltpu.make_async_copy(a, b, given_sem.at[n]) for n, (a, b) in enumerate(zip(given, held))
    ]
    for copy in given_copies:
        copy.start()

    place = row // 8, (col // 2) * 2 + lax.rem(row // 4, 2), lax.rem(row, 4), lax.rem(col, 2)
    z, y, x, core = place
    barrier = pltpu.get_barrier_semaphore()

    def greet_along(other):
        to = device_at(lax.rem(z + other, 4), y, x, core)
        return dict(inc=1, device_id=to, device_id_type=BY_MESH)

    for _, dy, dx, dc in (offset for offset in FAR_FIRST if offset[0] == 0):
        to = device_at(z, lax.rem(y + dy, 4), lax.rem(x + dx, 4), lax.rem(core + dc, 2))
        pl.semaphore_signal(barrier, inc=1, device_id=to, device_id_type=BY_MESH)
    for other in range(1, 4):
        pl.semaphore_signal(barrier, **greet_along(other))
    pl.semaphore_wait(barrier, 34)
    for other in range(1, 4):
        pl.semaphore_signal(plane_sem, **greet_along(other))
    pl.semaphore_wait(plane_sem, 3)

    rows_of = [
        [lax.rem(z + n, 4) * 8 for n in range(4)],
        [lax.rem(y + n, 2) * 4 for n in range(4)],
        [lax.rem(x + n, 4) for n in range(4)],
    ]
    cols_of = [
        [lax.rem(y + n, 4) // 2 * 2 for n in range(4)],
        [lax.rem(core + n, 2) for n in range(2)],
    ]

    def send_loop(source_of, target, send_sem, recv_sem):
        def one(step, carry):
            to_row, to_col = partner(place, step)
            pltpu.make_async_remote_copy(
                src_ref=source_of(to_row * 4 + to_col),
                dst_ref=target,
                send_sem=send_sem,
                recv_sem=recv_sem,
                device_id=(to_row, to_col),
                device_id_type=BY_MESH,
            ).start()
            return carry

        lax.fori_loop(1, DEVICES, one, 0)

    def send_all(order, source_of, target, send_sem, recv_sem_of):
        for n, (dz, dy, dx, dc) in enumerate(order):
            to_row = rows_of[0][dz] + rows_of[1][dy] + rows_of[2][dx]
            to_col = cols_of[0][dy] + cols_of[1][dc]
            pltpu.make_async_remote_copy(
                src_ref=source_of(to_row * 4 + to_col),
                dst_ref=target,
                send_sem=send_sem,
                recv_sem=recv_sem_of(n + 1),
                device_id=(to_row, to_col),
                device_id_type=BY_MESH,
            ).start()

    def tile_rows(part):
        return pl.ds(pl.multiple_of(part * TILE, TILE), TILE)

    def wait_part(buffer, sem):
        ref = buffer.at[pl.ds(0, DEVICES - 1), :, pl.ds(0, TILE), :]
        pltpu.make_async_copy(ref, ref, sem).wait()

    def voltage_part(part, carry):
        send_loop(
            lambda to: voltage.at[
                :, tile_rows(part), pl.ds(pl.multiple_of(to * LANES, LANES), LANES)
            ],
            recv1.at[me, :, tile_rows(part), :],
            send_sems.at[0],
            sems1.at[part],
        )
        return carry

    lax.fori_loop(0, PARTS, voltage_part, 0)

    phase_copy.wait()

    def phase_out(b, carry):
        block = phase_in[:, pl.ds(pl.multiple_of(b * LANES, LANES), LANES)]
        phase_send[:, pl.ds(b, 1), :] = jnp.transpose(block).reshape(DEVICES, 1, LANES)
        return carry

    lax.fori_loop(0, ROWS, phase_out, 0)

    send_loop(
        lambda to: phase_send.at[to],
        phase_recv.at[me],
        send_sems.at[1],
        phase_sem,
    )
    phase_recv[me] = phase_send[me]

    def fill(a, carry):
        cos_part, sin_part = unit(sublane * a, 12)
        table_a[a, 0] = cos_part
        table_a[a, 1] = -sin_part
        cos_part, sin_part = unit((a + 128 * sublane) * (128 * me + lane), LOG_TOTAL)
        table_b[a, 0] = cos_part
        table_b[a, 1] = -sin_part
        return carry

    lax.fori_loop(0, DEVICES, fill, 0)

    own_copy.wait()

    def first_part(part, carry):
        wait_part(recv1, sems1.at[part])
        at = tile_rows(part)

        def load(n):
            return recv1[n, 0, at, :], recv1[n, 1, at, :]

        def finish(k, value):
            turn = table_a[k, 0, at, :], table_a[k, 1, at, :]
            value = times(value, turn)
            work[k, 0, at, :] = value[0]
            work[k, 1, at, :] = value[1]

        block_dft(load, tiles, finish, -1)
        return carry

    lax.fori_loop(0, PARTS, first_part, 0)

    for copy in given_copies:
        copy.wait()

    first_lanes = lax.broadcasted_iota(jnp.int32, (8, LANES), 1) < HALF
    for high in range(8):
        columns = slice(high * LANES, high * LANES + LANES)
        straight = taps[:, columns]
        half_taps[0, :, columns] = jnp.where(first_lanes, straight, swapped(straight))
        half_taps[1, :, columns] = jnp.where(first_lanes, swapped(straight), straight)

    def split_dot(matrix, columns):
        high, low = halves(columns)
        return jnp.dot(
            matrix[...],
            jnp.concatenate([high, low, high], axis=0),
            preferred_element_type=F32,
        )

    def in_pairs(places):
        return zip(places[::2], places[1::2])

    def second_step(group, carry):
        done = []
        for pair in in_pairs([8 * group + n for n in range(8)]):
            both = split_dot(
                rows_fwd, jnp.concatenate([work[a].reshape(64, LANES) for a in pair], axis=1)
            )
            for n, a in enumerate(pair):
                columns = slice(n * LANES, n * LANES + LANES)
                done.append((a, (both[:ROWS, columns], both[ROWS:, columns])))
        for a, value in done:
            value = times(value, (table_b[a, 0], table_b[a, 1]))
            send2[a, 0] = value[0]
            send2[a, 1] = value[1]
        return carry

    lax.fori_loop(0, DEVICES // 8, second_step, 0)
    recv2[me] = send2[me]

    def send2_part(part, carry):
        send_loop(
            lambda to: send2.at[to, :, tile_rows(part), :],
            recv2.at[me, :, tile_rows(part), :],
            send_sems.at[2],
            sems2.at[part],
        )
        return carry

    lax.fori_loop(0, PARTS, send2_part, 0)

    phase_all = phase_recv.at[pl.ds(0, DEVICES - 1)]
    pltpu.make_async_copy(phase_all, phase_all, phase_sem).wait()

    def phase_back(b, carry):
        block = phase_recv[:, pl.ds(b, 1), :].reshape(DEVICES, LANES)
        cos_part, sin_part = phase_unit(jnp.transpose(block))
        chirp[:, 0, pl.ds(b, 1), :] = cos_part.reshape(DEVICES, 1, LANES)
        chirp[:, 1, pl.ds(b, 1), :] = sin_part.reshape(DEVICES, 1, LANES)
        return carry

    lax.fori_loop(0, ROWS, phase_back, 0)

    back_tables = table_b, work
    sign = lane_sign((ROWS, LANES))

    def refill(h, carry):
        for half in range(2):
            at = 128 * h + HALF * half + (lane & (HALF - 1))
            cos_part, sin_part = unit((me + 128 * sublane) * at, LOG_TOTAL)
            back_tables[half][h, 0] = cos_part
            back_tables[half][h, 1] = sin_part * sign
        return carry

    lax.fori_loop(0, DEVICES, refill, 0)

    def middle_part(part, carry):
        wait_part(recv2, sems2.at[part])
        at = tile_rows(part)

        def load(n):
            return recv2[n, 0, at, :], recv2[n, 1, at, :]

        def finish(k, value):
            turn = mid_turn[0, pl.ds(k, 1), :], mid_turn[1, pl.ds(k, 1), :]
            value = times(value, turn)
            wide[k, :, :LANES] = value[0]
            wide[k, :, LANES:] = value[1]

        block_dft(load, tiles, finish, -1)

        def lanes_step(group, inner):
            rows = pl.ds(group * 32, 32)
            high, low = halves(wide[rows].reshape(32 * TILE, 2 * LANES))
            there = jnp.dot(
                jnp.concatenate([high, low, high], axis=1),
                lanes_fwd[...],
                preferred_element_type=F32,
            )
            turn = (
                chirp[rows, 0, at, :].reshape(32 * TILE, LANES),
                chirp[rows, 1, at, :].reshape(32 * TILE, LANES),
            )
            there = times((there[:, :LANES], there[:, LANES:]), turn)
            high, low = halves(jnp.concatenate(there, axis=1))
            back = jnp.dot(
                jnp.concatenate([high, low, high], axis=1),
                lanes_inv[...],
                preferred_element_type=F32,
            )
            wide[rows] = back.reshape(32, TILE, 2 * LANES)
            return inner

        lax.fori_loop(0, 4, lanes_step, 0)

        for half in range(2):
            columns = slice(half * LANES, half * LANES + LANES)

            def load_back(n, half=half, columns=columns):
                turn = mid_back[2 * half, pl.ds(n, 1), :], mid_back[2 * half + 1, pl.ds(n, 1), :]
                return (packed_times(wide[n, :, columns], turn),)

            def finish_back(k, value, half=half):
                table = back_tables[half]
                send3[k, half, at, :] = packed_times(
                    value[0], (table[k, 0, at, :], table[k, 1, at, :])
                )

            block_dft(load_back, tiles, finish_back, 1)
            recv3[me, half, at, :] = send3[me, half, at, :]
        send3_rows(0, at, part * GROUPS)
        return carry

    def send3_rows(half, rows, first_sem):
        send_all(
            IN_STEPS,
            lambda to: send3.at[to, half, rows, :],
            recv3.at[me, half, rows, :],
            send_sems.at[3],
            lambda n: sems3.at[first_sem + n // 16],
        )

    lax.fori_loop(0, PARTS, middle_part, 0)
    send3_rows(1, slice(0, ROWS), PARTS * GROUPS)

    def third_step(half, group, eighth):
        places = []
        for n in range(8):
            from_row, from_col = partner(place, 16 * group + 8 * eighth + n, 3)
            places.append(from_row * 4 + from_col)
        done = []
        for pair in in_pairs(places):
            straight = [recv3[a, half] for a in pair]
            turned_up = [swapped(value) * sign for value in straight]
            both = split_dot(
                rows_inv,
                jnp.concatenate(
                    [jnp.concatenate(straight, axis=1), jnp.concatenate(turned_up, axis=1)], axis=0
                ),
            )
            for n, a in enumerate(pair):
                done.append((a, both[:, n * LANES : n * LANES + LANES]))
        for a, value in done:
            work[a, half] = packed_times(value, (table_a[a, 0], -sign * table_a[a, 1]))

    def third_group(half, group, count):
        def wait_rows(rows, sem):
            ref = recv3.at[pl.ds(0, count), half, pl.ds(0, rows), :]
            pltpu.make_async_copy(ref, ref, sems3.at[sem + group]).wait()

        def wait_one(part, inner):
            wait_rows(TILE, part * GROUPS)
            return inner

        if half == 0:
            lax.fori_loop(0, PARTS, wait_one, 0)
        else:
            wait_rows(ROWS, PARTS * GROUPS)

        def one(eighth, inner):
            third_step(half, group, eighth)
            return inner

        lax.fori_loop(0, 2, one, 0)

    def third_half(half):
        def later_group(group, carry):
            third_group(half, group, 16)
            return carry

        third_group(half, 0, 15)
        lax.fori_loop(1, GROUPS, later_group, 0)

    def fourth_part(half, part):
        at = slice(part * TILE, part * TILE + TILE)

        def load(n):
            return (work[n, half, at, :],)

        def finish(k, value):
            send4[k, half, at, :] = value[0]
            if half == 1 and part < 3:
                edge_send[k, part : part + 1, :] = value[0][TILE - 1 :]

        block_dft(load, tiles, finish, 1)
        recv4[me, half, at, :] = send4[me, half, at, :]

    def send4_tiles(half, first, count):
        at = slice(first * TILE, (first + count) * TILE)
        send_all(
            FAR_FIRST,
            lambda to: send4.at[to, half, at, :],
            recv4.at[me, half, at, :],
            send_sems.at[4],
            lambda n: sems4.at[half * PARTS + first],
        )

    def edge_pieces():
        send_all(
            FAR_FIRST,
            lambda to: edge_send.at[to],
            edge_recv.at[me],
            send_sems.at[5],
            lambda n: edge_sem,
        )

    def wait4(half, first, count):
        ref = recv4.at[pl.ds(0, DEVICES - 1), half, pl.ds(0, count * TILE), :]
        pltpu.make_async_copy(ref, ref, sems4.at[half * PARTS + first]).wait()

    following = lax.rem(me + 1, DEVICES)
    span_copies = [
        pltpu.make_async_remote_copy(
            src_ref=span_send.at[half],
            dst_ref=span_recv.at[half],
            send_sem=send_sems.at[6 + half],
            recv_sem=span_sems.at[half],
            device_id=(following // 4, lax.rem(following, 4)),
            device_id_type=BY_MESH,
        )
        for half in range(2)
    ]

    def send_span(half):
        def span_row(j, carry):
            span_send[half, pl.ds(j, 1), :] = recv4[FIRST_EDGE + j, half, ROWS - 1 :, :]
            return carry

        lax.fori_loop(0, DEVICES - FIRST_EDGE, span_row, 0)
        span_copies[half].start()

    with_edges = me >= FIRST_EDGE
    third_half(0)
    fourth_part(0, 3)
    send4_tiles(0, 3, 1)
    for part in (2, 1, 0):
        fourth_part(0, part)
    send4_tiles(0, 0, 3)
    third_half(1)
    for part in (3, 2, 1, 0):
        fourth_part(1, part)
    edge_recv[me] = edge_send[me]
    wait4(0, 3, 1)
    send_span(0)
    pl.when(with_edges)(edge_pieces)
    send4_tiles(1, 3, 1)
    send4_tiles(1, 2, 1)
    send4_tiles(1, 1, 1)

    first_row = lax.broadcasted_iota(jnp.int32, (TILE, LANES), 0) == 0
    ahead = me > 0
    frames = table_a.reshape(PARTS, 8, 2, 128, LANES)
    gathered = table_b.reshape(PARTS, 2, 1024, LANES)

    def filter_part(half, part):
        at = slice(part * TILE, part * TILE + TILE)

        def edge_row(high, m):
            if part == 0:
                edge = span_recv[half, pl.ds(8 * m + high - FIRST_EDGE, 1), :]
                return jnp.where(ahead, edge, 0.0)
            if half == 1:
                return edge_recv[8 * m + high, part - 1 : part, :]
            return recv4[8 * m + high, half, part * TILE - 1 : part * TILE, :]

        def one_position(high, carry):
            weights = [
                half_taps[half, t : t + 1, pl.ds(pl.multiple_of(high * LANES, LANES), LANES)]
                for t in range(8)
            ]
            now = [recv4[8 * m + high, half, at, :] for m in range(16)]
            old = [None] * 16
            for m in range(9, 16):
                old[m] = jnp.where(first_row, edge_row(high, m), pltpu.roll(now[m], 1, 0))
            for m in range(16):
                total = weights[0] * now[m]
                for t in range(1, 8):
                    total = total + weights[t] * (now[m - t] if m >= t else old[m - t + 16])
                work[16 * high + m, half, at, :] = total
            return carry

        lax.fori_loop(0, 8, one_position, 0)

        def some_frames(step, carry):
            ms = [8 * step + n for n in range(8)]
            given = [[(work[16 * high + m, half, at, :],) for high in range(8)] for m in ms]
            done = [small_dft(values, -1) for values in given]
            for m, values in zip(ms, done):
                for a, value in enumerate(values):
                    turn = (
                        out_turn[2 * half, a : a + 1, :],
                        out_turn[2 * half + 1, a : a + 1, :],
                    )
                    frames[part, a, half, pl.ds(m, TILE, stride=16), :] = packed_times(
                        value[0], turn
                    )
            return carry

        lax.fori_loop(0, 2, some_frames, 0)

    def ready_copy(part):
        return pltpu.make_async_copy(gathered.at[part], ready.at[part - 1], out_sem.at[part])

    def finish_parts(parts):
        classes = 2 // len(parts)

        def some_classes(step, carry):
            done = []
            for group in (2 * step, 2 * step + 1):
                each = [(p, classes * group + n) for n in range(classes) for p in parts]
                both = frames_dft(
                    lanes_out,
                    *[jnp.concatenate([frames[p, a, c] for p, a in each]) for c in range(2)],
                )
                done.append((each, both))
            for each, both in done:
                for c in range(2):
                    for n, (p, a) in enumerate(each):
                        gathered[p, c, pl.ds(a, 128, stride=8), :] = both[
                            c * 128 : c * 128 + 128, n * LANES : n * LANES + LANES
                        ]
            return carry

        lax.fori_loop(0, 4 // classes, some_classes, 0)
        for p in parts:
            ready_copy(p).start()

    wait4(0, 0, 3)
    for part in (3, 2, 1):
        filter_part(0, part)
    wait4(1, 3, 1)
    send_span(1)
    send4_tiles(1, 0, 1)
    span_copies[0].wait_recv()
    filter_part(0, 0)

    def wait_edges(count):
        ref = edge_recv.at[pl.ds(0, count)]
        pltpu.make_async_copy(ref, ref, edge_sem).wait()

    pl.when(with_edges)(lambda: wait_edges(DEVICES - FIRST_EDGE - 1))
    pl.when(jnp.logical_not(with_edges))(lambda: wait_edges(DEVICES - FIRST_EDGE))
    filter_part(1, 3)
    wait4(1, 2, 1)
    filter_part(1, 2)
    finish_parts((2, 3))
    wait4(1, 1, 1)
    filter_part(1, 1)
    finish_parts((1,))
    wait4(1, 0, 1)
    span_copies[1].wait_recv()
    filter_part(1, 0)
    late_copy = pltpu.make_async_copy(frames.at[0], late, out_sem.at[0])
    late_copy.start()
    for part in range(1, PARTS):
        ready_copy(part).wait()
    late_copy.wait()
    for copy in span_copies:
        copy.wait_send()

    def wait_edges_sent():
        ref = edge_recv.at[pl.ds(0, DEVICES - 1)]
        pltpu.make_async_copy(ref, ref, send_sems.at[5]).wait()

    pl.when(with_edges)(wait_edges_sent)
    pieces = recv1.at[pl.ds(0, DEVICES - 1)]
    for at in (0, 2, 3, 4):
        pltpu.make_async_copy(pieces, pieces, send_sems.at[at]).wait()
    pltpu.make_async_copy(phase_all, phase_all, send_sems.at[1]).wait()


def last_kernel(late, ready, lanes_out, result, frames, passing, gathered, matrix, sems, more):
    frame_copies = [pltpu.make_async_copy(late.at[a], frames.at[a], sems.at[a]) for a in range(8)]
    matrix_copy = pltpu.make_async_copy(lanes_out, matrix, more.at[0])
    pass_in = [
        pltpu.make_async_copy(ready.at[n], passing.at[n], more.at[1 + n]) for n in range(3)
    ]

    def to_result(source, column, sem):
        return pltpu.make_async_copy(source, result.at[:, :, pl.ds(column * LANES, LANES)], sem)

    passed = [to_result(passing.at[n], 1 + n, more.at[4 + n]) for n in range(3)]
    computed = to_result(gathered, 0, more.at[7])
    matrix_copy.start()
    for copy in frame_copies + pass_in:
        copy.start()
    matrix_copy.wait()
    for a in range(0, 8, 2):
        frame_copies[a].wait()
        frame_copies[a + 1].wait()
        both = frames_dft(
            matrix, *[jnp.concatenate([frames[a, c], frames[a + 1, c]]) for c in range(2)]
        )
        for c in range(2):
            for n in range(2):
                gathered[c, pl.ds(a + n, 128, stride=8), :] = both[
                    c * 128 : c * 128 + 128, n * LANES : n * LANES + LANES
                ]
        if a < 6:
            pass_in[a // 2].wait()
            passed[a // 2].start()
    computed.start()
    for copy in passed + [computed]:
        copy.wait()


def dft_parts(size, sign, scale=1.0):
    digits = np.arange(size)
    angle = sign * 2.0 * np.pi * ((digits[:, None] * digits[None, :]) % size) / size
    return scale * np.cos(angle), scale * np.sin(angle)


def bf16_halves(matrix):
    matrix = np.asarray(matrix, np.float32)
    high = matrix.astype(BF16)
    return high, (matrix - high.astype(np.float32)).astype(BF16)


BY_HALVES = np.concatenate([c * LANES + h * HALF + np.arange(HALF) for h in (0, 1) for c in (0, 1)])


def beside(matrix):
    high, low = bf16_halves(matrix)
    return np.concatenate([high, high, low], axis=1)


def above(matrix):
    high, low = bf16_halves(matrix)
    return np.concatenate([high, high, low], axis=0)


def left_matrix(size, sign):
    c, s = dft_parts(size, sign)
    return np.block([[c, -s], [s, c]])


def right_matrix(size, sign, scale=1.0):
    c, s = dft_parts(size, sign, scale)
    return np.block([[c, s], [-s, c]])


def turn_table(rows, cols, sign):
    whole = rows * cols
    angle = sign * 2.0 * np.pi * (np.arange(rows)[:, None] * np.arange(cols)[None, :]) / whole
    return np.stack([np.cos(angle), np.sin(angle)]).astype(np.float32)


def packed_table(rows, cols, sign):
    c, s = turn_table(rows, cols, sign)
    each = []
    for half in (slice(0, HALF), slice(HALF, LANES)):
        each.append(np.concatenate([c[:, half], c[:, half]], axis=1))
        each.append(np.concatenate([-s[:, half], s[:, half]], axis=1))
    return np.stack(each)


def local(voltage, chirp_phase, filter_taps):
    constants = [
        beside(left_matrix(ROWS, -1)),
        beside(np.concatenate(dft_parts(ROWS, 1), axis=1)),
        above(right_matrix(LANES, -1)),
        above(right_matrix(LANES, 1, 2.0**-LOG_TOTAL)[:, BY_HALVES]),
        beside(left_matrix(LANES, -1)[:, BY_HALVES]),
        turn_table(128, LANES, -1),
        packed_table(128, LANES, 1),
        packed_table(8, LANES, -1),
    ]
    blocks = pltpu.VMEM((DEVICES, 2, ROWS, LANES), F32)
    phases = pltpu.VMEM((DEVICES, ROWS, LANES), F32)
    in_hbm = pl.BlockSpec(memory_space=pl.ANY)
    given = [filter_taps] + [jnp.asarray(c) for c in constants]
    late, ready = pl.pallas_call(
        kernel,
        out_shape=[
            jax.ShapeDtypeStruct((8, 2, 128, LANES), F32),
            jax.ShapeDtypeStruct((3, 2, 1024, LANES), F32),
        ],
        in_specs=[in_hbm] * (2 + len(given)),
        out_specs=[in_hbm] * 2,
        scratch_shapes=[pltpu.VMEM(c.shape, c.dtype) for c in given]
        + [blocks] * 8
        + [pltpu.VMEM((DEVICES, 4096), F32)]
        + [phases] * 2
        + [blocks] * 3
        + [
            pltpu.VMEM((DEVICES, 2, TILE, LANES), F32),
            pltpu.VMEM((DEVICES, TILE, 2 * LANES), F32),
            pltpu.VMEM((DEVICES, 3, LANES), F32),
            pltpu.VMEM((DEVICES, 3, LANES), F32),
            pltpu.VMEM((2, DEVICES - FIRST_EDGE, LANES), F32),
            pltpu.VMEM((2, DEVICES - FIRST_EDGE, LANES), F32),
            pltpu.VMEM((2, 8, 1024), F32),
            pltpu.SemaphoreType.DMA((2,)),
            pltpu.SemaphoreType.DMA((PARTS,)),
            pltpu.SemaphoreType.DMA((PARTS,)),
            pltpu.SemaphoreType.DMA(((PARTS + 1) * GROUPS,)),
            pltpu.SemaphoreType.DMA((2 * PARTS,)),
            pltpu.SemaphoreType.DMA,
            pltpu.SemaphoreType.DMA,
            pltpu.SemaphoreType.DMA((2,)),
            pltpu.SemaphoreType.DMA((8,)),
            pltpu.SemaphoreType.DMA((PARTS,)),
            pltpu.SemaphoreType.DMA((CONSTANTS,)),
            pltpu.SemaphoreType.REGULAR,
        ],
        compiler_params=pltpu.CompilerParams(
            collective_id=0, has_side_effects=True, vmem_limit_bytes=67043328
        ),
    )(voltage, chirp_phase, *given)
    return pl.pallas_call(
        last_kernel,
        out_shape=jax.ShapeDtypeStruct((2, 1024, 512), F32),
        in_specs=[in_hbm] * 3,
        out_specs=in_hbm,
        scratch_shapes=[
            pltpu.VMEM((8, 2, 128, LANES), F32),
            pltpu.VMEM((3, 2, 1024, LANES), F32),
            pltpu.VMEM((2, 1024, LANES), F32),
            pltpu.VMEM((256, 768), BF16),
            pltpu.SemaphoreType.DMA((8,)),
            pltpu.SemaphoreType.DMA((8,)),
        ],
        compiler_params=pltpu.CompilerParams(vmem_limit_bytes=67043328),
    )(late, ready, given[5])


def solution(mesh):
    in_specs = (P(None, ("row", "col"), None), P(("row", "col"), None), P())
    out_specs = P(None, None, ("row", "col"))
    return jax.shard_map(local, mesh=mesh, in_specs=in_specs, out_specs=out_specs, check_vma=False)
```

```python
import math
import random

import jax
import jax.numpy as jnp
import numpy as np
from jax import lax
from jax.experimental import pallas as pl
from jax.experimental.pallas import tpu as pltpu
from jax.sharding import PartitionSpec as P

DEVICES = 128
ROWS = 32
TILE = 8
PARTS = ROWS // TILE
LANES = 128
HALF = LANES // 2
LOG_TOTAL = 26
GROUPS = DEVICES // 16
CONSTANTS = 9
FIRST_EDGE = 72
IN_STEPS = [
    (n % 4, (n % 4 + n // 4) % 4, (n % 4 + n // 4 + n // 16) % 4, n // 64)
    for n in range(1, DEVICES)
]
FAR_FIRST = list(IN_STEPS)
random.Random(1).shuffle(FAR_FIRST)
FAR_FIRST.sort(key=lambda offset: -sum(min(d, 4 - d) for d in offset[:3]))
BY_MESH = pl.DeviceIdType.MESH
F32 = jnp.float32
BF16 = jnp.bfloat16


def device_at(z, y, x, core):
    return z * 8 + lax.rem(y, 2) * 4 + x, (y // 2) * 2 + core


def partner(here, step, way=1):
    z, y, x, core = here
    low = lax.rem(step, 4)
    mid = low + lax.rem(step // 4, 4)
    high = mid + lax.rem(step // 16, 4)
    return device_at(
        lax.rem(z + way * low, 4),
        lax.rem(y + way * mid, 4),
        lax.rem(x + way * high, 4),
        lax.rem(core + step // 64, 2),
    )


def times(a, b):
    return a[0] * b[0] - a[1] * b[1], a[0] * b[1] + a[1] * b[0]


def plus(a, b):
    return tuple(x + y for x, y in zip(a, b))


def minus(a, b):
    return tuple(x - y for x, y in zip(a, b))


def turned(a, part, whole, sign):
    part = part % whole
    eighths = 8 * part / whole
    if eighths == 0:
        return a
    if eighths == 2:
        return (-a[1], a[0]) if sign > 0 else (a[1], -a[0])
    if eighths == 4:
        return -a[0], -a[1]
    if eighths == 6:
        return (a[1], -a[0]) if sign > 0 else (-a[1], a[0])
    angle = sign * 2.0 * math.pi * part / whole
    cos_part, sin_part = math.cos(angle), math.sin(angle)
    if eighths in (1, 3, 5, 7):
        half = math.sqrt(0.5)
        c = half if cos_part > 0 else -half
        same = (cos_part > 0) == (sin_part > 0)
        if same:
            return (a[0] - a[1]) * c, (a[0] + a[1]) * c
        return (a[0] + a[1]) * c, (a[1] - a[0]) * c
    return a[0] * cos_part - a[1] * sin_part, a[0] * sin_part + a[1] * cos_part


def lane_sign(shape):
    return jnp.where(lax.broadcasted_iota(jnp.int32, shape, len(shape) - 1) < HALF, -1.0, 1.0)


def swapped(x):
    return pltpu.roll(x, HALF, x.ndim - 1)


def packed_times(x, turn):
    return x * turn[0] + swapped(x) * turn[1]


def packed_turned(a, part, whole, sign):
    part = part % whole
    angle = sign * 2.0 * math.pi * part / whole
    (x,) = a
    if part == 0:
        return a
    if 2 * part == whole:
        return (-x,)
    if 4 * part in (whole, 3 * whole):
        up = (4 * part == whole) == (sign > 0)
        return (swapped(x) * (lane_sign(x.shape) if up else -lane_sign(x.shape)),)
    return (math.cos(angle) * x + swapped(x) * (math.sin(angle) * lane_sign(x.shape)),)


def small_dft(xs, sign):
    n = len(xs)
    turn = turned if len(xs[0]) == 2 else packed_turned
    if n == 1:
        return xs
    if n == 2:
        return [plus(xs[0], xs[1]), minus(xs[0], xs[1])]
    parts = [small_dft(xs[r::4], sign) for r in range(4)]
    out = [None] * n
    for k in range(n // 4):
        a, b, c, d = (turn(parts[r][k], r * k, n, sign) for r in range(4))
        ac, bd = plus(a, c), plus(b, d)
        ac_, bd_ = minus(a, c), turn(minus(b, d), 1, 4, sign)
        out[k] = plus(ac, bd)
        out[k + n // 4] = plus(ac_, bd_)
        out[k + n // 2] = minus(ac, bd)
        out[k + 3 * n // 4] = minus(ac_, bd_)
    return out


def block_dft(load, scratch, finish, sign):
    for low in range(8):
        values = small_dft([load(8 * high + low) for high in range(16)], sign)
        for k, value in enumerate(values):
            turn = turned if len(value) == 2 else packed_turned
            value = turn(value, low * k, 128, sign)
            for c, x in enumerate(value):
                scratch[8 * k + low, c] = x
    parts = range(len(value))
    together = 1 if len(value) == 2 else 4

    def second(step, carry):
        ks = [together * step + n for n in range(together)]
        given = [
            [tuple(scratch[8 * k + low, c] for c in parts) for low in range(8)] for k in ks
        ]
        done = [small_dft(values, sign) for values in given]
        for k, values in zip(ks, done):
            for high, value in enumerate(values):
                finish(k + 16 * high, value)
        return carry

    lax.fori_loop(0, 16 // together, second, 0)


def quarter_sincos(angle, quarter):
    square = angle * angle
    sin_part = angle * (
        1.0 + square * (-1.0 / 6 + square * (1.0 / 120 + square * (-1.0 / 5040 + square / 362880)))
    )
    cos_part = 1.0 + square * (
        -0.5 + square * (1.0 / 24 + square * (-1.0 / 720 + square * (1.0 / 40320)))
    )
    odd = (quarter & 1) == 1
    first = jnp.where(odd, sin_part, cos_part)
    second = jnp.where(odd, cos_part, sin_part)
    return (
        jnp.where(((quarter + 1) & 2) == 2, -first, first),
        jnp.where((quarter & 2) == 2, -second, second),
    )


def unit(product, log_whole):
    quarter = (product + (1 << (log_whole - 3))) >> (log_whole - 2)
    rest = product - (quarter << (log_whole - 2))
    return quarter_sincos(rest.astype(F32) * (2.0 * math.pi / 2**log_whole), quarter)


def phase_unit(phase):
    quarter = jnp.floor(phase * (2.0 / math.pi) + 0.5)
    high = float(np.float32(1.5703125))
    angle = (phase - quarter * high) - quarter * (math.pi / 2 - high)
    return quarter_sincos(angle, quarter.astype(jnp.int32))


def halves(x):
    high = x.astype(BF16)
    return high, (x - high.astype(F32)).astype(BF16)


def frames_dft(matrix, real_part, imag_part):
    high, low = halves(jnp.concatenate([real_part, imag_part], axis=1))
    return lax.dot_general(
        matrix[...],
        jnp.concatenate([high, low, high], axis=1),
        (((1,), (1,)), ((), ())),
        preferred_element_type=F32,
    )


def kernel(
    voltage,
    phase,
    *refs,
):
    given, refs = refs[:CONSTANTS], refs[CONSTANTS:]
    late, ready, refs = refs[0], refs[1], refs[2:]
    held, refs = refs[:CONSTANTS], refs[CONSTANTS:]
    taps, rows_fwd, rows_inv, lanes_fwd, lanes_inv, lanes_out, mid_turn, mid_back, out_turn = held
    (
    recv1,
    work,
    send2,
    recv2,
    send3,
    recv3,
    send4,
    recv4,
    phase_in,
    phase_send,
    phase_recv,
    chirp,
    table_a,
    table_b,
    tiles,
    wide,
    edge_send,
    edge_recv,
    span_send,
    span_recv,
    half_taps,
    local_sem,
    sems1,
    sems2,
    sems3,
    sems4,
    phase_sem,
    edge_sem,
    span_sems,
    send_sems,
    out_sem,
    late_sem,
    given_sem,
    plane_sem,
    ) = refs
    row = lax.axis_index("row")
    col = lax.axis_index("col")
    me = row * 4 + col
    sublane = lax.broadcasted_iota(jnp.int32, (ROWS, LANES), 0)
    lane = lax.broadcasted_iota(jnp.int32, (ROWS, LANES), 1)

    phase_copy = pltpu.make_async_copy(phase, phase_in, local_sem.at[0])
    phase_copy.start()
    own_copy = pltpu.make_async_copy(
        voltage.at[:, :, pl.ds(pl.multiple_of(me * LANES, LANES), LANES)],
        recv1.at[me],
        local_sem.at[1],
    )
    own_copy.start()
    given_copies = [
        pltpu.make_async_copy(a, b, given_sem.at[n]) for n, (a, b) in enumerate(zip(given, held))
    ]
    for copy in given_copies:
        copy.start()

    place = row // 8, (col // 2) * 2 + lax.rem(row // 4, 2), lax.rem(row, 4), lax.rem(col, 2)
    z, y, x, core = place
    barrier = pltpu.get_barrier_semaphore()

    def greet_along(other):
        to = device_at(lax.rem(z + other, 4), y, x, core)
        return dict(inc=1, device_id=to, device_id_type=BY_MESH)

    for _, dy, dx, dc in (offset for offset in FAR_FIRST if offset[0] == 0):
        to = device_at(z, lax.rem(y + dy, 4), lax.rem(x + dx, 4), lax.rem(core + dc, 2))
        pl.semaphore_signal(barrier, inc=1, device_id=to, device_id_type=BY_MESH)
    for other in range(1, 4):
        pl.semaphore_signal(barrier, **greet_along(other))
    pl.semaphore_wait(barrier, 34)
    for other in range(1, 4):
        pl.semaphore_signal(plane_sem, **greet_along(other))
    pl.semaphore_wait(plane_sem, 3)

    rows_of = [
        [lax.rem(z + n, 4) * 8 for n in range(4)],
        [lax.rem(y + n, 2) * 4 for n in range(4)],
        [lax.rem(x + n, 4) for n in range(4)],
    ]
    cols_of = [
        [lax.rem(y + n, 4) // 2 * 2 for n in range(4)],
        [lax.rem(core + n, 2) for n in range(2)],
    ]

    def send_loop(source_of, target, send_sem, recv_sem):
        def one(step, carry):
            to_row, to_col = partner(place, step)
            pltpu.make_async_remote_copy(
                src_ref=source_of(to_row * 4 + to_col),
                dst_ref=target,
                send_sem=send_sem,
                recv_sem=recv_sem,
                device_id=(to_row, to_col),
                device_id_type=BY_MESH,
            ).start()
            return carry

        lax.fori_loop(1, DEVICES, one, 0)

    def send_all(order, source_of, target, send_sem, recv_sem_of):
        for n, (dz, dy, dx, dc) in enumerate(order):
            to_row = rows_of[0][dz] + rows_of[1][dy] + rows_of[2][dx]
            to_col = cols_of[0][dy] + cols_of[1][dc]
            pltpu.make_async_remote_copy(
                src_ref=source_of(to_row * 4 + to_col),
                dst_ref=target,
                send_sem=send_sem,
                recv_sem=recv_sem_of(n + 1),
                device_id=(to_row, to_col),
                device_id_type=BY_MESH,
            ).start()

    def tile_rows(part):
        return pl.ds(pl.multiple_of(part * TILE, TILE), TILE)

    def wait_part(buffer, sem):
        ref = buffer.at[pl.ds(0, DEVICES - 1), :, pl.ds(0, TILE), :]
        pltpu.make_async_copy(ref, ref, sem).wait()

    def voltage_part(part, carry):
        send_loop(
            lambda to: voltage.at[
                :, tile_rows(part), pl.ds(pl.multiple_of(to * LANES, LANES), LANES)
            ],
            recv1.at[me, :, tile_rows(part), :],
            send_sems.at[0],
            sems1.at[part],
        )
        return carry

    lax.fori_loop(0, PARTS, voltage_part, 0)

    phase_copy.wait()

    def phase_out(b, carry):
        block = phase_in[:, pl.ds(pl.multiple_of(b * LANES, LANES), LANES)]
        phase_send[:, pl.ds(b, 1), :] = jnp.transpose(block).reshape(DEVICES, 1, LANES)
        return carry

    lax.fori_loop(0, ROWS, phase_out, 0)

    send_loop(
        lambda to: phase_send.at[to],
        phase_recv.at[me],
        send_sems.at[1],
        phase_sem,
    )
    phase_recv[me] = phase_send[me]

    def fill(a, carry):
        cos_part, sin_part = unit(sublane * a, 12)
        table_a[a, 0] = cos_part
        table_a[a, 1] = -sin_part
        cos_part, sin_part = unit((a + 128 * sublane) * (128 * me + lane), LOG_TOTAL)
        table_b[a, 0] = cos_part
        table_b[a, 1] = -sin_part
        return carry

    lax.fori_loop(0, DEVICES, fill, 0)

    own_copy.wait()

    def first_part(part, carry):
        wait_part(recv1, sems1.at[part])
        at = tile_rows(part)

        def load(n):
            return recv1[n, 0, at, :], recv1[n, 1, at, :]

        def finish(k, value):
            turn = table_a[k, 0, at, :], table_a[k, 1, at, :]
            value = times(value, turn)
            work[k, 0, at, :] = value[0]
            work[k, 1, at, :] = value[1]

        block_dft(load, tiles, finish, -1)
        return carry

    lax.fori_loop(0, PARTS, first_part, 0)

    for copy in given_copies:
        copy.wait()

    first_lanes = lax.broadcasted_iota(jnp.int32, (8, LANES), 1) < HALF
    for high in range(8):
        columns = slice(high * LANES, high * LANES + LANES)
        straight = taps[:, columns]
        half_taps[0, :, columns] = jnp.where(first_lanes, straight, swapped(straight))
        half_taps[1, :, columns] = jnp.where(first_lanes, swapped(straight), straight)

    def split_dot(matrix, columns):
        high, low = halves(columns)
        return jnp.dot(
            matrix[...],
            jnp.concatenate([high, low, high], axis=0),
            preferred_element_type=F32,
        )

    def in_pairs(places):
        return zip(places[::2], places[1::2])

    def second_step(group, carry):
        done = []
        for pair in in_pairs([8 * group + n for n in range(8)]):
            both = split_dot(
                rows_fwd, jnp.concatenate([work[a].reshape(64, LANES) for a in pair], axis=1)
            )
            for n, a in enumerate(pair):
                columns = slice(n * LANES, n * LANES + LANES)
                done.append((a, (both[:ROWS, columns], both[ROWS:, columns])))
        for a, value in done:
            value = times(value, (table_b[a, 0], table_b[a, 1]))
            send2[a, 0] = value[0]
            send2[a, 1] = value[1]
        return carry

    lax.fori_loop(0, DEVICES // 8, second_step, 0)
    recv2[me] = send2[me]

    def send2_part(part, carry):
        send_loop(
            lambda to: send2.at[to, :, tile_rows(part), :],
            recv2.at[me, :, tile_rows(part), :],
            send_sems.at[2],
            sems2.at[part],
        )
        return carry

    lax.fori_loop(0, PARTS, send2_part, 0)

    phase_all = phase_recv.at[pl.ds(0, DEVICES - 1)]
    pltpu.make_async_copy(phase_all, phase_all, phase_sem).wait()

    def phase_back(b, carry):
        block = phase_recv[:, pl.ds(b, 1), :].reshape(DEVICES, LANES)
        cos_part, sin_part = phase_unit(jnp.transpose(block))
        chirp[:, 0, pl.ds(b, 1), :] = cos_part.reshape(DEVICES, 1, LANES)
        chirp[:, 1, pl.ds(b, 1), :] = sin_part.reshape(DEVICES, 1, LANES)
        return carry

    lax.fori_loop(0, ROWS, phase_back, 0)

    back_tables = table_b, work
    sign = lane_sign((ROWS, LANES))

    def refill(h, carry):
        for half in range(2):
            at = 128 * h + HALF * half + (lane & (HALF - 1))
            cos_part, sin_part = unit((me + 128 * sublane) * at, LOG_TOTAL)
            back_tables[half][h, 0] = cos_part
            back_tables[half][h, 1] = sin_part * sign
        return carry

    lax.fori_loop(0, DEVICES, refill, 0)

    def middle_part(part, carry):
        wait_part(recv2, sems2.at[part])
        at = tile_rows(part)

        def load(n):
            return recv2[n, 0, at, :], recv2[n, 1, at, :]

        def finish(k, value):
            turn = mid_turn[0, pl.ds(k, 1), :], mid_turn[1, pl.ds(k, 1), :]
            value = times(value, turn)
            wide[k, :, :LANES] = value[0]
            wide[k, :, LANES:] = value[1]

        block_dft(load, tiles, finish, -1)

        def lanes_step(group, inner):
            rows = pl.ds(group * 32, 32)
            high, low = halves(wide[rows].reshape(32 * TILE, 2 * LANES))
            there = jnp.dot(
                jnp.concatenate([high, low, high], axis=1),
                lanes_fwd[...],
                preferred_element_type=F32,
            )
            turn = (
                chirp[rows, 0, at, :].reshape(32 * TILE, LANES),
                chirp[rows, 1, at, :].reshape(32 * TILE, LANES),
            )
            there = times((there[:, :LANES], there[:, LANES:]), turn)
            high, low = halves(jnp.concatenate(there, axis=1))
            back = jnp.dot(
                jnp.concatenate([high, low, high], axis=1),
                lanes_inv[...],
                preferred_element_type=F32,
            )
            wide[rows] = back.reshape(32, TILE, 2 * LANES)
            return inner

        lax.fori_loop(0, 4, lanes_step, 0)

        for half in range(2):
            columns = slice(half * LANES, half * LANES + LANES)

            def load_back(n, half=half, columns=columns):
                turn = mid_back[2 * half, pl.ds(n, 1), :], mid_back[2 * half + 1, pl.ds(n, 1), :]
                return (packed_times(wide[n, :, columns], turn),)

            def finish_back(k, value, half=half):
                table = back_tables[half]
                send3[k, half, at, :] = packed_times(
                    value[0], (table[k, 0, at, :], table[k, 1, at, :])
                )

            block_dft(load_back, tiles, finish_back, 1)
            recv3[me, half, at, :] = send3[me, half, at, :]
        send3_rows(0, at, part * GROUPS)
        return carry

    def send3_rows(half, rows, first_sem):
        send_all(
            IN_STEPS,
            lambda to: send3.at[to, half, rows, :],
            recv3.at[me, half, rows, :],
            send_sems.at[3],
            lambda n: sems3.at[first_sem + n // 16],
        )

    lax.fori_loop(0, PARTS, middle_part, 0)
    send3_rows(1, slice(0, ROWS), PARTS * GROUPS)

    def third_step(half, group, eighth):
        places = []
        for n in range(8):
            from_row, from_col = partner(place, 16 * group + 8 * eighth + n, 3)
            places.append(from_row * 4 + from_col)
        done = []
        for pair in in_pairs(places):
            straight = [recv3[a, half] for a in pair]
            turned_up = [swapped(value) * sign for value in straight]
            both = split_dot(
                rows_inv,
                jnp.concatenate(
                    [jnp.concatenate(straight, axis=1), jnp.concatenate(turned_up, axis=1)], axis=0
                ),
            )
            for n, a in enumerate(pair):
                done.append((a, both[:, n * LANES : n * LANES + LANES]))
        for a, value in done:
            work[a, half] = packed_times(value, (table_a[a, 0], -sign * table_a[a, 1]))

    def third_group(half, group, count):
        def wait_rows(rows, sem):
            ref = recv3.at[pl.ds(0, count), half, pl.ds(0, rows), :]
            pltpu.make_async_copy(ref, ref, sems3.at[sem + group]).wait()

        def wait_one(part, inner):
            wait_rows(TILE, part * GROUPS)
            return inner

        if half == 0:
            lax.fori_loop(0, PARTS, wait_one, 0)
        else:
            wait_rows(ROWS, PARTS * GROUPS)

        def one(eighth, inner):
            third_step(half, group, eighth)
            return inner

        lax.fori_loop(0, 2, one, 0)

    def third_half(half):
        def later_group(group, carry):
            third_group(half, group, 16)
            return carry

        third_group(half, 0, 15)
        lax.fori_loop(1, GROUPS, later_group, 0)

    def fourth_part(half, part):
        at = slice(part * TILE, part * TILE + TILE)

        def load(n):
            return (work[n, half, at, :],)

        def finish(k, value):
            send4[k, half, at, :] = value[0]
            if half == 1 and part < 2:
                edge_send[k, part : part + 1, :] = value[0][TILE - 1 :]

        block_dft(load, tiles, finish, 1)
        recv4[me, half, at, :] = send4[me, half, at, :]

    def send4_tiles(half, first, count):
        at = slice(first * TILE, (first + count) * TILE)
        send_all(
            FAR_FIRST,
            lambda to: send4.at[to, half, at, :],
            recv4.at[me, half, at, :],
            send_sems.at[4],
            lambda n: sems4.at[half * PARTS + first],
        )

    def edge_pieces():
        send_all(
            FAR_FIRST,
            lambda to: edge_send.at[to],
            edge_recv.at[me],
            send_sems.at[5],
            lambda n: edge_sem,
        )

    def wait4(half, first, count):
        ref = recv4.at[pl.ds(0, DEVICES - 1), half, pl.ds(0, count * TILE), :]
        pltpu.make_async_copy(ref, ref, sems4.at[half * PARTS + first]).wait()

    following = lax.rem(me + 1, DEVICES)
    span_copies = [
        pltpu.make_async_remote_copy(
            src_ref=span_send.at[half],
            dst_ref=span_recv.at[half],
            send_sem=send_sems.at[6 + half],
            recv_sem=span_sems.at[half],
            device_id=(following // 4, lax.rem(following, 4)),
            device_id_type=BY_MESH,
        )
        for half in range(2)
    ]

    def send_span(half):
        def span_row(j, carry):
            span_send[half, pl.ds(j, 1), :] = recv4[FIRST_EDGE + j, half, ROWS - 1 :, :]
            return carry

        lax.fori_loop(0, DEVICES - FIRST_EDGE, span_row, 0)
        span_copies[half].start()

    with_edges = me >= FIRST_EDGE
    third_half(0)
    fourth_part(0, 3)
    send4_tiles(0, 3, 1)
    for part in (2, 1, 0):
        fourth_part(0, part)
    send4_tiles(0, 0, 3)
    third_half(1)
    for part in (3, 2, 1, 0):
        fourth_part(1, part)
    edge_recv[me] = edge_send[me]
    wait4(0, 3, 1)
    send_span(0)
    pl.when(with_edges)(edge_pieces)
    send4_tiles(1, 3, 1)
    send4_tiles(1, 2, 1)
    send4_tiles(1, 1, 1)

    first_row = lax.broadcasted_iota(jnp.int32, (TILE, LANES), 0) == 0
    ahead = me > 0
    frames = table_a.reshape(PARTS, 8, 2, 128, LANES)
    gathered = table_b.reshape(PARTS, 2, 1024, LANES)

    def filter_part(half, part):
        at = slice(part * TILE, part * TILE + TILE)

        def edge_row(high, m):
            if part == 0:
                edge = span_recv[half, pl.ds(8 * m + high - FIRST_EDGE, 1), :]
                return jnp.where(ahead, edge, 0.0)
            if half == 1 and part < 3:
                return edge_recv[8 * m + high, part - 1 : part, :]
            return recv4[8 * m + high, half, part * TILE - 1 : part * TILE, :]

        def one_position(high, carry):
            weights = [
                half_taps[half, t : t + 1, pl.ds(pl.multiple_of(high * LANES, LANES), LANES)]
                for t in range(8)
            ]
            now = [recv4[8 * m + high, half, at, :] for m in range(16)]
            old = [None] * 16
            for m in range(9, 16):
                old[m] = jnp.where(first_row, edge_row(high, m), pltpu.roll(now[m], 1, 0))
            for m in range(16):
                total = weights[0] * now[m]
                for t in range(1, 8):
                    total = total + weights[t] * (now[m - t] if m >= t else old[m - t + 16])
                work[16 * high + m, half, at, :] = total
            return carry

        lax.fori_loop(0, 8, one_position, 0)

        def some_frames(step, carry):
            ms = [8 * step + n for n in range(8)]
            given = [[(work[16 * high + m, half, at, :],) for high in range(8)] for m in ms]
            done = [small_dft(values, -1) for values in given]
            for m, values in zip(ms, done):
                for a, value in enumerate(values):
                    turn = (
                        out_turn[2 * half, a : a + 1, :],
                        out_turn[2 * half + 1, a : a + 1, :],
                    )
                    frames[part, a, half, pl.ds(m, TILE, stride=16), :] = packed_times(
                        value[0], turn
                    )
            return carry

        lax.fori_loop(0, 2, some_frames, 0)

    def ready_copy(part):
        return pltpu.make_async_copy(gathered.at[part], ready.at[part - 1], out_sem.at[part])

    def finish_parts(parts):
        classes = 2 // len(parts)

        def some_classes(step, carry):
            done = []
            for group in (2 * step, 2 * step + 1):
                each = [(p, classes * group + n) for n in range(classes) for p in parts]
                both = frames_dft(
                    lanes_out,
                    *[jnp.concatenate([frames[p, a, c] for p, a in each]) for c in range(2)],
                )
                done.append((each, both))
            for each, both in done:
                for c in range(2):
                    for n, (p, a) in enumerate(each):
                        gathered[p, c, pl.ds(a, 128, stride=8), :] = both[
                            c * 128 : c * 128 + 128, n * LANES : n * LANES + LANES
                        ]
            return carry

        lax.fori_loop(0, 4 // classes, some_classes, 0)
        for p in parts:
            ready_copy(p).start()

    late_copies = [
        pltpu.make_async_copy(frames.at[0, :, half], late.at[:, half], late_sem.at[half])
        for half in range(2)
    ]
    wait4(0, 0, 3)
    for part in (3, 2, 1):
        filter_part(0, part)
    wait4(1, 3, 1)
    send_span(1)
    send4_tiles(1, 0, 1)
    span_copies[0].wait_recv()
    filter_part(0, 0)
    late_copies[0].start()

    def wait_edges(count):
        ref = edge_recv.at[pl.ds(0, count)]
        pltpu.make_async_copy(ref, ref, edge_sem).wait()

    pl.when(with_edges)(lambda: wait_edges(DEVICES - FIRST_EDGE - 1))
    pl.when(jnp.logical_not(with_edges))(lambda: wait_edges(DEVICES - FIRST_EDGE))
    wait4(1, 2, 1)
    filter_part(1, 3)
    filter_part(1, 2)
    finish_parts((2, 3))
    wait4(1, 1, 1)
    filter_part(1, 1)
    finish_parts((1,))
    wait4(1, 0, 1)
    span_copies[1].wait_recv()
    filter_part(1, 0)
    late_copies[1].start()
    for part in range(1, PARTS):
        ready_copy(part).wait()
    for copy in late_copies:
        copy.wait()
    for copy in span_copies:
        copy.wait_send()

    def wait_edges_sent():
        ref = edge_recv.at[pl.ds(0, DEVICES - 1)]
        pltpu.make_async_copy(ref, ref, send_sems.at[5]).wait()

    pl.when(with_edges)(wait_edges_sent)
    pieces = recv1.at[pl.ds(0, DEVICES - 1)]
    for at in (0, 2, 3, 4):
        pltpu.make_async_copy(pieces, pieces, send_sems.at[at]).wait()
    pltpu.make_async_copy(phase_all, phase_all, send_sems.at[1]).wait()


def last_kernel(late, ready, lanes_out, result, frames, passing, gathered, matrix, sems, more):
    frame_copies = [
        pltpu.make_async_copy(late.at[pl.ds(4 * n, 4)], frames.at[pl.ds(4 * n, 4)], sems.at[n])
        for n in range(2)
    ]
    matrix_copy = pltpu.make_async_copy(lanes_out, matrix, more.at[0])
    pass_in = [
        pltpu.make_async_copy(ready.at[n], passing.at[n], more.at[1 + n]) for n in range(3)
    ]

    def to_result(source, column, sem):
        return pltpu.make_async_copy(source, result.at[:, :, pl.ds(column * LANES, LANES)], sem)

    passed = [to_result(passing.at[n], 1 + n, more.at[4 + n]) for n in range(3)]
    computed = to_result(gathered, 0, more.at[7])
    matrix_copy.start()
    for copy in frame_copies + pass_in:
        copy.start()
    matrix_copy.wait()
    for n in range(2):
        frame_copies[n].wait()
        pairs = [(4 * n, 4 * n + 1), (4 * n + 2, 4 * n + 3)]
        done = [
            frames_dft(matrix, *[jnp.concatenate([frames[a, c] for a in pair]) for c in range(2)])
            for pair in pairs
        ]
        for pair, both in zip(pairs, done):
            for c in range(2):
                for side, a in enumerate(pair):
                    gathered[c, pl.ds(a, 128, stride=8), :] = both[
                        c * 128 : c * 128 + 128, side * LANES : side * LANES + LANES
                    ]
        if n == 0:
            for copy_in, copy_out in zip(pass_in, passed):
                copy_in.wait()
                copy_out.start()
    computed.start()
    for copy in passed + [computed]:
        copy.wait()


def dft_parts(size, sign, scale=1.0):
    digits = np.arange(size)
    angle = sign * 2.0 * np.pi * ((digits[:, None] * digits[None, :]) % size) / size
    return scale * np.cos(angle), scale * np.sin(angle)


def bf16_halves(matrix):
    matrix = np.asarray(matrix, np.float32)
    high = matrix.astype(BF16)
    return high, (matrix - high.astype(np.float32)).astype(BF16)


BY_HALVES = np.concatenate([c * LANES + h * HALF + np.arange(HALF) for h in (0, 1) for c in (0, 1)])


def beside(matrix):
    high, low = bf16_halves(matrix)
    return np.concatenate([high, high, low], axis=1)


def above(matrix):
    high, low = bf16_halves(matrix)
    return np.concatenate([high, high, low], axis=0)


def left_matrix(size, sign):
    c, s = dft_parts(size, sign)
    return np.block([[c, -s], [s, c]])


def right_matrix(size, sign, scale=1.0):
    c, s = dft_parts(size, sign, scale)
    return np.block([[c, s], [-s, c]])


def turn_table(rows, cols, sign):
    whole = rows * cols
    angle = sign * 2.0 * np.pi * (np.arange(rows)[:, None] * np.arange(cols)[None, :]) / whole
    return np.stack([np.cos(angle), np.sin(angle)]).astype(np.float32)


def packed_table(rows, cols, sign):
    c, s = turn_table(rows, cols, sign)
    each = []
    for half in (slice(0, HALF), slice(HALF, LANES)):
        each.append(np.concatenate([c[:, half], c[:, half]], axis=1))
        each.append(np.concatenate([-s[:, half], s[:, half]], axis=1))
    return np.stack(each)


def local(voltage, chirp_phase, filter_taps):
    constants = [
        beside(left_matrix(ROWS, -1)),
        beside(np.concatenate(dft_parts(ROWS, 1), axis=1)),
        above(right_matrix(LANES, -1)),
        above(right_matrix(LANES, 1, 2.0**-LOG_TOTAL)[:, BY_HALVES]),
        beside(left_matrix(LANES, -1)[:, BY_HALVES]),
        turn_table(128, LANES, -1),
        packed_table(128, LANES, 1),
        packed_table(8, LANES, -1),
    ]
    blocks = pltpu.VMEM((DEVICES, 2, ROWS, LANES), F32)
    phases = pltpu.VMEM((DEVICES, ROWS, LANES), F32)
    in_hbm = pl.BlockSpec(memory_space=pl.ANY)
    given = [filter_taps] + [jnp.asarray(c) for c in constants]
    late, ready = pl.pallas_call(
        kernel,
        out_shape=[
            jax.ShapeDtypeStruct((8, 2, 128, LANES), F32),
            jax.ShapeDtypeStruct((3, 2, 1024, LANES), F32),
        ],
        in_specs=[in_hbm] * (2 + len(given)),
        out_specs=[in_hbm] * 2,
        scratch_shapes=[pltpu.VMEM(c.shape, c.dtype) for c in given]
        + [blocks] * 8
        + [pltpu.VMEM((DEVICES, 4096), F32)]
        + [phases] * 2
        + [blocks] * 3
        + [
            pltpu.VMEM((DEVICES, 2, TILE, LANES), F32),
            pltpu.VMEM((DEVICES, TILE, 2 * LANES), F32),
            pltpu.VMEM((DEVICES, 2, LANES), F32),
            pltpu.VMEM((DEVICES, 2, LANES), F32),
            pltpu.VMEM((2, DEVICES - FIRST_EDGE, LANES), F32),
            pltpu.VMEM((2, DEVICES - FIRST_EDGE, LANES), F32),
            pltpu.VMEM((2, 8, 1024), F32),
            pltpu.SemaphoreType.DMA((2,)),
            pltpu.SemaphoreType.DMA((PARTS,)),
            pltpu.SemaphoreType.DMA((PARTS,)),
            pltpu.SemaphoreType.DMA(((PARTS + 1) * GROUPS,)),
            pltpu.SemaphoreType.DMA((2 * PARTS,)),
            pltpu.SemaphoreType.DMA,
            pltpu.SemaphoreType.DMA,
            pltpu.SemaphoreType.DMA((2,)),
            pltpu.SemaphoreType.DMA((8,)),
            pltpu.SemaphoreType.DMA((PARTS,)),
            pltpu.SemaphoreType.DMA((2,)),
            pltpu.SemaphoreType.DMA((CONSTANTS,)),
            pltpu.SemaphoreType.REGULAR,
        ],
        compiler_params=pltpu.CompilerParams(
            collective_id=0, has_side_effects=True, vmem_limit_bytes=67043328
        ),
    )(voltage, chirp_phase, *given)
    return pl.pallas_call(
        last_kernel,
        out_shape=jax.ShapeDtypeStruct((2, 1024, 512), F32),
        in_specs=[in_hbm] * 3,
        out_specs=in_hbm,
        scratch_shapes=[
            pltpu.VMEM((8, 2, 128, LANES), F32),
            pltpu.VMEM((3, 2, 1024, LANES), F32),
            pltpu.VMEM((2, 1024, LANES), F32),
            pltpu.VMEM((256, 768), BF16),
            pltpu.SemaphoreType.DMA((8,)),
            pltpu.SemaphoreType.DMA((8,)),
        ],
        compiler_params=pltpu.CompilerParams(vmem_limit_bytes=67043328),
    )(late, ready, given[5])


def solution(mesh):
    in_specs = (P(None, ("row", "col"), None), P(("row", "col"), None), P())
    out_specs = P(None, None, ("row", "col"))
    return jax.shard_map(local, mesh=mesh, in_specs=in_specs, out_specs=out_specs, check_vma=False)
```

```python
import math
import random

import jax
import jax.numpy as jnp
import numpy as np
from jax import lax
from jax.experimental import pallas as pl
from jax.experimental.pallas import tpu as pltpu
from jax.sharding import PartitionSpec as P

DEVICES = 128
ROWS = 32
TILE = 8
PARTS = ROWS // TILE
LANES = 128
HALF = LANES // 2
LOG_TOTAL = 26
GROUPS = DEVICES // 16
CONSTANTS = 9
FIRST_EDGE = 72
IN_STEPS = [
    (n % 4, (n % 4 + n // 4) % 4, (n % 4 + n // 4 + n // 16) % 4, n // 64)
    for n in range(1, DEVICES)
]
FAR_FIRST = list(IN_STEPS)
random.Random(1).shuffle(FAR_FIRST)
FAR_FIRST.sort(key=lambda offset: -sum(min(d, 4 - d) for d in offset[:3]))
BY_MESH = pl.DeviceIdType.MESH
F32 = jnp.float32
BF16 = jnp.bfloat16


def device_at(z, y, x, core):
    return z * 8 + lax.rem(y, 2) * 4 + x, (y // 2) * 2 + core


def partner(here, step, way=1):
    z, y, x, core = here
    low = lax.rem(step, 4)
    mid = low + lax.rem(step // 4, 4)
    high = mid + lax.rem(step // 16, 4)
    return device_at(
        lax.rem(z + way * low, 4),
        lax.rem(y + way * mid, 4),
        lax.rem(x + way * high, 4),
        lax.rem(core + step // 64, 2),
    )


def times(a, b):
    return a[0] * b[0] - a[1] * b[1], a[0] * b[1] + a[1] * b[0]


def plus(a, b):
    return tuple(x + y for x, y in zip(a, b))


def minus(a, b):
    return tuple(x - y for x, y in zip(a, b))


def turned(a, part, whole, sign):
    part = part % whole
    eighths = 8 * part / whole
    if eighths == 0:
        return a
    if eighths == 2:
        return (-a[1], a[0]) if sign > 0 else (a[1], -a[0])
    if eighths == 4:
        return -a[0], -a[1]
    if eighths == 6:
        return (a[1], -a[0]) if sign > 0 else (-a[1], a[0])
    angle = sign * 2.0 * math.pi * part / whole
    cos_part, sin_part = math.cos(angle), math.sin(angle)
    if eighths in (1, 3, 5, 7):
        half = math.sqrt(0.5)
        c = half if cos_part > 0 else -half
        same = (cos_part > 0) == (sin_part > 0)
        if same:
            return (a[0] - a[1]) * c, (a[0] + a[1]) * c
        return (a[0] + a[1]) * c, (a[1] - a[0]) * c
    return a[0] * cos_part - a[1] * sin_part, a[0] * sin_part + a[1] * cos_part


def lane_sign(shape):
    return jnp.where(lax.broadcasted_iota(jnp.int32, shape, len(shape) - 1) < HALF, -1.0, 1.0)


def swapped(x):
    return pltpu.roll(x, HALF, x.ndim - 1)


def packed_times(x, turn):
    return x * turn[0] + swapped(x) * turn[1]


def packed_turned(a, part, whole, sign):
    part = part % whole
    angle = sign * 2.0 * math.pi * part / whole
    (x,) = a
    if part == 0:
        return a
    if 2 * part == whole:
        return (-x,)
    if 4 * part in (whole, 3 * whole):
        up = (4 * part == whole) == (sign > 0)
        return (swapped(x) * (lane_sign(x.shape) if up else -lane_sign(x.shape)),)
    return (math.cos(angle) * x + swapped(x) * (math.sin(angle) * lane_sign(x.shape)),)


def small_dft(xs, sign):
    n = len(xs)
    turn = turned if len(xs[0]) == 2 else packed_turned
    if n == 1:
        return xs
    if n == 2:
        return [plus(xs[0], xs[1]), minus(xs[0], xs[1])]
    parts = [small_dft(xs[r::4], sign) for r in range(4)]
    out = [None] * n
    for k in range(n // 4):
        a, b, c, d = (turn(parts[r][k], r * k, n, sign) for r in range(4))
        ac, bd = plus(a, c), plus(b, d)
        ac_, bd_ = minus(a, c), turn(minus(b, d), 1, 4, sign)
        out[k] = plus(ac, bd)
        out[k + n // 4] = plus(ac_, bd_)
        out[k + n // 2] = minus(ac, bd)
        out[k + 3 * n // 4] = minus(ac_, bd_)
    return out


def block_dft(load, scratch, finish, sign):
    for low in range(8):
        values = small_dft([load(8 * high + low) for high in range(16)], sign)
        for k, value in enumerate(values):
            turn = turned if len(value) == 2 else packed_turned
            value = turn(value, low * k, 128, sign)
            for c, x in enumerate(value):
                scratch[8 * k + low, c] = x
    parts = range(len(value))
    together = 1 if len(value) == 2 else 4

    def second(step, carry):
        ks = [together * step + n for n in range(together)]
        given = [
            [tuple(scratch[8 * k + low, c] for c in parts) for low in range(8)] for k in ks
        ]
        done = [small_dft(values, sign) for values in given]
        for k, values in zip(ks, done):
            for high, value in enumerate(values):
                finish(k + 16 * high, value)
        return carry

    lax.fori_loop(0, 16 // together, second, 0)


def quarter_sincos(angle, quarter):
    square = angle * angle
    sin_part = angle * (
        1.0 + square * (-1.0 / 6 + square * (1.0 / 120 + square * (-1.0 / 5040 + square / 362880)))
    )
    cos_part = 1.0 + square * (
        -0.5 + square * (1.0 / 24 + square * (-1.0 / 720 + square * (1.0 / 40320)))
    )
    odd = (quarter & 1) == 1
    first = jnp.where(odd, sin_part, cos_part)
    second = jnp.where(odd, cos_part, sin_part)
    return (
        jnp.where(((quarter + 1) & 2) == 2, -first, first),
        jnp.where((quarter & 2) == 2, -second, second),
    )


def unit(product, log_whole):
    quarter = (product + (1 << (log_whole - 3))) >> (log_whole - 2)
    rest = product - (quarter << (log_whole - 2))
    return quarter_sincos(rest.astype(F32) * (2.0 * math.pi / 2**log_whole), quarter)


def phase_unit(phase):
    quarter = jnp.floor(phase * (2.0 / math.pi) + 0.5)
    high = float(np.float32(1.5703125))
    angle = (phase - quarter * high) - quarter * (math.pi / 2 - high)
    return quarter_sincos(angle, quarter.astype(jnp.int32))


def halves(x):
    high = x.astype(BF16)
    return high, (x - high.astype(F32)).astype(BF16)


def frames_dft(matrix, real_part, imag_part):
    high, low = halves(jnp.concatenate([real_part, imag_part], axis=1))
    return lax.dot_general(
        matrix[...],
        jnp.concatenate([high, low, high], axis=1),
        (((1,), (1,)), ((), ())),
        preferred_element_type=F32,
    )


def kernel(
    voltage,
    phase,
    *refs,
):
    given, refs = refs[:CONSTANTS], refs[CONSTANTS:]
    late, ready, refs = refs[0], refs[1], refs[2:]
    held, refs = refs[:CONSTANTS], refs[CONSTANTS:]
    taps, rows_fwd, rows_inv, lanes_fwd, lanes_inv, lanes_out, mid_turn, mid_back, out_turn = held
    (
    recv1,
    work,
    send2,
    recv2,
    send3,
    recv3,
    send4,
    recv4,
    phase_in,
    phase_send,
    phase_recv,
    chirp,
    table_a,
    table_b,
    tiles,
    wide,
    edge_send,
    edge_recv,
    span_send,
    span_recv,
    half_taps,
    local_sem,
    sems1,
    sems2,
    sems3,
    sems4,
    phase_sem,
    edge_sem,
    span_sems,
    send_sems,
    out_sem,
    late_sem,
    given_sem,
    plane_sem,
    ) = refs
    row = lax.axis_index("row")
    col = lax.axis_index("col")
    me = row * 4 + col
    sublane = lax.broadcasted_iota(jnp.int32, (ROWS, LANES), 0)
    lane = lax.broadcasted_iota(jnp.int32, (ROWS, LANES), 1)

    phase_copy = pltpu.make_async_copy(phase, phase_in, local_sem.at[0])
    phase_copy.start()
    own_copy = pltpu.make_async_copy(
        voltage.at[:, :, pl.ds(pl.multiple_of(me * LANES, LANES), LANES)],
        recv1.at[me],
        local_sem.at[1],
    )
    own_copy.start()
    given_copies = [
        pltpu.make_async_copy(a, b, given_sem.at[n]) for n, (a, b) in enumerate(zip(given, held))
    ]
    for copy in given_copies:
        copy.start()

    place = row // 8, (col // 2) * 2 + lax.rem(row // 4, 2), lax.rem(row, 4), lax.rem(col, 2)
    z, y, x, core = place
    barrier = pltpu.get_barrier_semaphore()

    def greet_along(other):
        to = device_at(lax.rem(z + other, 4), y, x, core)
        return dict(inc=1, device_id=to, device_id_type=BY_MESH)

    for _, dy, dx, dc in (offset for offset in FAR_FIRST if offset[0] == 0):
        to = device_at(z, lax.rem(y + dy, 4), lax.rem(x + dx, 4), lax.rem(core + dc, 2))
        pl.semaphore_signal(barrier, inc=1, device_id=to, device_id_type=BY_MESH)
    for other in range(1, 4):
        pl.semaphore_signal(barrier, **greet_along(other))
    pl.semaphore_wait(barrier, 34)
    for other in range(1, 4):
        pl.semaphore_signal(plane_sem, **greet_along(other))
    pl.semaphore_wait(plane_sem, 3)

    rows_of = [
        [lax.rem(z + n, 4) * 8 for n in range(4)],
        [lax.rem(y + n, 2) * 4 for n in range(4)],
        [lax.rem(x + n, 4) for n in range(4)],
    ]
    cols_of = [
        [lax.rem(y + n, 4) // 2 * 2 for n in range(4)],
        [lax.rem(core + n, 2) for n in range(2)],
    ]

    def send_loop(source_of, target, send_sem, recv_sem):
        def one(step, carry):
            to_row, to_col = partner(place, step)
            pltpu.make_async_remote_copy(
                src_ref=source_of(to_row * 4 + to_col),
                dst_ref=target,
                send_sem=send_sem,
                recv_sem=recv_sem,
                device_id=(to_row, to_col),
                device_id_type=BY_MESH,
            ).start()
            return carry

        lax.fori_loop(1, DEVICES, one, 0)

    def send_all(order, source_of, target, send_sem, recv_sem_of):
        for n, (dz, dy, dx, dc) in enumerate(order):
            to_row = rows_of[0][dz] + rows_of[1][dy] + rows_of[2][dx]
            to_col = cols_of[0][dy] + cols_of[1][dc]
            pltpu.make_async_remote_copy(
                src_ref=source_of(to_row * 4 + to_col),
                dst_ref=target,
                send_sem=send_sem,
                recv_sem=recv_sem_of(n + 1),
                device_id=(to_row, to_col),
                device_id_type=BY_MESH,
            ).start()

    def tile_rows(part):
        return pl.ds(pl.multiple_of(part * TILE, TILE), TILE)

    def wait_part(buffer, sem):
        ref = buffer.at[pl.ds(0, DEVICES - 1), :, pl.ds(0, TILE), :]
        pltpu.make_async_copy(ref, ref, sem).wait()

    def voltage_part(part, carry):
        send_loop(
            lambda to: voltage.at[
                :, tile_rows(part), pl.ds(pl.multiple_of(to * LANES, LANES), LANES)
            ],
            recv1.at[me, :, tile_rows(part), :],
            send_sems.at[0],
            sems1.at[part],
        )
        return carry

    lax.fori_loop(0, PARTS, voltage_part, 0)

    phase_copy.wait()

    def phase_out(b, carry):
        block = phase_in[:, pl.ds(pl.multiple_of(b * LANES, LANES), LANES)]
        phase_send[:, pl.ds(b, 1), :] = jnp.transpose(block).reshape(DEVICES, 1, LANES)
        return carry

    lax.fori_loop(0, ROWS, phase_out, 0)

    send_loop(
        lambda to: phase_send.at[to],
        phase_recv.at[me],
        send_sems.at[1],
        phase_sem,
    )
    phase_recv[me] = phase_send[me]

    def fill(a, carry):
        cos_part, sin_part = unit(sublane * a, 12)
        table_a[a, 0] = cos_part
        table_a[a, 1] = -sin_part
        cos_part, sin_part = unit((a + 128 * sublane) * (128 * me + lane), LOG_TOTAL)
        table_b[a, 0] = cos_part
        table_b[a, 1] = -sin_part
        return carry

    lax.fori_loop(0, DEVICES, fill, 0)

    own_copy.wait()

    def first_part(part, carry):
        wait_part(recv1, sems1.at[part])
        at = tile_rows(part)

        def load(n):
            return recv1[n, 0, at, :], recv1[n, 1, at, :]

        def finish(k, value):
            turn = table_a[k, 0, at, :], table_a[k, 1, at, :]
            value = times(value, turn)
            work[k, 0, at, :] = value[0]
            work[k, 1, at, :] = value[1]

        block_dft(load, tiles, finish, -1)
        return carry

    lax.fori_loop(0, PARTS, first_part, 0)

    for copy in given_copies:
        copy.wait()

    first_lanes = lax.broadcasted_iota(jnp.int32, (8, LANES), 1) < HALF
    for high in range(8):
        columns = slice(high * LANES, high * LANES + LANES)
        straight = taps[:, columns]
        half_taps[0, :, columns] = jnp.where(first_lanes, straight, swapped(straight))
        half_taps[1, :, columns] = jnp.where(first_lanes, swapped(straight), straight)

    def split_dot(matrix, columns):
        high, low = halves(columns)
        return jnp.dot(
            matrix[...],
            jnp.concatenate([high, low, high], axis=0),
            preferred_element_type=F32,
        )

    def in_pairs(places):
        return zip(places[::2], places[1::2])

    def second_step(group, carry):
        done = []
        for pair in in_pairs([8 * group + n for n in range(8)]):
            both = split_dot(
                rows_fwd, jnp.concatenate([work[a].reshape(64, LANES) for a in pair], axis=1)
            )
            for n, a in enumerate(pair):
                columns = slice(n * LANES, n * LANES + LANES)
                done.append((a, (both[:ROWS, columns], both[ROWS:, columns])))
        for a, value in done:
            value = times(value, (table_b[a, 0], table_b[a, 1]))
            send2[a, 0] = value[0]
            send2[a, 1] = value[1]
        return carry

    lax.fori_loop(0, DEVICES // 8, second_step, 0)
    recv2[me] = send2[me]

    def send2_part(part, carry):
        send_loop(
            lambda to: send2.at[to, :, tile_rows(part), :],
            recv2.at[me, :, tile_rows(part), :],
            send_sems.at[2],
            sems2.at[part],
        )
        return carry

    lax.fori_loop(0, PARTS, send2_part, 0)

    phase_all = phase_recv.at[pl.ds(0, DEVICES - 1)]
    pltpu.make_async_copy(phase_all, phase_all, phase_sem).wait()

    def phase_back(b, carry):
        block = phase_recv[:, pl.ds(b, 1), :].reshape(DEVICES, LANES)
        cos_part, sin_part = phase_unit(jnp.transpose(block))
        chirp[:, 0, pl.ds(b, 1), :] = cos_part.reshape(DEVICES, 1, LANES)
        chirp[:, 1, pl.ds(b, 1), :] = sin_part.reshape(DEVICES, 1, LANES)
        return carry

    lax.fori_loop(0, ROWS, phase_back, 0)

    back_tables = table_b, work
    sign = lane_sign((ROWS, LANES))

    def refill(h, carry):
        for half in range(2):
            at = 128 * h + HALF * half + (lane & (HALF - 1))
            cos_part, sin_part = unit((me + 128 * sublane) * at, LOG_TOTAL)
            back_tables[half][h, 0] = cos_part
            back_tables[half][h, 1] = sin_part * sign
        return carry

    lax.fori_loop(0, DEVICES, refill, 0)

    def middle_part(part, carry):
        wait_part(recv2, sems2.at[part])
        at = tile_rows(part)

        def load(n):
            return recv2[n, 0, at, :], recv2[n, 1, at, :]

        def finish(k, value):
            turn = mid_turn[0, pl.ds(k, 1), :], mid_turn[1, pl.ds(k, 1), :]
            value = times(value, turn)
            wide[k, :, :LANES] = value[0]
            wide[k, :, LANES:] = value[1]

        block_dft(load, tiles, finish, -1)

        def lanes_step(group, inner):
            rows = pl.ds(group * 32, 32)
            high, low = halves(wide[rows].reshape(32 * TILE, 2 * LANES))
            there = jnp.dot(
                jnp.concatenate([high, low, high], axis=1),
                lanes_fwd[...],
                preferred_element_type=F32,
            )
            turn = (
                chirp[rows, 0, at, :].reshape(32 * TILE, LANES),
                chirp[rows, 1, at, :].reshape(32 * TILE, LANES),
            )
            there = times((there[:, :LANES], there[:, LANES:]), turn)
            high, low = halves(jnp.concatenate(there, axis=1))
            back = jnp.dot(
                jnp.concatenate([high, low, high], axis=1),
                lanes_inv[...],
                preferred_element_type=F32,
            )
            wide[rows] = back.reshape(32, TILE, 2 * LANES)
            return inner

        lax.fori_loop(0, 4, lanes_step, 0)

        for half in range(2):
            columns = slice(half * LANES, half * LANES + LANES)

            def load_back(n, half=half, columns=columns):
                turn = mid_back[2 * half, pl.ds(n, 1), :], mid_back[2 * half + 1, pl.ds(n, 1), :]
                return (packed_times(wide[n, :, columns], turn),)

            def finish_back(k, value, half=half):
                table = back_tables[half]
                send3[k, half, at, :] = packed_times(
                    value[0], (table[k, 0, at, :], table[k, 1, at, :])
                )

            block_dft(load_back, tiles, finish_back, 1)
            recv3[me, half, at, :] = send3[me, half, at, :]
        send3_rows(0, at, part * GROUPS)
        return carry

    def send3_rows(half, rows, first_sem):
        send_all(
            IN_STEPS,
            lambda to: send3.at[to, half, rows, :],
            recv3.at[me, half, rows, :],
            send_sems.at[3],
            lambda n: sems3.at[first_sem + n // 16],
        )

    lax.fori_loop(0, PARTS, middle_part, 0)
    send3_rows(1, slice(0, ROWS), PARTS * GROUPS)

    def third_step(half, group, eighth):
        places = []
        for n in range(8):
            from_row, from_col = partner(place, 16 * group + 8 * eighth + n, 3)
            places.append(from_row * 4 + from_col)
        done = []
        for pair in in_pairs(places):
            straight = [recv3[a, half] for a in pair]
            turned_up = [swapped(value) * sign for value in straight]
            both = split_dot(
                rows_inv,
                jnp.concatenate(
                    [jnp.concatenate(straight, axis=1), jnp.concatenate(turned_up, axis=1)], axis=0
                ),
            )
            for n, a in enumerate(pair):
                done.append((a, both[:, n * LANES : n * LANES + LANES]))
        for a, value in done:
            work[a, half] = packed_times(value, (table_a[a, 0], -sign * table_a[a, 1]))

    def third_group(half, group, count):
        def wait_rows(rows, sem):
            ref = recv3.at[pl.ds(0, count), half, pl.ds(0, rows), :]
            pltpu.make_async_copy(ref, ref, sems3.at[sem + group]).wait()

        def wait_one(part, inner):
            wait_rows(TILE, part * GROUPS)
            return inner

        if half == 0:
            lax.fori_loop(0, PARTS, wait_one, 0)
        else:
            wait_rows(ROWS, PARTS * GROUPS)

        def one(eighth, inner):
            third_step(half, group, eighth)
            return inner

        lax.fori_loop(0, 2, one, 0)

    def third_half(half):
        def later_group(group, carry):
            third_group(half, group, 16)
            return carry

        third_group(half, 0, 15)
        lax.fori_loop(1, GROUPS, later_group, 0)

    def fourth_part(half, part):
        at = slice(part * TILE, part * TILE + TILE)

        def load(n):
            return (work[n, half, at, :],)

        def finish(k, value):
            send4[k, half, at, :] = value[0]
            if half == 1 and part < 2:
                edge_send[k, part : part + 1, :] = value[0][TILE - 1 :]

        block_dft(load, tiles, finish, 1)
        recv4[me, half, at, :] = send4[me, half, at, :]

    def send4_tiles(half, first, count):
        at = slice(first * TILE, (first + count) * TILE)
        send_all(
            FAR_FIRST,
            lambda to: send4.at[to, half, at, :],
            recv4.at[me, half, at, :],
            send_sems.at[4],
            lambda n: sems4.at[half * PARTS + first],
        )

    def edge_pieces():
        send_all(
            FAR_FIRST,
            lambda to: edge_send.at[to],
            edge_recv.at[me],
            send_sems.at[5],
            lambda n: edge_sem,
        )

    def wait4(half, first, count):
        ref = recv4.at[pl.ds(0, DEVICES - 1), half, pl.ds(0, count * TILE), :]
        pltpu.make_async_copy(ref, ref, sems4.at[half * PARTS + first]).wait()

    following = lax.rem(me + 1, DEVICES)
    span_copies = [
        pltpu.make_async_remote_copy(
            src_ref=span_send.at[half],
            dst_ref=span_recv.at[half],
            send_sem=send_sems.at[6 + half],
            recv_sem=span_sems.at[half],
            device_id=(following // 4, lax.rem(following, 4)),
            device_id_type=BY_MESH,
        )
        for half in range(2)
    ]

    def send_span(half):
        def span_row(j, carry):
            span_send[half, pl.ds(j, 1), :] = recv4[FIRST_EDGE + j, half, ROWS - 1 :, :]
            return carry

        lax.fori_loop(0, DEVICES - FIRST_EDGE, span_row, 0)
        span_copies[half].start()

    with_edges = me >= FIRST_EDGE
    third_half(0)
    fourth_part(0, 3)
    send4_tiles(0, 3, 1)
    for part in (2, 1, 0):
        fourth_part(0, part)
    send4_tiles(0, 0, 3)
    third_half(1)
    for part in (3, 2, 1, 0):
        fourth_part(1, part)
    edge_recv[me] = edge_send[me]
    send4_tiles(1, 3, 1)
    wait4(0, 3, 1)
    send_span(0)
    pl.when(with_edges)(edge_pieces)
    send4_tiles(1, 2, 1)
    send4_tiles(1, 1, 1)

    first_row = lax.broadcasted_iota(jnp.int32, (TILE, LANES), 0) == 0
    ahead = me > 0
    frames = table_a.reshape(PARTS, 8, 2, 128, LANES)
    gathered = table_b.reshape(PARTS, 2, 1024, LANES)

    def filter_part(half, part):
        at = slice(part * TILE, part * TILE + TILE)

        def edge_row(high, m):
            if part == 0:
                edge = span_recv[half, pl.ds(8 * m + high - FIRST_EDGE, 1), :]
                return jnp.where(ahead, edge, 0.0)
            if half == 1 and part < 3:
                return edge_recv[8 * m + high, part - 1 : part, :]
            return recv4[8 * m + high, half, part * TILE - 1 : part * TILE, :]

        def one_position(high, carry):
            weights = [
                half_taps[half, t : t + 1, pl.ds(pl.multiple_of(high * LANES, LANES), LANES)]
                for t in range(8)
            ]
            now = [recv4[8 * m + high, half, at, :] for m in range(16)]
            old = [None] * 16
            for m in range(9, 16):
                old[m] = jnp.where(first_row, edge_row(high, m), pltpu.roll(now[m], 1, 0))
            for m in range(16):
                total = weights[0] * now[m]
                for t in range(1, 8):
                    total = total + weights[t] * (now[m - t] if m >= t else old[m - t + 16])
                work[16 * high + m, half, at, :] = total
            return carry

        lax.fori_loop(0, 8, one_position, 0)

        def some_frames(step, carry):
            ms = [8 * step + n for n in range(8)]
            given = [[(work[16 * high + m, half, at, :],) for high in range(8)] for m in ms]
            done = [small_dft(values, -1) for values in given]
            for m, values in zip(ms, done):
                for a, value in enumerate(values):
                    turn = (
                        out_turn[2 * half, a : a + 1, :],
                        out_turn[2 * half + 1, a : a + 1, :],
                    )
                    frames[part, a, half, pl.ds(m, TILE, stride=16), :] = packed_times(
                        value[0], turn
                    )
            return carry

        lax.fori_loop(0, 2, some_frames, 0)

    def ready_copy(part):
        return pltpu.make_async_copy(gathered.at[part], ready.at[part - 1], out_sem.at[part])

    def finish_parts(parts):
        classes = 2 // len(parts)

        def some_classes(step, carry):
            done = []
            for group in (2 * step, 2 * step + 1):
                each = [(p, classes * group + n) for n in range(classes) for p in parts]
                both = frames_dft(
                    lanes_out,
                    *[jnp.concatenate([frames[p, a, c] for p, a in each]) for c in range(2)],
                )
                done.append((each, both))
            for each, both in done:
                for c in range(2):
                    for n, (p, a) in enumerate(each):
                        gathered[p, c, pl.ds(a, 128, stride=8), :] = both[
                            c * 128 : c * 128 + 128, n * LANES : n * LANES + LANES
                        ]
            return carry

        lax.fori_loop(0, 4 // classes, some_classes, 0)
        for p in parts:
            ready_copy(p).start()

    late_copies = [
        pltpu.make_async_copy(frames.at[0, :, half], late.at[:, half], late_sem.at[half])
        for half in range(2)
    ]
    wait4(0, 0, 3)
    for part in (3, 2, 1):
        filter_part(0, part)
    wait4(1, 3, 1)
    send_span(1)
    send4_tiles(1, 0, 1)
    span_copies[0].wait_recv()
    filter_part(0, 0)
    late_copies[0].start()

    def wait_edges(count):
        ref = edge_recv.at[pl.ds(0, count)]
        pltpu.make_async_copy(ref, ref, edge_sem).wait()

    pl.when(with_edges)(lambda: wait_edges(DEVICES - FIRST_EDGE - 1))
    pl.when(jnp.logical_not(with_edges))(lambda: wait_edges(DEVICES - FIRST_EDGE))
    wait4(1, 2, 1)
    filter_part(1, 3)
    filter_part(1, 2)
    finish_parts((2, 3))
    wait4(1, 1, 1)
    filter_part(1, 1)
    finish_parts((1,))
    wait4(1, 0, 1)
    span_copies[1].wait_recv()
    filter_part(1, 0)
    late_copies[1].start()
    for part in range(1, PARTS):
        ready_copy(part).wait()
    for copy in late_copies:
        copy.wait()
    for copy in span_copies:
        copy.wait_send()

    def wait_edges_sent():
        ref = edge_recv.at[pl.ds(0, DEVICES - 1)]
        pltpu.make_async_copy(ref, ref, send_sems.at[5]).wait()

    pl.when(with_edges)(wait_edges_sent)
    pieces = recv1.at[pl.ds(0, DEVICES - 1)]
    for at in (0, 2, 3, 4):
        pltpu.make_async_copy(pieces, pieces, send_sems.at[at]).wait()
    pltpu.make_async_copy(phase_all, phase_all, send_sems.at[1]).wait()


def last_kernel(late, ready, lanes_out, result, frames, passing, gathered, matrix, sems, more):
    frame_copies = [
        pltpu.make_async_copy(late.at[pl.ds(4 * n, 4)], frames.at[pl.ds(4 * n, 4)], sems.at[n])
        for n in range(2)
    ]
    matrix_copy = pltpu.make_async_copy(lanes_out, matrix, more.at[0])
    pass_in = [
        pltpu.make_async_copy(ready.at[n], passing.at[n], more.at[1 + n]) for n in range(3)
    ]

    def to_result(source, column, sem):
        return pltpu.make_async_copy(source, result.at[:, :, pl.ds(column * LANES, LANES)], sem)

    passed = [to_result(passing.at[n], 1 + n, more.at[4 + n]) for n in range(3)]
    computed = to_result(gathered, 0, more.at[7])
    matrix_copy.start()
    for copy in frame_copies + pass_in:
        copy.start()
    matrix_copy.wait()
    for n in range(2):
        frame_copies[n].wait()
        pairs = [(4 * n, 4 * n + 1), (4 * n + 2, 4 * n + 3)]
        done = [
            frames_dft(matrix, *[jnp.concatenate([frames[a, c] for a in pair]) for c in range(2)])
            for pair in pairs
        ]
        for pair, both in zip(pairs, done):
            for c in range(2):
                for side, a in enumerate(pair):
                    gathered[c, pl.ds(a, 128, stride=8), :] = both[
                        c * 128 : c * 128 + 128, side * LANES : side * LANES + LANES
                    ]
        if n == 0:
            for copy_in, copy_out in zip(pass_in, passed):
                copy_in.wait()
                copy_out.start()
    computed.start()
    for copy in passed + [computed]:
        copy.wait()


def dft_parts(size, sign, scale=1.0):
    digits = np.arange(size)
    angle = sign * 2.0 * np.pi * ((digits[:, None] * digits[None, :]) % size) / size
    return scale * np.cos(angle), scale * np.sin(angle)


def bf16_halves(matrix):
    matrix = np.asarray(matrix, np.float32)
    high = matrix.astype(BF16)
    return high, (matrix - high.astype(np.float32)).astype(BF16)


BY_HALVES = np.concatenate([c * LANES + h * HALF + np.arange(HALF) for h in (0, 1) for c in (0, 1)])


def beside(matrix):
    high, low = bf16_halves(matrix)
    return np.concatenate([high, high, low], axis=1)


def above(matrix):
    high, low = bf16_halves(matrix)
    return np.concatenate([high, high, low], axis=0)


def left_matrix(size, sign):
    c, s = dft_parts(size, sign)
    return np.block([[c, -s], [s, c]])


def right_matrix(size, sign, scale=1.0):
    c, s = dft_parts(size, sign, scale)
    return np.block([[c, s], [-s, c]])


def turn_table(rows, cols, sign):
    whole = rows * cols
    angle = sign * 2.0 * np.pi * (np.arange(rows)[:, None] * np.arange(cols)[None, :]) / whole
    return np.stack([np.cos(angle), np.sin(angle)]).astype(np.float32)


def packed_table(rows, cols, sign):
    c, s = turn_table(rows, cols, sign)
    each = []
    for half in (slice(0, HALF), slice(HALF, LANES)):
        each.append(np.concatenate([c[:, half], c[:, half]], axis=1))
        each.append(np.concatenate([-s[:, half], s[:, half]], axis=1))
    return np.stack(each)


def local(voltage, chirp_phase, filter_taps):
    constants = [
        beside(left_matrix(ROWS, -1)),
        beside(np.concatenate(dft_parts(ROWS, 1), axis=1)),
        above(right_matrix(LANES, -1)),
        above(right_matrix(LANES, 1, 2.0**-LOG_TOTAL)[:, BY_HALVES]),
        beside(left_matrix(LANES, -1)[:, BY_HALVES]),
        turn_table(128, LANES, -1),
        packed_table(128, LANES, 1),
        packed_table(8, LANES, -1),
    ]
    blocks = pltpu.VMEM((DEVICES, 2, ROWS, LANES), F32)
    phases = pltpu.VMEM((DEVICES, ROWS, LANES), F32)
    in_hbm = pl.BlockSpec(memory_space=pl.ANY)
    given = [filter_taps] + [jnp.asarray(c) for c in constants]
    late, ready = pl.pallas_call(
        kernel,
        out_shape=[
            jax.ShapeDtypeStruct((8, 2, 128, LANES), F32),
            jax.ShapeDtypeStruct((3, 2, 1024, LANES), F32),
        ],
        in_specs=[in_hbm] * (2 + len(given)),
        out_specs=[in_hbm] * 2,
        scratch_shapes=[pltpu.VMEM(c.shape, c.dtype) for c in given]
        + [blocks] * 8
        + [pltpu.VMEM((DEVICES, 4096), F32)]
        + [phases] * 2
        + [blocks] * 3
        + [
            pltpu.VMEM((DEVICES, 2, TILE, LANES), F32),
            pltpu.VMEM((DEVICES, TILE, 2 * LANES), F32),
            pltpu.VMEM((DEVICES, 2, LANES), F32),
            pltpu.VMEM((DEVICES, 2, LANES), F32),
            pltpu.VMEM((2, DEVICES - FIRST_EDGE, LANES), F32),
            pltpu.VMEM((2, DEVICES - FIRST_EDGE, LANES), F32),
            pltpu.VMEM((2, 8, 1024), F32),
            pltpu.SemaphoreType.DMA((2,)),
            pltpu.SemaphoreType.DMA((PARTS,)),
            pltpu.SemaphoreType.DMA((PARTS,)),
            pltpu.SemaphoreType.DMA(((PARTS + 1) * GROUPS,)),
            pltpu.SemaphoreType.DMA((2 * PARTS,)),
            pltpu.SemaphoreType.DMA,
            pltpu.SemaphoreType.DMA,
            pltpu.SemaphoreType.DMA((2,)),
            pltpu.SemaphoreType.DMA((8,)),
            pltpu.SemaphoreType.DMA((PARTS,)),
            pltpu.SemaphoreType.DMA((2,)),
            pltpu.SemaphoreType.DMA((CONSTANTS,)),
            pltpu.SemaphoreType.REGULAR,
        ],
        compiler_params=pltpu.CompilerParams(
            collective_id=0, has_side_effects=True, vmem_limit_bytes=67043328
        ),
    )(voltage, chirp_phase, *given)
    return pl.pallas_call(
        last_kernel,
        out_shape=jax.ShapeDtypeStruct((2, 1024, 512), F32),
        in_specs=[in_hbm] * 3,
        out_specs=in_hbm,
        scratch_shapes=[
            pltpu.VMEM((8, 2, 128, LANES), F32),
            pltpu.VMEM((3, 2, 1024, LANES), F32),
            pltpu.VMEM((2, 1024, LANES), F32),
            pltpu.VMEM((256, 768), BF16),
            pltpu.SemaphoreType.DMA((8,)),
            pltpu.SemaphoreType.DMA((8,)),
        ],
        compiler_params=pltpu.CompilerParams(vmem_limit_bytes=67043328),
    )(late, ready, given[5])


def solution(mesh):
    in_specs = (P(None, ("row", "col"), None), P(("row", "col"), None), P())
    out_specs = P(None, None, ("row", "col"))
    return jax.shard_map(local, mesh=mesh, in_specs=in_specs, out_specs=out_specs, check_vma=False)
```
